32 devices in a mesh: leg: 2 (over y), ping: 8 (over z, core), rng: 2 (over x).
Axes of the slice: x: 2, y: 2, z: 4, core: 2. Of those that a mesh axis runs over, the one named last changes fastest.
Arguments:
- echo: bfloat16 [2, 16384, 256], P(None, ('leg', 'ping'), 'rng'), parts along dimension 1, may hold values from -6 to 6
- steer: bfloat16 [2, 16384, 8192], P(None, ('leg', 'rng'), 'ping'), parts along dimension 1, may hold values from -0.046875 to 0.046875
- offsets: int32 [256], P(('leg', 'ping')), parts along dimension 0, may hold values from 0 to 15
- taps: float32 [256, 4], P(('leg', 'ping')), parts along dimension 0, may hold values from 0.1 to 1
- centers: int32 [512], P(('leg', 'ping', 'rng')), parts along dimension 0, may hold values from 0 to 8191
- halves: int32 [512], P(('leg', 'ping', 'rng')), parts along dimension 0, may hold values from 128 to 1024
Outputs:
- focused: float32 [2, 512, 8192], P(None, ('leg', 'ping', 'rng')), parts along dimension 1
- phase_error: float32 [16384], P('leg'), parts along dimension 0
The draws below stay inside these ranges and needn't reach their ends.
There are 2 independent parts, one for each index of `leg`. The reference program is written for one: setup_inputs(seed, part) draws one part's arguments, and reference() takes and returns one part's arrays. A program takes and returns all parts, laid end to end along the dimension named above; each array names one. Nothing has to cross between parts.
All inputs are finite; a program needn't handle non-finite values.
Results may differ from the reference program's by a relative error of at most 0.0049.
Values may be sent and summed in bfloat16 or wider, within the bound.
A program may use at most 64 MiB of HBM per device.

```python
import math
import jax
import jax.numpy as jnp
from jax import lax

A = 8192
PBLK = 64
NTAP = 4
MAXOFF = 16
R = 256
P_SIZE = 8192
NBLK = 128


def place_ends(array, key, smallest, high):
    place = [jax.random.randint(jax.random.fold_in(key, axis), (), 0, length) for axis, length in enumerate(array.shape)]
    widest = array.shape.index(max(array.shape))
    beside = place[:widest] + [(place[widest] + 1) % array.shape[widest]] + place[widest + 1:]
    return array.at[tuple(place)].set(smallest).at[tuple(beside)].set(high)


def level_of(rng, shape, shards, low, high):
    level, own = 1.0, jax.random.fold_in(rng, 6)
    for axis_at, blocks in shards:
        draws = jnp.exp(jax.random.uniform(jax.random.fold_in(own, axis_at), (blocks,), jnp.float32, low / len(shards), high / len(shards)))
        level = level * jnp.repeat(draws, shape[axis_at] // blocks).reshape([-1 if axis == axis_at else 1 for axis in range(len(shape))])
    return level


def normal_values(key, shape, width, most, pieces=(), kind=jnp.bfloat16):
    entries = width * jax.random.normal(key, shape, jnp.float32)
    if pieces:
        entries = entries * level_of(key, shape, pieces, -0.22, 0.18)
    return jnp.clip(entries, -most, most).astype(kind)


def setup_inputs(seed: int = 0, part: int = 0) -> dict:
    arg_keys = jax.random.split(jax.random.key(seed), 7)
    part_splits = jax.random.split(jax.random.fold_in(arg_keys[6], part), 7)
    return {
        "echo": normal_values(part_splits[0], (2, P_SIZE, R), 1.0, 6.0, ((1, 8), (2, 2))),
        "steer": normal_values(part_splits[1], (2, A, P_SIZE), (2 * P_SIZE) ** -0.5, 0.046875, ((1, 2), (2, 8))),
        "offsets": place_ends(jax.random.randint(part_splits[2], (NBLK,), 0, MAXOFF), jax.random.fold_in(part_splits[2], 1), 0, MAXOFF - 1).astype(jnp.int32),
        "taps": jnp.clip(0.1 + 0.9 * jax.random.uniform(part_splits[3], (NBLK, NTAP), jnp.float32) ** level_of(part_splits[3], (NBLK, NTAP), ((0, 8),), -0.2, 0.2), 0.1, 1.0),
        "centers": place_ends(jax.random.randint(part_splits[4], (R,), 0, A), jax.random.fold_in(part_splits[4], 1), 0, A - 1).astype(jnp.int32),
        "halves": place_ends(jax.random.randint(part_splits[5], (R,), A // 64, A // 8 + 1), jax.random.fold_in(part_splits[5], 1), A // 64, (A // 8 + 1) - 1).astype(jnp.int32),
    }


epsilon = 1e-6


def shift_segment(segment, offset, weights, length):
    margin = MAXOFF + NTAP - 1
    first_col = (margin - offset - (NTAP - 1)).astype(jnp.int32)
    window = lax.dynamic_slice_in_dim(segment, first_col, length + NTAP - 1, axis=2)
    result = jnp.zeros(segment.shape[:2] + (length,), jnp.float32)
    for tap_index in range(NTAP):
        lead_cols = NTAP - 1 - tap_index
        result = result + weights[tap_index] * window[:, :, lead_cols:lead_cols + length]
    return result


def reference(echo, steer, offsets, taps, centers, halves):
    margin = MAXOFF + NTAP - 1
    padded = jnp.pad(echo.astype(jnp.float32), ((0, 0), (0, 0), (margin, 0)))
    blocks = padded.reshape(2, NBLK, PBLK, margin + R)
    shifted = jax.vmap(lambda segment, offset, weights: shift_segment(segment, offset, weights, R),
                       in_axes=(1, 0, 0), out_axes=1)(blocks, offsets, taps)
    interp = shifted.reshape(2, P_SIZE, R).astype(jnp.bfloat16)
    interp = lax.optimization_barrier(interp).astype(jnp.float32)
    weights_full = steer.astype(jnp.float32)
    highest = lax.Precision.HIGHEST
    image_real = jnp.dot(interp[0].T, weights_full[0].T, precision=highest) - jnp.dot(interp[1].T, weights_full[1].T, precision=highest)
    image_imag = jnp.dot(interp[0].T, weights_full[1].T, precision=highest) + jnp.dot(interp[1].T, weights_full[0].T, precision=highest)
    image = lax.complex(image_real, image_imag)
    spectrum = jnp.fft.fft(image, axis=1)
    cells = jnp.arange(A, dtype=jnp.int32)
    distance = (cells[None, :] - centers[:, None]) % A
    distance = jnp.minimum(distance, (A - distance) % A)
    inside = (distance <= halves[:, None]).astype(jnp.float32)
    windowed = jnp.fft.fft(image * inside, axis=1)
    angle = (2.0 * math.pi / A) * centers.astype(jnp.float32)
    turned = lax.complex(jnp.cos(angle), jnp.sin(angle))
    cross = jnp.conj(windowed) * jnp.roll(windowed, -1, axis=1) * turned[:, None]
    numer = jnp.sum(jnp.imag(cross), axis=0)
    denom = jnp.sum(jnp.real(windowed) ** 2 + jnp.imag(windowed) ** 2, axis=0)
    slope = numer / (denom + epsilon)
    phase_error = jnp.cumsum(slope) - slope - jnp.arange(A, dtype=jnp.float32) * (jnp.sum(slope) / A)
    rotation = lax.complex(jnp.cos(phase_error), -jnp.sin(phase_error))
    corrected = jnp.fft.ifft(spectrum * rotation[None, :], axis=1)
    focused = jnp.stack([jnp.real(corrected), jnp.imag(corrected)])
    return focused, phase_error
```

```python
import functools
import math

import jax
import jax.numpy as jnp
from jax import lax
from jax.experimental import pallas as pl
from jax.experimental.pallas import tpu as pltpu
from jax.sharding import PartitionSpec as P

PBLK = 64
NTAP = 4


epsilon = 1e-06


MESH = pl.DeviceIdType.MESH


CORES = 2
LAG = 2


def meet(peers, extra):
    barrier = pltpu.get_barrier_semaphore()
    for peer in peers:
        pl.semaphore_signal(barrier, inc=1, device_id=peer, device_id_type=MESH)
    total = len(peers)
    for present, peer in extra:
        total = total + present.astype(jnp.int32)

        @pl.when(present)
        def _():
            pl.semaphore_signal(barrier, inc=1, device_id=peer, device_id_type=MESH)

    pl.semaphore_wait(barrier, total)


def encode(value, target):
    count, width = value.shape
    groups = count // 16
    peak = jnp.max(jnp.abs(value), axis=1, keepdims=True)
    power = jnp.floor(jnp.log2(jnp.maximum(peak, 1e-30)) + 1.01)
    whole = jnp.round(value * jnp.exp2(15.0 - power)).astype(jnp.int32).astype(jnp.int16)
    for piece in range(width // 128):
        target[piece * count:(piece + 1) * count, :] = whole[:, piece * 128:(piece + 1) * 128]
    lane = lax.broadcasted_iota(jnp.int32, (16, 128), 1) // (128 // groups)
    powers = jnp.zeros((16, 128), jnp.float32)
    for group in range(groups):
        powers = jnp.where(lane == group, power[group * 16:(group + 1) * 16], powers)
    target[width // 128 * count:, :] = powers.astype(jnp.int32).astype(jnp.int16)


def decode(source, count, width):
    groups = count // 16
    powers = source[width // 128 * count:, :].astype(jnp.int32).astype(jnp.float32)
    scales = jnp.exp2(powers - 15.0)
    span = 128 // groups
    scale = jnp.concatenate(
        [scales[:, group * span:group * span + 1] for group in range(groups)], axis=0
    )
    pieces = [
        source[piece * count:(piece + 1) * count, :].astype(jnp.int32).astype(jnp.float32) * scale
        for piece in range(width // 128)
    ]
    return jnp.concatenate(pieces, axis=1)


def image_kernel(
    plan, offsets_ref, taps_ref, echo_ref, steer_ref, out_ref,
    held, left, weights, part, got, away, near, fin, side,
    own_sem, echo_send, echo_recv, load_sem, pair_send, pair_recv,
    line_send, line_recv, side_send, side_recv,
):
    tiles, chips, chunks, width, lines = plan
    pings = echo_ref.shape[1]
    columns = echo_ref.shape[2]
    count = tiles * 2 * lines
    me = lax.axis_index("rng")
    chip = lax.axis_index("ping") // CORES
    core = lax.axis_index("ping") % CORES
    last = chips - 1

    def load(chunk, half):
        return pltpu.make_async_copy(
            steer_ref.at[half, pl.ds(chunk * width, width), :],
            weights.at[chunk, :, pl.ds(half * pings, pings)],
            load_sem.at[chunk, half],
        )

    for chunk in range(chunks):
        for half in range(2):
            load(chunk, half).start()
    own = pltpu.make_async_copy(echo_ref, held.at[me], own_sem)
    own.start()
    peers = [{"rng": lax.rem(me + step, tiles)} for step in range(1, tiles)]
    partner = {"ping": chip * CORES + 1 - core}
    above = {"ping": (chip + 1) * CORES + core}
    below = {"ping": (chip - 1) * CORES + core}
    meet(peers + [partner], [(chip < last, above), (chip > 0, below)])
    copies = []
    for step, peer in enumerate(peers):
        copy = pltpu.make_async_remote_copy(
            src_ref=echo_ref,
            dst_ref=held.at[me],
            send_sem=echo_send.at[step],
            recv_sem=echo_recv.at[step],
            device_id=peer,
            device_id_type=MESH,
        )
        copy.start()
        copies.append(copy)
    own.wait()
    for copy in copies:
        copy.wait()

    full = tiles * columns
    column = lax.broadcasted_iota(jnp.int32, (PBLK, full), 1)

    def interpolate(index, carry):
        cols = pl.multiple_of(index * 128, 128)
        turned = []
        for half in range(2):
            blocks = []
            for inner in range(128 // PBLK):
                block = index * (128 // PBLK) + inner
                rows = pl.ds(pl.multiple_of(block * PBLK, PBLK), PBLK)
                value = jnp.concatenate([held[tile, half, rows, :] for tile in range(tiles)], axis=1)
                value = value.astype(jnp.float32)
                offset = offsets_ref[block]
                result = jnp.zeros((PBLK, full), jnp.float32)
                for tap in range(NTAP):
                    shift = offset + tap
                    moved = jnp.where(column >= shift, pltpu.roll(value, shift, axis=1), 0.0)
                    result = result + taps_ref[block, tap] * moved
                blocks.append(result)
            turned.append(jnp.concatenate(blocks, axis=0).T)
        real, imag = turned
        for parity in range(CORES):
            for target in range(chips):
                for tile in range(tiles):
                    first = ((target * CORES + parity) * tiles + tile) * lines
                    place = ((parity * chips + target) * tiles + tile) * 2 * lines
                    a = real[first:first + lines].astype(jnp.bfloat16)
                    b = imag[first:first + lines].astype(jnp.bfloat16)
                    left[place:place + lines, pl.ds(cols, 128)] = a
                    left[place + lines:place + 2 * lines, pl.ds(cols, 128)] = b
                    left[place:place + lines, pl.ds(pings + cols, 128)] = -b
                    left[place + lines:place + 2 * lines, pl.ds(pings + cols, 128)] = a
        return carry

    lax.fori_loop(0, pings // 128, interpolate, 0)

    def pair(chunk):
        return pltpu.make_async_remote_copy(
            src_ref=part.at[chunk, 1 - core],
            dst_ref=got.at[chunk],
            send_sem=pair_send.at[chunk],
            recv_sem=pair_recv.at[chunk],
            device_id=partner,
            device_id_type=MESH,
        )

    def line(way, target, chunk):
        return pltpu.make_async_remote_copy(
            src_ref=away.at[way, target, chunk],
            dst_ref=near.at[way, target, chunk],
            send_sem=line_send.at[way, target, chunk],
            recv_sem=line_recv.at[way, target, chunk],
            device_id=(above, below)[way],
            device_id_type=MESH,
        )

    def collect(way, target, chunk):
        line(way, target, chunk).wait_recv()
        rows = pl.ds(pl.multiple_of(target * count, count), count)
        part[chunk, core, rows, :] += decode(near.at[way, target, chunk], count, width)

    def pass_on(way, target, chunk, first):
        @pl.when(jnp.logical_not(first))
        def _():
            collect(way, target, chunk)

        encode(part[chunk, core, target * count:(target + 1) * count, :], away.at[way, target, chunk])
        line(way, target, chunk).start()

    block = min(512, CORES * chips * count)
    halves = chips * count

    def multiply(chunk):
        for half in range(2):
            load(chunk, half).wait()

        def rows_of(index, carry):
            rows = pl.ds(pl.multiple_of(index * block, block), block)
            value = lax.dot_general(
                left[rows, :], weights[chunk], (((1,), (1,)), ((), ())),
                preferred_element_type=jnp.float32,
            )
            if block > halves:
                part[chunk, 0] = value[:halves]
                part[chunk, 1] = value[halves:]
            else:
                inside = pl.ds(pl.multiple_of(index % (halves // block) * block, block), block)
                part[chunk, index // (halves // block), inside, :] = value
            return carry

        lax.fori_loop(0, CORES * halves // block, rows_of, 0)
        pair(chunk).start()

    def step(time, carry):
        @pl.when(time < chunks)
        def _():
            multiply(time)

        chunk = time - 1

        @pl.when(jnp.logical_and(chunk >= 0, chunk < chunks))
        def _():
            pair(chunk).wait_recv()
            part[chunk, core] += got[chunk]

        for way in range(2):
            hops = (chip, last - chip)[way]
            at = chunk - hops * LAG
            ready = jnp.logical_and(at >= 0, at < chunks)
            for away_by in range(chips - 2):
                target = (last - away_by, away_by)[way]
                ahead = (chip < target, chip > target)[way]

                @pl.when(jnp.logical_and(ready, ahead))
                def _():
                    pass_on(way, target, at, hops == 0)

        return carry

    lax.fori_loop(0, chunks + 1 + (chips - 1) * LAG, step, 0)

    def nearest(chunk, carry):
        @pl.when(chip == 0)
        def _():
            pass_on(0, 1, chunk, True)

        @pl.when(chip == last)
        def _():
            pass_on(1, last - 1, chunk, True)

        return carry

    lax.fori_loop(0, chunks, nearest, 0)

    def across(step, chunk):
        peer = lax.rem(me + step, tiles)
        return pltpu.make_async_remote_copy(
            src_ref=fin.at[chunk, peer],
            dst_ref=side.at[chunk, step - 1],
            send_sem=side_send.at[step - 1, chunk],
            recv_sem=side_recv.at[step - 1, chunk],
            device_id={"rng": peer},
            device_id_type=MESH,
        )

    def place(source, chunk, value):
        start = pl.multiple_of(source * (chunks * width) + chunk * width, width)
        out_ref[0, :, pl.ds(start, width)] = value[:lines]
        out_ref[1, :, pl.ds(start, width)] = value[lines:]

    def finish(chunk, carry):
        @pl.when(chip > 0)
        def _():
            collect(0, chip, chunk)

        @pl.when(chip < last)
        def _():
            collect(1, chip, chunk)

        for tile in range(tiles):
            rows = pl.ds(pl.multiple_of(chip * count + tile * 2 * lines, 2 * lines), 2 * lines)
            fin[chunk, tile] = part[chunk, core, rows, :]
        for step in range(1, tiles):
            across(step, chunk).start()
        place(me, chunk, fin[chunk, me])
        return carry

    lax.fori_loop(0, chunks, finish, 0)

    def arrive(chunk, carry):
        for step in range(1, tiles):
            across(step, chunk).wait()
            place(lax.rem(me + tiles - step, tiles), chunk, side[chunk, step - 1])
        pair(chunk).wait_send()
        for way in range(2):
            for target in range(chips):
                ahead = (chip < target, chip > target)[way]

                @pl.when(ahead)
                def _():
                    line(way, target, chunk).wait_send()

        return carry

    lax.fori_loop(0, chunks, arrive, 0)


def lines_image(echo, steer, offsets, taps):
    tiles = lax.axis_size("rng")
    chips = lax.axis_size("ping") // CORES
    pings, columns = echo.shape[1:]
    cells = steer.shape[1]
    width = 512 if cells % 4096 == 0 else 256
    chunks = cells // width
    lines = columns // (chips * CORES)
    count = tiles * 2 * lines
    rows = chips * count
    vmem = pl.BlockSpec(memory_space=pltpu.VMEM)
    smem = pl.BlockSpec(memory_space=pltpu.SMEM)
    dma = pltpu.SemaphoreType.DMA
    message = (width // 128 * count + 16, 128)
    others = max(tiles - 1, 1)
    return pl.pallas_call(
        functools.partial(image_kernel, (tiles, chips, chunks, width, lines)),
        out_shape=jax.ShapeDtypeStruct((2, lines, tiles * cells), jnp.float32),
        in_specs=[smem, smem, vmem, pl.BlockSpec(memory_space=pl.ANY)],
        out_specs=vmem,
        scratch_shapes=[
            pltpu.VMEM((tiles, 2, pings, columns), jnp.bfloat16),
            pltpu.VMEM((CORES * rows, 2 * pings), jnp.bfloat16),
            pltpu.VMEM((chunks, width, 2 * pings), jnp.bfloat16),
            pltpu.VMEM((chunks, CORES, rows, width), jnp.float32),
            pltpu.VMEM((chunks, rows, width), jnp.float32),
            pltpu.VMEM((2, chips, chunks) + message, jnp.int16),
            pltpu.VMEM((2, chips, chunks) + message, jnp.int16),
            pltpu.VMEM((chunks, tiles, 2 * lines, width), jnp.float32),
            pltpu.VMEM((chunks, others, 2 * lines, width), jnp.float32),
            dma,
            dma((others,)),
            dma((others,)),
            dma((chunks, 2)),
            dma((chunks,)),
            dma((chunks,)),
            dma((2, chips, chunks)),
            dma((2, chips, chunks)),
            dma((others, chunks)),
            dma((others, chunks)),
        ],
        compiler_params=pltpu.CompilerParams(
            collective_id=0, has_side_effects=True, vmem_limit_bytes=60 * 2**20
        ),
    )(offsets, taps, echo, steer)


def total_kernel(pings, tiles, value_ref, out_ref, held, full, send_sem, recv_sem, send_two, recv_two):
    count = pings * tiles
    me = lax.axis_index("ping") * tiles + lax.axis_index("rng")
    ids = [lax.rem(me + step, count) for step in range(1, count)]
    peers = [{"ping": lax.div(one, tiles), "rng": lax.rem(one, tiles)} for one in ids]
    meet(peers, [])
    copies = []
    for step, peer in enumerate(peers):
        copy = pltpu.make_async_remote_copy(
            src_ref=value_ref.at[ids[step]],
            dst_ref=held.at[step],
            send_sem=send_sem.at[step],
            recv_sem=recv_sem.at[step],
            device_id=peer,
            device_id_type=MESH,
        )
        copy.start()
        copies.append(copy)
    total = value_ref[me]
    for step, copy in enumerate(copies):
        copy.wait()
        total = total + held[step]
    full[me] = total
    copies = []
    for step, peer in enumerate(peers):
        copy = pltpu.make_async_remote_copy(
            src_ref=full.at[me],
            dst_ref=full.at[me],
            send_sem=send_two.at[step],
            recv_sem=recv_two.at[step],
            device_id=peer,
            device_id_type=MESH,
        )
        copy.start()
        copies.append(copy)
    for copy in copies:
        copy.wait()
    out_ref[...] = full[...]


def total_over(first, second):
    pings, tiles = lax.axis_size("ping"), lax.axis_size("rng")
    count = pings * tiles
    length = first.shape[0]
    value = jnp.concatenate([first, second]).reshape(count, -1, 128)
    vmem = pl.BlockSpec(memory_space=pltpu.VMEM)
    semaphores = pltpu.SemaphoreType.DMA((count - 1,))
    total = pl.pallas_call(
        functools.partial(total_kernel, pings, tiles),
        out_shape=jax.ShapeDtypeStruct(value.shape, jnp.float32),
        in_specs=[vmem],
        out_specs=vmem,
        scratch_shapes=[
            pltpu.VMEM((count - 1,) + value.shape[1:], jnp.float32),
            pltpu.VMEM(value.shape, jnp.float32),
            semaphores,
            semaphores,
            semaphores,
            semaphores,
        ],
        compiler_params=pltpu.CompilerParams(collective_id=1, has_side_effects=True),
    )(value).reshape(2, length)
    return total[0], total[1]


def split_length(length):
    factor_low = 1
    candidate = 1
    while candidate * candidate <= length:
        if length % candidate == 0:
            factor_low = candidate
        candidate = candidate + 1
    return factor_low


def table(rows_count, cols_count, modulus, direction):
    row_ids = jnp.arange(rows_count, dtype=jnp.int32)
    col_ids = jnp.arange(cols_count, dtype=jnp.int32)
    product = row_ids[:, None] * col_ids[None, :] % modulus
    angle = direction * 2.0 * math.pi / modulus * product.astype(jnp.float32)
    return (jnp.cos(angle), jnp.sin(angle))


def transform(real_part, imag_part, direction):
    length = real_part.shape[-1]
    size_low = split_length(length)
    size_high = length // size_low
    lead_shape = real_part.shape[:-1]
    highest = lax.Precision.HIGHEST
    real_grid = real_part.reshape(lead_shape + (size_low, size_high))
    imag_grid = imag_part.reshape(lead_shape + (size_low, size_high))
    first_cos, first_sin = table(size_low, size_low, size_low, direction)
    section_real = jnp.einsum(
        "kn,...nm->...km", first_cos, real_grid, precision=highest
    ) - jnp.einsum("kn,...nm->...km", first_sin, imag_grid, precision=highest)
    section_imag = jnp.einsum(
        "kn,...nm->...km", first_cos, imag_grid, precision=highest
    ) + jnp.einsum("kn,...nm->...km", first_sin, real_grid, precision=highest)
    twist_cos, twist_sin = table(size_low, size_high, length, direction)
    twisted_real = section_real * twist_cos - section_imag * twist_sin
    twisted_imag = section_real * twist_sin + section_imag * twist_cos
    second_cos, second_sin = table(size_high, size_high, size_high, direction)
    final_real = jnp.einsum(
        "bm,...km->...bk", second_cos, twisted_real, precision=highest
    ) - jnp.einsum("bm,...km->...bk", second_sin, twisted_imag, precision=highest)
    final_imag = jnp.einsum(
        "bm,...km->...bk", second_cos, twisted_imag, precision=highest
    ) + jnp.einsum("bm,...km->...bk", second_sin, twisted_real, precision=highest)
    return (final_real.reshape(lead_shape + (length,)), final_imag.reshape(lead_shape + (length,)))


def on_device(echo, steer, offsets, taps, centers, halves):
    image = lines_image(echo, steer, offsets, taps)
    length = image.shape[2]
    cells = jnp.arange(length, dtype=jnp.int32)
    distance = (cells[None, :] - centers[:, None]) % length
    distance = jnp.minimum(distance, (length - distance) % length)
    inside = (distance <= halves[:, None]).astype(jnp.float32)
    stacked_real = jnp.stack([image[0], image[0] * inside])
    stacked_imag = jnp.stack([image[1], image[1] * inside])
    spec_real, spec_imag = transform(stacked_real, stacked_imag, -1.0)
    window_real = spec_real[1]
    window_imag = spec_imag[1]
    next_real = jnp.roll(window_real, -1, axis=1)
    next_imag = jnp.roll(window_imag, -1, axis=1)
    cross_real = window_real * next_real + window_imag * next_imag
    cross_imag = window_real * next_imag - window_imag * next_real
    angle = 2.0 * math.pi / length * centers.astype(jnp.float32)
    numer_local = jnp.sum(
        cross_real * jnp.sin(angle)[:, None] + cross_imag * jnp.cos(angle)[:, None], axis=0
    )
    denom_local = jnp.sum(window_real * window_real + window_imag * window_imag, axis=0)
    numer, denom = total_over(numer_local, denom_local)
    slope = numer / (denom + epsilon)
    phase_error = (
        jnp.cumsum(slope)
        - slope
        - jnp.arange(length, dtype=jnp.float32) * (jnp.sum(slope) / length)
    )
    cos_phase = jnp.cos(phase_error)[None, :]
    sin_phase = jnp.sin(phase_error)[None, :]
    full_real = spec_real[0]
    full_imag = spec_imag[0]
    fixed_real = full_real * cos_phase + full_imag * sin_phase
    fixed_imag = full_imag * cos_phase - full_real * sin_phase
    out_real, out_imag = transform(fixed_real, fixed_imag, 1.0)
    focused = jnp.stack([out_real, out_imag]) / length
    return (focused, phase_error)


def solution(mesh):
    in_specs = (
        P(None, ("leg", "ping"), "rng"),
        P(None, ("leg", "rng"), "ping"),
        P(("leg", "ping")),
        P(("leg", "ping"), None),
        P(("leg", "ping", "rng")),
        P(("leg", "ping", "rng")),
    )
    out_specs = (P(None, ("leg", "ping", "rng"), None), P("leg"))
    return jax.shard_map(
        on_device, mesh=mesh, in_specs=in_specs, out_specs=out_specs, check_vma=False
    )
```

```python
import functools
import math

import jax
import jax.numpy as jnp
import numpy as np
from jax import lax
from jax.experimental import pallas as pl
from jax.experimental.pallas import tpu as pltpu
from jax.sharding import PartitionSpec as P

PBLK = 64
NTAP = 4


epsilon = 1e-06


MESH = pl.DeviceIdType.MESH


CORES = 2
LAG = 2


def meet(peers, extra):
    barrier = pltpu.get_barrier_semaphore()
    for peer in peers:
        pl.semaphore_signal(barrier, inc=1, device_id=peer, device_id_type=MESH)
    total = len(peers)
    for present, peer in extra:
        total = total + present.astype(jnp.int32)

        @pl.when(present)
        def _():
            pl.semaphore_signal(barrier, inc=1, device_id=peer, device_id_type=MESH)

    pl.semaphore_wait(barrier, total)


def encode(value, target):
    count, width = value.shape
    groups = count // 16
    peak = jnp.max(jnp.abs(value), axis=1, keepdims=True)
    power = jnp.floor(jnp.log2(jnp.maximum(peak, 1e-30)) + 1.01)
    whole = jnp.round(value * jnp.exp2(15.0 - power)).astype(jnp.int32).astype(jnp.int16)
    for piece in range(width // 128):
        target[piece * count:(piece + 1) * count, :] = whole[:, piece * 128:(piece + 1) * 128]
    lane = lax.broadcasted_iota(jnp.int32, (16, 128), 1) // (128 // groups)
    powers = jnp.zeros((16, 128), jnp.float32)
    for group in range(groups):
        powers = jnp.where(lane == group, power[group * 16:(group + 1) * 16], powers)
    target[width // 128 * count:, :] = powers.astype(jnp.int32).astype(jnp.int16)


def decode(source, count, width):
    groups = count // 16
    powers = source[width // 128 * count:, :].astype(jnp.int32).astype(jnp.float32)
    scales = jnp.exp2(powers - 15.0)
    span = 128 // groups
    scale = jnp.concatenate(
        [scales[:, group * span:group * span + 1] for group in range(groups)], axis=0
    )
    pieces = [
        source[piece * count:(piece + 1) * count, :].astype(jnp.int32).astype(jnp.float32) * scale
        for piece in range(width // 128)
    ]
    return jnp.concatenate(pieces, axis=1)


def image_kernel(
    plan, offsets_ref, taps_ref, echo_ref, steer_ref, out_ref,
    held, left, weights, part, got, away, near, fin, side,
    own_sem, echo_send, echo_recv, load_sem, pair_send, pair_recv,
    line_send, line_recv, side_send, side_recv,
):
    tiles, chips, chunks, width, lines = plan
    pings = echo_ref.shape[1]
    columns = echo_ref.shape[2]
    count = tiles * 2 * lines
    me = lax.axis_index("rng")
    chip = lax.axis_index("ping") // CORES
    core = lax.axis_index("ping") % CORES
    last = chips - 1

    def load(chunk, half):
        return pltpu.make_async_copy(
            steer_ref.at[half, pl.ds(chunk * width, width), :],
            weights.at[chunk, :, pl.ds(half * pings, pings)],
            load_sem.at[chunk, half],
        )

    for chunk in range(chunks):
        for half in range(2):
            load(chunk, half).start()
    own = pltpu.make_async_copy(echo_ref, held.at[me], own_sem)
    own.start()
    peers = [{"rng": lax.rem(me + step, tiles)} for step in range(1, tiles)]
    partner = {"ping": chip * CORES + 1 - core}
    above = {"ping": (chip + 1) * CORES + core}
    below = {"ping": (chip - 1) * CORES + core}
    meet(peers + [partner], [(chip < last, above), (chip > 0, below)])
    copies = []
    for step, peer in enumerate(peers):
        copy = pltpu.make_async_remote_copy(
            src_ref=echo_ref,
            dst_ref=held.at[me],
            send_sem=echo_send.at[step],
            recv_sem=echo_recv.at[step],
            device_id=peer,
            device_id_type=MESH,
        )
        copy.start()
        copies.append(copy)
    own.wait()
    for copy in copies:
        copy.wait()

    full = tiles * columns
    column = lax.broadcasted_iota(jnp.int32, (PBLK, full), 1)

    def interpolate(index, carry):
        cols = pl.multiple_of(index * 128, 128)
        turned = []
        for half in range(2):
            blocks = []
            for inner in range(128 // PBLK):
                block = index * (128 // PBLK) + inner
                rows = pl.ds(pl.multiple_of(block * PBLK, PBLK), PBLK)
                value = jnp.concatenate([held[tile, half, rows, :] for tile in range(tiles)], axis=1)
                value = value.astype(jnp.float32)
                offset = offsets_ref[block]
                result = jnp.zeros((PBLK, full), jnp.float32)
                for tap in range(NTAP):
                    shift = offset + tap
                    moved = jnp.where(column >= shift, pltpu.roll(value, shift, axis=1), 0.0)
                    result = result + taps_ref[block, tap] * moved
                blocks.append(result)
            turned.append(jnp.concatenate(blocks, axis=0).T)
        real, imag = turned
        for parity in range(CORES):
            for target in range(chips):
                for tile in range(tiles):
                    first = ((target * CORES + parity) * tiles + tile) * lines
                    place = ((parity * chips + target) * tiles + tile) * 2 * lines
                    a = real[first:first + lines].astype(jnp.bfloat16)
                    b = imag[first:first + lines].astype(jnp.bfloat16)
                    left[place:place + lines, pl.ds(cols, 128)] = a
                    left[place + lines:place + 2 * lines, pl.ds(cols, 128)] = b
                    left[place:place + lines, pl.ds(pings + cols, 128)] = -b
                    left[place + lines:place + 2 * lines, pl.ds(pings + cols, 128)] = a
        return carry

    lax.fori_loop(0, pings // 128, interpolate, 0)

    def pair(chunk):
        return pltpu.make_async_remote_copy(
            src_ref=part.at[chunk, 1 - core],
            dst_ref=got.at[chunk],
            send_sem=pair_send.at[chunk],
            recv_sem=pair_recv.at[chunk],
            device_id=partner,
            device_id_type=MESH,
        )

    def line(way, target, chunk):
        return pltpu.make_async_remote_copy(
            src_ref=away.at[way, target, chunk],
            dst_ref=near.at[way, target, chunk],
            send_sem=line_send.at[way, target, chunk],
            recv_sem=line_recv.at[way, target, chunk],
            device_id=(above, below)[way],
            device_id_type=MESH,
        )

    def collect(way, target, chunk):
        line(way, target, chunk).wait_recv()
        rows = pl.ds(pl.multiple_of(target * count, count), count)
        part[chunk, core, rows, :] += decode(near.at[way, target, chunk], count, width)

    def pass_on(way, target, chunk, first):
        @pl.when(jnp.logical_not(first))
        def _():
            collect(way, target, chunk)

        encode(part[chunk, core, target * count:(target + 1) * count, :], away.at[way, target, chunk])
        line(way, target, chunk).start()

    block = min(512, CORES * chips * count)
    halves = chips * count

    def multiply(chunk):
        for half in range(2):
            load(chunk, half).wait()

        def rows_of(index, carry):
            rows = pl.ds(pl.multiple_of(index * block, block), block)
            value = lax.dot_general(
                left[rows, :], weights[chunk], (((1,), (1,)), ((), ())),
                preferred_element_type=jnp.float32,
            )
            if block > halves:
                part[chunk, 0] = value[:halves]
                part[chunk, 1] = value[halves:]
            else:
                inside = pl.ds(pl.multiple_of(index % (halves // block) * block, block), block)
                part[chunk, index // (halves // block), inside, :] = value
            return carry

        lax.fori_loop(0, CORES * halves // block, rows_of, 0)
        pair(chunk).start()

    def step(time, carry):
        @pl.when(time < chunks)
        def _():
            multiply(time)

        chunk = time - 1

        @pl.when(jnp.logical_and(chunk >= 0, chunk < chunks))
        def _():
            pair(chunk).wait_recv()
            part[chunk, core] += got[chunk]

        for way in range(2):
            hops = (chip, last - chip)[way]
            at = chunk - hops * LAG
            ready = jnp.logical_and(at >= 0, at < chunks)
            for away_by in range(chips - 2):
                target = (last - away_by, away_by)[way]
                ahead = (chip < target, chip > target)[way]

                @pl.when(jnp.logical_and(ready, ahead))
                def _():
                    pass_on(way, target, at, hops == 0)

        return carry

    lax.fori_loop(0, chunks + 1 + (chips - 1) * LAG, step, 0)

    def nearest(chunk, carry):
        @pl.when(chip == 0)
        def _():
            pass_on(0, 1, chunk, True)

        @pl.when(chip == last)
        def _():
            pass_on(1, last - 1, chunk, True)

        return carry

    lax.fori_loop(0, chunks, nearest, 0)

    def across(step, chunk):
        peer = lax.rem(me + step, tiles)
        return pltpu.make_async_remote_copy(
            src_ref=fin.at[chunk, peer],
            dst_ref=side.at[chunk, step - 1],
            send_sem=side_send.at[step - 1, chunk],
            recv_sem=side_recv.at[step - 1, chunk],
            device_id={"rng": peer},
            device_id_type=MESH,
        )

    def place(source, chunk, value):
        start = pl.multiple_of(source * (chunks * width) + chunk * width, width)
        out_ref[0, :, pl.ds(start, width)] = value[:lines]
        out_ref[1, :, pl.ds(start, width)] = value[lines:]

    def finish(chunk, carry):
        @pl.when(chip > 0)
        def _():
            collect(0, chip, chunk)

        @pl.when(chip < last)
        def _():
            collect(1, chip, chunk)

        for tile in range(tiles):
            rows = pl.ds(pl.multiple_of(chip * count + tile * 2 * lines, 2 * lines), 2 * lines)
            fin[chunk, tile] = part[chunk, core, rows, :]
        for step in range(1, tiles):
            across(step, chunk).start()
        place(me, chunk, fin[chunk, me])
        return carry

    lax.fori_loop(0, chunks, finish, 0)

    def arrive(chunk, carry):
        for step in range(1, tiles):
            across(step, chunk).wait()
            place(lax.rem(me + tiles - step, tiles), chunk, side[chunk, step - 1])
        pair(chunk).wait_send()
        for way in range(2):
            for target in range(chips):
                ahead = (chip < target, chip > target)[way]

                @pl.when(ahead)
                def _():
                    line(way, target, chunk).wait_send()

        return carry

    lax.fori_loop(0, chunks, arrive, 0)


def lines_image(echo, steer, offsets, taps):
    tiles = lax.axis_size("rng")
    chips = lax.axis_size("ping") // CORES
    pings, columns = echo.shape[1:]
    cells = steer.shape[1]
    width = 512 if cells % 4096 == 0 else 256
    chunks = cells // width
    lines = columns // (chips * CORES)
    count = tiles * 2 * lines
    rows = chips * count
    vmem = pl.BlockSpec(memory_space=pltpu.VMEM)
    smem = pl.BlockSpec(memory_space=pltpu.SMEM)
    dma = pltpu.SemaphoreType.DMA
    message = (width // 128 * count + 16, 128)
    others = max(tiles - 1, 1)
    return pl.pallas_call(
        functools.partial(image_kernel, (tiles, chips, chunks, width, lines)),
        out_shape=jax.ShapeDtypeStruct((2, lines, tiles * cells), jnp.float32),
        in_specs=[smem, smem, vmem, pl.BlockSpec(memory_space=pl.ANY)],
        out_specs=vmem,
        scratch_shapes=[
            pltpu.VMEM((tiles, 2, pings, columns), jnp.bfloat16),
            pltpu.VMEM((CORES * rows, 2 * pings), jnp.bfloat16),
            pltpu.VMEM((chunks, width, 2 * pings), jnp.bfloat16),
            pltpu.VMEM((chunks, CORES, rows, width), jnp.float32),
            pltpu.VMEM((chunks, rows, width), jnp.float32),
            pltpu.VMEM((2, chips, chunks) + message, jnp.int16),
            pltpu.VMEM((2, chips, chunks) + message, jnp.int16),
            pltpu.VMEM((chunks, tiles, 2 * lines, width), jnp.float32),
            pltpu.VMEM((chunks, others, 2 * lines, width), jnp.float32),
            dma,
            dma((others,)),
            dma((others,)),
            dma((chunks, 2)),
            dma((chunks,)),
            dma((chunks,)),
            dma((2, chips, chunks)),
            dma((2, chips, chunks)),
            dma((others, chunks)),
            dma((others, chunks)),
        ],
        compiler_params=pltpu.CompilerParams(
            collective_id=0, has_side_effects=True, vmem_limit_bytes=60 * 2**20
        ),
    )(offsets, taps, echo, steer)


LANES = 128


def split(value):
    high = value.astype(jnp.bfloat16)
    return high, (value - high.astype(jnp.float32)).astype(jnp.bfloat16)


def exact_dot(left, right):
    total = None
    for _ in range(3):
        piece = right.astype(jnp.bfloat16)
        term = jnp.dot(left, piece, preferred_element_type=jnp.float32)
        total = term if total is None else total + term
        right = right - piece.astype(jnp.float32)
    return total


def dot_exact(left, right):
    total = None
    for _ in range(3):
        piece = left.astype(jnp.bfloat16)
        term = jnp.dot(piece, right, preferred_element_type=jnp.float32)
        total = term if total is None else total + term
        left = left - piece.astype(jnp.float32)
    return total


def focus_kernel(
    count, tiles, centers_ref, halves_ref, down_ref, up_ref, over_ref, back_ref, twist_ref,
    image_ref, out_ref, phase_ref,
    grid, spec, value, held, full, turned, send_sem, recv_sem, send_two, recv_two,
):
    me = lax.axis_index("ping") * tiles + lax.axis_index("rng")
    ids = [lax.rem(me + step, count) for step in range(1, count)]
    peers = [{"ping": lax.div(one, tiles), "rng": lax.rem(one, tiles)} for one in ids]
    barrier = pltpu.get_barrier_semaphore()
    for peer in peers:
        pl.semaphore_signal(barrier, inc=1, device_id=peer, device_id_type=MESH)

    lines, length = image_ref.shape[1:]
    high = length // LANES
    for half in range(2):
        for row in range(high):
            grid[pl.ds(half * high + row, lines, stride=2 * high), :] = image_ref[
                half, :, row * LANES:(row + 1) * LANES
            ]

    cells = lax.broadcasted_iota(jnp.int32, (high, LANES), 0) * LANES
    cells = cells + lax.broadcasted_iota(jnp.int32, (high, LANES), 1)
    bottom = lax.broadcasted_iota(jnp.int32, (8, LANES), 0) == 7
    lane = lax.broadcasted_iota(jnp.int32, (8, LANES), 1)
    angle = jnp.zeros((8, LANES), jnp.float32)
    for line in range(lines):
        angle = jnp.where(lane == line, centers_ref[line].astype(jnp.float32), angle)
    angle = angle * (2.0 * math.pi / length)
    turned[0] = jnp.cos(angle)
    turned[1] = jnp.sin(angle)

    def after(part):
        moved = pltpu.roll(part, high - 1, axis=0)
        end = moved[high - 8:]
        end = jnp.where(bottom, pltpu.roll(end, LANES - 1, axis=1), end)
        return jnp.concatenate([moved[:high - 8], end], axis=0)

    def forward(line, carry):
        numer, denom = carry
        rows = pl.ds(pl.multiple_of(line * 2 * high, 2 * high), 2 * high)
        whole = grid[rows, :]
        distance = cells - centers_ref[line]
        distance = jnp.where(distance < 0, distance + length, distance)
        distance = jnp.minimum(distance, length - distance)
        inside = (distance <= halves_ref[line]).astype(jnp.float32)
        chosen = whole * jnp.concatenate([inside, inside], axis=0)
        top, low = split(jnp.concatenate([whole, chosen], axis=1))
        first = jnp.dot(
            down_ref[...], jnp.concatenate([top, low, top], axis=0), preferred_element_type=jnp.float32
        )
        pieces = []
        for which in range(2):
            real = first[:high, which * LANES:(which + 1) * LANES]
            imag = first[high:, which * LANES:(which + 1) * LANES]
            pieces.append(
                jnp.concatenate(
                    [
                        real * twist_ref[0] + imag * twist_ref[1],
                        imag * twist_ref[0] - real * twist_ref[1],
                    ],
                    axis=1,
                )
            )
        top, low = split(jnp.concatenate(pieces, axis=0))
        second = jnp.dot(
            jnp.concatenate([top, low, top], axis=1), over_ref[...], preferred_element_type=jnp.float32
        )
        spec[pl.ds(pl.multiple_of(line * high, high), high), :] = second[:high]
        real = second[high:, :LANES]
        imag = second[high:, LANES:]
        next_real = after(real)
        next_imag = after(imag)
        here = lane == line
        cos = jnp.sum(jnp.where(here, turned[0], 0.0), axis=1, keepdims=True)[:1]
        sin = jnp.sum(jnp.where(here, turned[1], 0.0), axis=1, keepdims=True)[:1]
        numer = numer + (real * next_real + imag * next_imag) * sin
        numer = numer + (real * next_imag - imag * next_real) * cos
        denom = denom + (real * real + imag * imag)
        return numer, denom

    zero = jnp.zeros((high, LANES), jnp.float32)
    numer, denom = lax.fori_loop(0, lines, forward, (zero, zero), unroll=2)
    each = value.shape[1]
    for block in range(count // 2):
        value[block] = numer[block * each:(block + 1) * each]
        value[count // 2 + block] = denom[block * each:(block + 1) * each]

    pl.semaphore_wait(barrier, len(peers))
    copies = []
    for step, peer in enumerate(peers):
        copy = pltpu.make_async_remote_copy(
            src_ref=value.at[ids[step]],
            dst_ref=held.at[step],
            send_sem=send_sem.at[step],
            recv_sem=recv_sem.at[step],
            device_id=peer,
            device_id_type=MESH,
        )
        copy.start()
        copies.append(copy)
    total = value[me]
    for step, copy in enumerate(copies):
        copy.wait()
        total = total + held[step]
    full[me] = total
    copies = []
    for step, peer in enumerate(peers):
        copy = pltpu.make_async_remote_copy(
            src_ref=full.at[me],
            dst_ref=full.at[me],
            send_sem=send_two.at[step],
            recv_sem=recv_two.at[step],
            device_id=peer,
            device_id_type=MESH,
        )
        copy.start()
        copies.append(copy)
    for copy in copies:
        copy.wait()
    numer = jnp.concatenate([full[block] for block in range(count // 2)], axis=0)
    denom = jnp.concatenate([full[count // 2 + block] for block in range(count // 2)], axis=0)
    slope = numer / (denom + epsilon)
    below = lax.broadcasted_iota(jnp.int32, (high, high), 1) < lax.broadcasted_iota(jnp.int32, (high, high), 0)
    ahead = lax.broadcasted_iota(jnp.int32, (LANES, LANES), 0) < lax.broadcasted_iota(jnp.int32, (LANES, LANES), 1)
    within = exact_dot(below.astype(jnp.float32).astype(jnp.bfloat16), slope)
    sums = jnp.broadcast_to(jnp.sum(slope, axis=0, keepdims=True), (8, LANES))
    across = dot_exact(sums, ahead.astype(jnp.float32).astype(jnp.bfloat16))
    mean = jnp.sum(sums[:1], axis=1, keepdims=True) / length
    order = lax.broadcasted_iota(jnp.int32, (high, LANES), 0)
    order = order + high * lax.broadcasted_iota(jnp.int32, (high, LANES), 1)
    phase = within + across[:1] - order.astype(jnp.float32) * mean
    phase_ref[...] = phase
    cos = jnp.cos(phase)
    sin = jnp.sin(phase)

    def inverse(line, carry):
        rows = pl.ds(pl.multiple_of(line * high, high), high)
        real = spec[rows, :LANES]
        imag = spec[rows, LANES:]
        fixed = jnp.concatenate([real * cos + imag * sin, imag * cos - real * sin], axis=1)
        top, low = split(fixed)
        first = jnp.dot(
            jnp.concatenate([top, low, top], axis=1), back_ref[...], preferred_element_type=jnp.float32
        )
        real = first[:, :LANES]
        imag = first[:, LANES:]
        undone = jnp.concatenate(
            [
                real * twist_ref[2] - imag * twist_ref[3],
                real * twist_ref[3] + imag * twist_ref[2],
            ],
            axis=0,
        )
        top, low = split(undone)
        grid[pl.ds(pl.multiple_of(line * 2 * high, 2 * high), 2 * high), :] = jnp.dot(
            up_ref[...], jnp.concatenate([top, low, top], axis=0), preferred_element_type=jnp.float32
        )
        return carry

    lax.fori_loop(0, lines, inverse, 0, unroll=2)
    for half in range(2):
        for row in range(high):
            out_ref[half, :, row * LANES:(row + 1) * LANES] = grid[
                pl.ds(half * high + row, lines, stride=2 * high), :
            ]


def waves(size, modulus, columns):
    angle = 2.0 * np.pi / modulus * (np.outer(np.arange(size), np.arange(columns)) % modulus)
    return np.cos(angle), np.sin(angle)


def pieces_of(matrix, axis):
    high = matrix.astype(jnp.bfloat16)
    low = (matrix - high.astype(np.float64)).astype(jnp.bfloat16)
    return np.concatenate([high, high, low], axis=axis)


def focus(image, centers, halves):
    pings, tiles = lax.axis_size("ping"), lax.axis_size("rng")
    count = pings * tiles
    lines, length = image.shape[1:]
    high = length // LANES
    cos, sin = waves(high, high, high)
    down = pieces_of(np.block([[cos, sin], [-sin, cos]]), 1)
    up = pieces_of(np.block([[cos, -sin], [sin, cos]]), 1)
    cos, sin = waves(LANES, LANES, LANES)
    over = pieces_of(np.block([[cos, -sin], [sin, cos]]), 0)
    back = pieces_of(np.block([[cos, sin], [-sin, cos]]), 0)
    cos, sin = waves(high, length, LANES)
    twist = np.stack([cos, sin, cos / length, sin / length]).astype(np.float32)
    each = 2 * high // count
    vmem = pl.BlockSpec(memory_space=pltpu.VMEM)
    smem = pl.BlockSpec(memory_space=pltpu.SMEM)
    semaphores = pltpu.SemaphoreType.DMA((count - 1,))
    focused, phase = pl.pallas_call(
        functools.partial(focus_kernel, count, tiles),
        out_shape=(
            jax.ShapeDtypeStruct((2, lines, length), jnp.float32),
            jax.ShapeDtypeStruct((high, LANES), jnp.float32),
        ),
        in_specs=[smem, smem] + [vmem] * 6,
        out_specs=(vmem, vmem),
        scratch_shapes=[
            pltpu.VMEM((lines * 2 * high, LANES), jnp.float32),
            pltpu.VMEM((lines * high, 2 * LANES), jnp.float32),
            pltpu.VMEM((count, each, LANES), jnp.float32),
            pltpu.VMEM((count - 1, each, LANES), jnp.float32),
            pltpu.VMEM((count, each, LANES), jnp.float32),
            pltpu.VMEM((2, 8, LANES), jnp.float32),
            semaphores,
            semaphores,
            semaphores,
            semaphores,
        ],
        compiler_params=pltpu.CompilerParams(collective_id=1, has_side_effects=True),
    )(centers, halves, down, up, over, back, twist, image)
    return focused, phase.T.reshape(length)


def on_device(echo, steer, offsets, taps, centers, halves):
    image = lines_image(echo, steer, offsets, taps)
    return focus(image, centers, halves)


def solution(mesh):
    in_specs = (
        P(None, ("leg", "ping"), "rng"),
        P(None, ("leg", "rng"), "ping"),
        P(("leg", "ping")),
        P(("leg", "ping"), None),
        P(("leg", "ping", "rng")),
        P(("leg", "ping", "rng")),
    )
    out_specs = (P(None, ("leg", "ping", "rng"), None), P("leg"))
    return jax.shard_map(
        on_device, mesh=mesh, in_specs=in_specs, out_specs=out_specs, check_vma=False
    )
```

```python
import functools
import math

import jax
import jax.numpy as jnp
import numpy as np
from jax import lax
from jax.experimental import pallas as pl
from jax.experimental.pallas import tpu as pltpu
from jax.sharding import PartitionSpec as P

PBLK = 64
NTAP = 4


epsilon = 1e-06


MESH = pl.DeviceIdType.MESH


CORES = 2
LAG = 3
EDGE = 32


def encode(value, target):
    count, width = value.shape
    groups = count // 16
    peak = jnp.max(jnp.abs(value), axis=1, keepdims=True)
    power = jnp.floor(jnp.log2(jnp.maximum(peak, 1e-30)) + 1.01)
    whole = jnp.round(value * jnp.exp2(15.0 - power)).astype(jnp.int32).astype(jnp.int16)
    for piece in range(width // 128):
        target[piece * count:(piece + 1) * count, :] = whole[:, piece * 128:(piece + 1) * 128]
    lane = lax.broadcasted_iota(jnp.int32, (16, 128), 1) // (128 // groups)
    powers = jnp.zeros((16, 128), jnp.float32)
    for group in range(groups):
        powers = jnp.where(lane == group, power[group * 16:(group + 1) * 16], powers)
    target[width // 128 * count:, :] = powers.astype(jnp.int32).astype(jnp.int16)


def decode(source, count, width):
    groups = count // 16
    powers = source[width // 128 * count:, :].astype(jnp.int32).astype(jnp.float32)
    scales = jnp.exp2(powers - 15.0)
    span = 128 // groups
    scale = jnp.concatenate(
        [scales[:, group * span:group * span + 1] for group in range(groups)], axis=0
    )
    pieces = [
        source[piece * count:(piece + 1) * count, :].astype(jnp.int32).astype(jnp.float32) * scale
        for piece in range(width // 128)
    ]
    return jnp.concatenate(pieces, axis=1)


def order_of(targets, own):
    return [one for one in targets if one in own] + [one for one in targets if one not in own]


def pick(table, row, column):
    found = jnp.int32(table[0][0])
    for at_row, entries in enumerate(table):
        for at_column, entry in enumerate(entries):
            here = jnp.logical_and(row == at_row, column == at_column)
            found = jnp.where(here, jnp.int32(entry), found)
    return found


def image_kernel(
    plan, offsets_ref, taps_hbm, echo_ref, steer_ref, out_ref,
    taps_ref, held, edge_out, edge_in, left, weights, part, got, away, near, fin, side,
    taps_sem, own_sem, edge_send, edge_recv, echo_send, echo_recv, load_sem, pair_send, pair_recv,
    line_send, line_recv, side_send, side_recv,
):
    tiles, chips, chunks, width, lines, groups = plan
    pings = echo_ref.shape[1]
    columns = echo_ref.shape[2]
    count = tiles * 2 * lines
    share = chips // groups
    me = lax.axis_index("rng")
    chip = lax.axis_index("ping") // CORES
    core = lax.axis_index("ping") % CORES
    last = chips - 1
    partner = {"ping": chip * CORES + 1 - core}
    above = {"ping": (chip + 1) * CORES + core}
    below = {"ping": (chip - 1) * CORES + core}
    peers = [{"rng": lax.rem(me + step, tiles)} for step in range(1, tiles)]

    barrier = pltpu.get_barrier_semaphore()
    for peer in peers + [partner]:
        pl.semaphore_signal(barrier, inc=1, device_id=peer, device_id_type=MESH)

    @pl.when(chip < last)
    def _():
        pl.semaphore_signal(barrier, inc=1, device_id=above, device_id_type=MESH)

    @pl.when(chip > 0)
    def _():
        pl.semaphore_signal(barrier, inc=1, device_id=below, device_id_type=MESH)

    tap_copy = pltpu.make_async_copy(taps_hbm, taps_ref, taps_sem)
    tap_copy.start()
    own = pltpu.make_async_copy(echo_ref, held.at[me], own_sem)
    own.start()

    def load(chunk, half):
        return pltpu.make_async_copy(
            steer_ref.at[half, pl.ds(chunk * width, width), :],
            weights.at[chunk, :, pl.ds(half * pings, pings)],
            load_sem.at[chunk, half],
        )

    for chunk in range(chunks):
        for half in range(2):
            load(chunk, half).start()

    def edge():
        return pltpu.make_async_remote_copy(
            src_ref=edge_out,
            dst_ref=edge_in,
            send_sem=edge_send,
            recv_sem=edge_recv,
            device_id={"rng": lax.rem(me + 1, tiles)},
            device_id_type=MESH,
        )

    if groups > 1:
        def pack(index, carry):
            cols = pl.ds(pl.multiple_of(index * 128, 128), 128)
            for half in range(2):
                value = echo_ref[half, cols, :].astype(jnp.float32).T
                edge_out[half, :, cols] = value[columns - EDGE:].astype(jnp.bfloat16)
            return carry

        lax.fori_loop(0, pings // 128, pack, 0)

    reached = len(peers) + 1 + (chip < last).astype(jnp.int32) + (chip > 0).astype(jnp.int32)
    pl.semaphore_wait(barrier, reached)
    if groups > 1:
        @pl.when(me < tiles - 1)
        def _():
            edge().start()

    copies = []
    for step, peer in enumerate(peers):
        copy = pltpu.make_async_remote_copy(
            src_ref=echo_ref,
            dst_ref=held.at[me],
            send_sem=echo_send.at[step],
            recv_sem=echo_recv.at[step],
            device_id=peer,
            device_id_type=MESH,
        )
        copy.start()
        copies.append(copy)
    own.wait()
    tap_copy.wait()
    column = lax.broadcasted_iota(jnp.int32, (PBLK, 2 * columns), 1)

    def interpolate(tile, before):
        def one(index, carry):
            cols = pl.multiple_of(index * 128, 128)
            turned = []
            for half in range(2):
                ahead = before(half, cols)
                value = held[tile, half, pl.ds(cols, 128), :].astype(jnp.float32)
                value = jnp.concatenate([ahead, value], axis=1)
                blocks = []
                for inner in range(128 // PBLK):
                    block = index * (128 // PBLK) + inner
                    piece = value[inner * PBLK:(inner + 1) * PBLK]
                    offset = offsets_ref[block]
                    result = jnp.zeros((PBLK, columns), jnp.float32)
                    for tap in range(NTAP):
                        moved = pltpu.roll(piece, offset + tap, axis=1)[:, columns:]
                        result = result + taps_ref[tap, block] * moved
                    blocks.append(result)
                turned.append(jnp.concatenate(blocks, axis=0).T)
            real, imag = turned
            for piece in range(columns // lines):
                row = tile * (columns // lines) + piece
                owner = row // tiles
                target = owner // CORES
                place = (target // share * CORES + owner % CORES) * share + target % share
                place = pl.multiple_of((place * tiles + row % tiles) * 2 * lines, 2 * lines)
                a = real[piece * lines:(piece + 1) * lines].astype(jnp.bfloat16)
                b = imag[piece * lines:(piece + 1) * lines].astype(jnp.bfloat16)
                left[pl.ds(place, lines), pl.ds(cols, 128)] = a
                left[pl.ds(place + lines, lines), pl.ds(cols, 128)] = b
                left[pl.ds(place, lines), pl.ds(pings + cols, 128)] = -b
                left[pl.ds(place + lines, lines), pl.ds(pings + cols, 128)] = a
            return carry

        lax.fori_loop(0, pings // 128, one, 0)

    def from_edge(half, cols):
        value = edge_in[half, :, pl.ds(cols, 128)].astype(jnp.float32)
        value = jnp.where(me > 0, value, 0.0)
        return jnp.concatenate([jnp.zeros((columns - EDGE, 128), jnp.float32), value], axis=0).T

    def from_tile(tile):
        def before(half, cols):
            value = held[lax.max(tile - 1, 0), half, pl.ds(cols, 128), :].astype(jnp.float32)
            return jnp.where(tile > 0, value, 0.0)

        return before

    def pair(group, chunk):
        rows = pl.ds(pl.multiple_of(group * share * count, share * count), share * count)
        return pltpu.make_async_remote_copy(
            src_ref=part.at[chunk, 1 - core, rows],
            dst_ref=got.at[chunk, rows],
            send_sem=pair_send.at[group, chunk],
            recv_sem=pair_recv.at[group, chunk],
            device_id=partner,
            device_id_type=MESH,
        )

    def line(way, target, chunk):
        return pltpu.make_async_remote_copy(
            src_ref=away.at[way, target, chunk],
            dst_ref=near.at[way, target, chunk],
            send_sem=line_send.at[way, target, chunk],
            recv_sem=line_recv.at[way, target, chunk],
            device_id=(above, below)[way],
            device_id_type=MESH,
        )

    def rows_of(target):
        return pl.ds(pl.multiple_of(target * count, count), count)

    def collect(way, target, chunk):
        line(way, target, chunk).wait_recv()
        part[chunk, core, rows_of(target), :] += decode(near.at[way, target, chunk], count, width)

    def pass_on(way, target, chunk, first):
        @pl.when(jnp.logical_not(first))
        def _():
            collect(way, target, chunk)

        encode(part[chunk, core, rows_of(target), :], away.at[way, target, chunk])
        line(way, target, chunk).start()

    half_rows = share * count
    block = min(512, CORES * half_rows)

    def multiply(group, chunk, first):
        if first:
            for half in range(2):
                load(chunk, half).wait()
        base = group * CORES * half_rows
        if block == CORES * half_rows:
            rows = pl.ds(pl.multiple_of(base, block), block)
            value = lax.dot_general(
                left[rows, :], weights[chunk], (((1,), (1,)), ((), ())),
                preferred_element_type=jnp.float32,
            )
            into = pl.ds(pl.multiple_of(group * half_rows, half_rows), half_rows)
            part[chunk, 0, into, :] = value[:half_rows]
            part[chunk, 1, into, :] = value[half_rows:]
        else:
            def rows_at(index, carry):
                rows = pl.ds(pl.multiple_of(base + index * block, block), block)
                value = lax.dot_general(
                    left[rows, :], weights[chunk], (((1,), (1,)), ((), ())),
                    preferred_element_type=jnp.float32,
                )
                start = group * half_rows + index % (half_rows // block) * block
                into = pl.ds(pl.multiple_of(start, block), block)
                part[chunk, index // (half_rows // block), into, :] = value
                return carry

            lax.fori_loop(0, CORES * half_rows // block, rows_at, 0)
        pair(group, chunk).start()

    def join(group, chunk):
        pair(group, chunk).wait_recv()
        rows = pl.ds(pl.multiple_of(group * half_rows, half_rows), half_rows)
        part[chunk, core, rows, :] += got[chunk, rows, :]

    tables = []
    for way in range(2):
        far_first = (list(range(last, 0, -1)), list(range(last)))[way]
        tables.append(
            [
                order_of(far_first, range(group * share, (group + 1) * share))
                for group in range(groups)
            ]
        )

    def across(step, chunk):
        peer = lax.rem(me + step, tiles)
        return pltpu.make_async_remote_copy(
            src_ref=fin.at[chunk, peer],
            dst_ref=side.at[chunk, step - 1],
            send_sem=side_send.at[step - 1, chunk],
            recv_sem=side_recv.at[step - 1, chunk],
            device_id={"rng": peer},
            device_id_type=MESH,
        )

    def place(source, chunk, value):
        start = pl.multiple_of(source * (chunks * width) + chunk * width, width)
        out_ref[0, :, pl.ds(start, width)] = value[:lines]
        out_ref[1, :, pl.ds(start, width)] = value[lines:]

    def finish(chunk):
        @pl.when(chip > 0)
        def _():
            collect(0, chip, chunk)

        @pl.when(chip < last)
        def _():
            collect(1, chip, chunk)

        for tile in range(tiles):
            rows = pl.ds(pl.multiple_of(chip * count + tile * 2 * lines, 2 * lines), 2 * lines)
            fin[chunk, tile] = part[chunk, core, rows, :]
        for step in range(1, tiles):
            across(step, chunk).start()
        place(me, chunk, fin[chunk, me])

    begins = []
    for way in range(2):
        begins.append(
            [
                [
                    row.index(target) * chunks + (target, last - target)[way] * LAG if target in row else 0
                    for target in range(chips)
                ]
                for row in tables[way]
            ]
        )
    mine = me if groups > 1 else 0
    begin = jnp.maximum(pick(begins[0], mine, chip), pick(begins[1], mine, chip))

    def stream(time):
        for way in range(2):
            hops = (chip, last - chip)[way]
            at = time - hops * LAG
            target = pick(tables[way], mine, at // chunks)
            ahead = (chip < target, chip > target)[way]
            ready = jnp.logical_and(at >= 0, at < last * chunks)

            @pl.when(jnp.logical_and(ready, ahead))
            def _():
                pass_on(way, target, at % chunks, hops == 0)

        done = time - begin

        @pl.when(jnp.logical_and(done >= 0, done < chunks))
        def _():
            finish(done)

    def steps(group, turn):
        def one(chunk, carry):
            multiply(group, chunk, turn == 0)

            @pl.when(chunk > 0)
            def _():
                join(group, chunk - 1)
                stream(turn * chunks + chunk - 1)

            return carry

        lax.fori_loop(0, chunks, one, 0)
        join(group, chunks - 1)
        stream(turn * chunks + chunks - 1)

    if groups > 1:
        @pl.when(me > 0)
        def _():
            edge().wait_recv()

        interpolate(me, from_edge)
        steps(me, 0)
        for step, copy in enumerate(copies):
            source = lax.rem(me + tiles - 1 - step, tiles)
            copy.wait_recv()
        for step, copy in enumerate(copies):
            source = lax.rem(me + tiles - 1 - step, tiles)
            interpolate(source, from_tile(source))
            steps(source, 1 + step)
    else:
        for copy in copies:
            copy.wait_recv()

        def each(tile, carry):
            interpolate(tile, from_tile(tile))
            return carry

        lax.fori_loop(0, tiles, each, 0)
        steps(0, 0)

    def rest(time, carry):
        stream(time)
        return carry

    lax.fori_loop(groups * chunks, last * chunks + last * LAG, rest, 0)

    def arrive(chunk, carry):
        for step in range(1, tiles):
            across(step, chunk).wait()
            place(lax.rem(me + tiles - step, tiles), chunk, side[chunk, step - 1])
        for group in range(groups):
            pair(group, chunk).wait_send()
        for way in range(2):
            for target in range(chips):
                ahead = (chip < target, chip > target)[way]

                @pl.when(ahead)
                def _():
                    line(way, target, chunk).wait_send()

        return carry

    lax.fori_loop(0, chunks, arrive, 0)
    for copy in copies:
        copy.wait_send()
    if groups > 1:
        @pl.when(me < tiles - 1)
        def _():
            edge().wait_send()


def lines_image(echo, steer, offsets, taps):
    tiles = lax.axis_size("rng")
    chips = lax.axis_size("ping") // CORES
    pings, columns = echo.shape[1:]
    cells = steer.shape[1]
    width = 512 if cells % 4096 == 0 else 256
    chunks = cells // width
    lines = columns // (chips * CORES)
    count = tiles * 2 * lines
    rows = chips * count
    groups = tiles if chips % tiles == 0 else 1
    vmem = pl.BlockSpec(memory_space=pltpu.VMEM)
    smem = pl.BlockSpec(memory_space=pltpu.SMEM)
    anywhere = pl.BlockSpec(memory_space=pl.ANY)
    dma = pltpu.SemaphoreType.DMA
    message = (width // 128 * count + 16, 128)
    others = max(tiles - 1, 1)
    return pl.pallas_call(
        functools.partial(image_kernel, (tiles, chips, chunks, width, lines, groups)),
        out_shape=jax.ShapeDtypeStruct((2, lines, tiles * cells), jnp.float32),
        in_specs=[smem, anywhere, vmem, anywhere],
        out_specs=vmem,
        scratch_shapes=[
            pltpu.SMEM(taps.shape[::-1], jnp.float32),
            pltpu.VMEM((tiles, 2, pings, columns), jnp.bfloat16),
            pltpu.VMEM((2, EDGE, pings), jnp.bfloat16),
            pltpu.VMEM((2, EDGE, pings), jnp.bfloat16),
            pltpu.VMEM((CORES * rows, 2 * pings), jnp.bfloat16),
            pltpu.VMEM((chunks, width, 2 * pings), jnp.bfloat16),
            pltpu.VMEM((chunks, CORES, rows, width), jnp.float32),
            pltpu.VMEM((chunks, rows, width), jnp.float32),
            pltpu.VMEM((2, chips, chunks) + message, jnp.int16),
            pltpu.VMEM((2, chips, chunks) + message, jnp.int16),
            pltpu.VMEM((chunks, tiles, 2 * lines, width), jnp.float32),
            pltpu.VMEM((chunks, others, 2 * lines, width), jnp.float32),
            dma,
            dma,
            dma,
            dma,
            dma((others,)),
            dma((others,)),
            dma((chunks, 2)),
            dma((groups, chunks)),
            dma((groups, chunks)),
            dma((2, chips, chunks)),
            dma((2, chips, chunks)),
            dma((others, chunks)),
            dma((others, chunks)),
        ],
        compiler_params=pltpu.CompilerParams(
            collective_id=0, has_side_effects=True, vmem_limit_bytes=60 * 2**20
        ),
    )(offsets, taps.T, echo, steer)


LANES = 128
BATCH = 4


def split(value):
    high = value.astype(jnp.bfloat16)
    return high, (value - high.astype(jnp.float32)).astype(jnp.bfloat16)


def exact_dot(left, right):
    total = None
    for _ in range(3):
        piece = right.astype(jnp.bfloat16)
        term = jnp.dot(left, piece, preferred_element_type=jnp.float32)
        total = term if total is None else total + term
        right = right - piece.astype(jnp.float32)
    return total


def dot_exact(left, right):
    total = None
    for _ in range(3):
        piece = left.astype(jnp.bfloat16)
        term = jnp.dot(piece, right, preferred_element_type=jnp.float32)
        total = term if total is None else total + term
        left = left - piece.astype(jnp.float32)
    return total


def stacked(value, axis):
    top, low = split(value)
    return jnp.concatenate([top, low, top], axis=axis)


def spectrum_of(fields, down_ref, over_ref, twist_ref):
    size = len(fields)
    high = fields[0].shape[0] // 2
    first = jnp.dot(
        down_ref[...], stacked(jnp.concatenate(fields, axis=1), 0), preferred_element_type=jnp.float32
    )
    rows = []
    for one in range(size):
        real = first[:high, one * LANES:(one + 1) * LANES]
        imag = first[high:, one * LANES:(one + 1) * LANES]
        rows.append(
            jnp.concatenate(
                [
                    real * twist_ref[0] + imag * twist_ref[1],
                    imag * twist_ref[0] - real * twist_ref[1],
                ],
                axis=1,
            )
        )
    return jnp.dot(
        stacked(jnp.concatenate(rows, axis=0), 1), over_ref[...], preferred_element_type=jnp.float32
    )


def gradient_kernel(
    count, tiles, centers_ref, halves_ref, down_ref, over_ref, twist_ref, image_ref, total_ref, spec_ref,
    grid, value, held, full, turned, send_sem, recv_sem, send_two, recv_two,
):
    me = lax.axis_index("ping") * tiles + lax.axis_index("rng")
    ids = [lax.rem(me + step, count) for step in range(1, count)]
    peers = [{"ping": lax.div(one, tiles), "rng": lax.rem(one, tiles)} for one in ids]
    barrier = pltpu.get_barrier_semaphore()
    for peer in peers:
        pl.semaphore_signal(barrier, inc=1, device_id=peer, device_id_type=MESH)

    lines, length = image_ref.shape[1:]
    high = length // LANES
    for half in range(2):
        for row in range(high):
            grid[pl.ds(half * high + row, lines, stride=2 * high), :] = image_ref[
                half, :, row * LANES:(row + 1) * LANES
            ]

    cells = lax.broadcasted_iota(jnp.int32, (high, LANES), 0) * LANES
    cells = cells + lax.broadcasted_iota(jnp.int32, (high, LANES), 1)
    bottom = lax.broadcasted_iota(jnp.int32, (8, LANES), 0) == 7
    lane = lax.broadcasted_iota(jnp.int32, (8, LANES), 1)
    angle = jnp.zeros((8, LANES), jnp.float32)
    for line in range(lines):
        angle = jnp.where(lane == line, centers_ref[line].astype(jnp.float32), angle)
    angle = angle * (2.0 * math.pi / length)
    turned[0] = jnp.cos(angle)
    turned[1] = jnp.sin(angle)

    def after(part):
        moved = pltpu.roll(part, high - 1, axis=0)
        end = moved[high - 8:]
        end = jnp.where(bottom, pltpu.roll(end, LANES - 1, axis=1), end)
        return jnp.concatenate([moved[:high - 8], end], axis=0)

    def field(line):
        return grid[pl.ds(pl.multiple_of(line * 2 * high, 2 * high), 2 * high), :]

    def windowed(index, carry):
        numer, denom = carry
        chosen = []
        for inner in range(BATCH):
            line = index * BATCH + inner
            distance = cells - centers_ref[line]
            distance = jnp.where(distance < 0, distance + length, distance)
            distance = jnp.minimum(distance, length - distance)
            inside = (distance <= halves_ref[line]).astype(jnp.float32)
            chosen.append(field(line) * jnp.concatenate([inside, inside], axis=0))
        found = spectrum_of(chosen, down_ref, over_ref, twist_ref)
        for inner in range(BATCH):
            real = found[inner * high:(inner + 1) * high, :LANES]
            imag = found[inner * high:(inner + 1) * high, LANES:]
            next_real = after(real)
            next_imag = after(imag)
            here = lane == index * BATCH + inner
            cos = jnp.sum(jnp.where(here, turned[0], 0.0), axis=1, keepdims=True)[:1]
            sin = jnp.sum(jnp.where(here, turned[1], 0.0), axis=1, keepdims=True)[:1]
            numer = numer + (real * next_real + imag * next_imag) * sin
            numer = numer + (real * next_imag - imag * next_real) * cos
            denom = denom + (real * real + imag * imag)
        return numer, denom

    zero = jnp.zeros((high, LANES), jnp.float32)
    numer, denom = lax.fori_loop(0, lines // BATCH, windowed, (zero, zero))
    each = value.shape[1]
    for block in range(count // 2):
        value[block] = numer[block * each:(block + 1) * each]
        value[count // 2 + block] = denom[block * each:(block + 1) * each]

    pl.semaphore_wait(barrier, len(peers))
    copies = []
    for step, peer in enumerate(peers):
        copy = pltpu.make_async_remote_copy(
            src_ref=value.at[ids[step]],
            dst_ref=held.at[step],
            send_sem=send_sem.at[step],
            recv_sem=recv_sem.at[step],
            device_id=peer,
            device_id_type=MESH,
        )
        copy.start()
        copies.append(copy)

    def whole(index, carry):
        found = spectrum_of(
            [field(index * BATCH + inner) for inner in range(BATCH)], down_ref, over_ref, twist_ref
        )
        spec_ref[pl.ds(pl.multiple_of(index * BATCH * high, BATCH * high), BATCH * high), :] = found
        return carry

    lax.fori_loop(0, lines // BATCH, whole, 0)
    total = value[me]
    for step, copy in enumerate(copies):
        copy.wait()
        total = total + held[step]
    full[me] = total
    copies = []
    for step, peer in enumerate(peers):
        copy = pltpu.make_async_remote_copy(
            src_ref=full.at[me],
            dst_ref=full.at[me],
            send_sem=send_two.at[step],
            recv_sem=recv_two.at[step],
            device_id=peer,
            device_id_type=MESH,
        )
        copy.start()
        copies.append(copy)
    for copy in copies:
        copy.wait()
    for block in range(count):
        total_ref[block * each:(block + 1) * each, :] = full[block]


def correct_kernel(
    up_ref, back_ref, twist_ref, total_ref, spec_ref, out_ref, phase_ref, grid, turn, tall,
):
    group = out_ref.shape[1]
    length = out_ref.shape[2]
    high = length // LANES

    @pl.when(pl.program_id(0) == 0)
    def _():
        slope = total_ref[:high] / (total_ref[high:] + epsilon)
        row = lax.broadcasted_iota(jnp.int32, (high, high), 0)
        below = (lax.broadcasted_iota(jnp.int32, (high, high), 1) < row).astype(jnp.float32)
        row = lax.broadcasted_iota(jnp.int32, (LANES, LANES), 0)
        ahead = (row < lax.broadcasted_iota(jnp.int32, (LANES, LANES), 1)).astype(jnp.float32)
        within = exact_dot(below.astype(jnp.bfloat16), slope)
        sums = jnp.broadcast_to(jnp.sum(slope, axis=0, keepdims=True), (8, LANES))
        across = dot_exact(sums, ahead.astype(jnp.bfloat16))
        mean = jnp.sum(sums[:1], axis=1, keepdims=True) / length
        order = lax.broadcasted_iota(jnp.int32, (high, LANES), 0)
        order = order + high * lax.broadcasted_iota(jnp.int32, (high, LANES), 1)
        phase = within + across[:1] - order.astype(jnp.float32) * mean
        ratio = LANES // high
        tall[:, :high] = phase.T
        phase_ref[...] = jnp.concatenate(
            [tall[pl.ds(part, LANES // ratio, stride=ratio), :high] for part in range(ratio)], axis=1
        )
        turn[0] = jnp.cos(phase)
        turn[1] = jnp.sin(phase)

    cos = turn[0]
    sin = turn[1]
    start = pl.program_id(0) * group * high
    rows = []
    for line in range(group):
        at = pl.ds(pl.multiple_of(start + line * high, high), high)
        real = spec_ref[at, :LANES]
        imag = spec_ref[at, LANES:]
        rows.append(jnp.concatenate([real * cos + imag * sin, imag * cos - real * sin], axis=1))
    first = jnp.dot(
        stacked(jnp.concatenate(rows, axis=0), 1), back_ref[...], preferred_element_type=jnp.float32
    )
    fields = []
    for line in range(group):
        real = first[line * high:(line + 1) * high, :LANES]
        imag = first[line * high:(line + 1) * high, LANES:]
        fields.append(
            jnp.concatenate(
                [
                    real * twist_ref[2] - imag * twist_ref[3],
                    real * twist_ref[3] + imag * twist_ref[2],
                ],
                axis=0,
            )
        )
    second = jnp.dot(
        up_ref[...], stacked(jnp.concatenate(fields, axis=1), 0), preferred_element_type=jnp.float32
    )
    for line in range(group):
        grid[line * 2 * high:(line + 1) * 2 * high, :] = second[:, line * LANES:(line + 1) * LANES]
    for half in range(2):
        for row in range(high):
            out_ref[half, :, row * LANES:(row + 1) * LANES] = grid[
                pl.ds(half * high + row, group, stride=2 * high), :
            ]


def waves(size, modulus, columns):
    angle = 2.0 * np.pi / modulus * (np.outer(np.arange(size), np.arange(columns)) % modulus)
    return np.cos(angle), np.sin(angle)


def pieces_of(matrix, axis):
    high = matrix.astype(jnp.bfloat16)
    low = (matrix - high.astype(np.float64)).astype(jnp.bfloat16)
    return np.concatenate([high, high, low], axis=axis)


def focus(image, centers, halves):
    pings, tiles = lax.axis_size("ping"), lax.axis_size("rng")
    count = pings * tiles
    lines, length = image.shape[1:]
    high = length // LANES
    cos, sin = waves(high, high, high)
    down = pieces_of(np.block([[cos, sin], [-sin, cos]]), 1)
    up = pieces_of(np.block([[cos, -sin], [sin, cos]]), 1)
    cos, sin = waves(LANES, LANES, LANES)
    over = pieces_of(np.block([[cos, -sin], [sin, cos]]), 0)
    back = pieces_of(np.block([[cos, sin], [-sin, cos]]), 0)
    cos, sin = waves(high, length, LANES)
    twist = np.stack([cos, sin, cos / length, sin / length]).astype(np.float32)
    each = 2 * high // count
    group = 8
    vmem = pl.BlockSpec(memory_space=pltpu.VMEM)
    smem = pl.BlockSpec(memory_space=pltpu.SMEM)
    semaphores = pltpu.SemaphoreType.DMA((count - 1,))
    total, spec = pl.pallas_call(
        functools.partial(gradient_kernel, count, tiles),
        out_shape=(
            jax.ShapeDtypeStruct((2 * high, LANES), jnp.float32),
            jax.ShapeDtypeStruct((lines * high, 2 * LANES), jnp.float32),
        ),
        in_specs=[smem, smem] + [vmem] * 4,
        out_specs=(vmem, vmem),
        scratch_shapes=[
            pltpu.VMEM((lines * 2 * high, LANES), jnp.float32),
            pltpu.VMEM((count, each, LANES), jnp.float32),
            pltpu.VMEM((count - 1, each, LANES), jnp.float32),
            pltpu.VMEM((count, each, LANES), jnp.float32),
            pltpu.VMEM((2, 8, LANES), jnp.float32),
            semaphores,
            semaphores,
            semaphores,
            semaphores,
        ],
        compiler_params=pltpu.CompilerParams(collective_id=1, has_side_effects=True),
    )(centers, halves, down, over, twist, image)
    focused, phase = pl.pallas_call(
        correct_kernel,
        grid=(lines // group,),
        out_shape=(
            jax.ShapeDtypeStruct((2, lines, length), jnp.float32),
            jax.ShapeDtypeStruct((high, LANES), jnp.float32),
        ),
        in_specs=[vmem] * 5,
        out_specs=(
            pl.BlockSpec((2, group, length), lambda index: (0, index, 0)),
            pl.BlockSpec((high, LANES), lambda index: (0, 0)),
        ),
        scratch_shapes=[
            pltpu.VMEM((group * 2 * high, LANES), jnp.float32),
            pltpu.VMEM((2, high, LANES), jnp.float32),
            pltpu.VMEM((LANES, LANES), jnp.float32),
        ],
    )(up, back, twist, total, spec)
    return focused, phase.reshape(length)


def on_device(echo, steer, offsets, taps, centers, halves):
    image = lines_image(echo, steer, offsets, taps)
    return focus(image, centers, halves)


def solution(mesh):
    in_specs = (
        P(None, ("leg", "ping"), "rng"),
        P(None, ("leg", "rng"), "ping"),
        P(("leg", "ping")),
        P(("leg", "ping"), None),
        P(("leg", "ping", "rng")),
        P(("leg", "ping", "rng")),
    )
    out_specs = (P(None, ("leg", "ping", "rng"), None), P("leg"))
    return jax.shard_map(
        on_device, mesh=mesh, in_specs=in_specs, out_specs=out_specs, check_vma=False
    )
```

```python
import functools
import math

import jax
import jax.numpy as jnp
import numpy as np
from jax import lax
from jax.experimental import pallas as pl
from jax.experimental.pallas import tpu as pltpu
from jax.sharding import PartitionSpec as P

PBLK = 64
NTAP = 4


epsilon = 1e-06


MESH = pl.DeviceIdType.MESH


CORES = 2
LAG = 3
EDGE = 32


def encode(value, target, scales):
    count, width = value.shape
    peak = jnp.max(jnp.abs(value), axis=1, keepdims=True)
    power = jnp.floor(jnp.log2(jnp.maximum(peak, 1e-30)) + 1.01)
    whole = jnp.round(value * jnp.exp2(15.0 - power)).astype(jnp.int32).astype(jnp.int16)
    for piece in range(width // 128):
        target[piece * count:(piece + 1) * count, :] = whole[:, piece * 128:(piece + 1) * 128]
    size = min(count, 128)
    lane = lax.broadcasted_iota(jnp.int32, (size, 128), 1)
    here = lane == lax.broadcasted_iota(jnp.int32, (size, 128), 0)
    for piece in range(count // size):
        part = jnp.where(here, power[piece * size:(piece + 1) * size], 0.0)
        scales[piece:piece + 1, :] = jnp.sum(part, axis=0, keepdims=True)


def decode(source, scales, count, width):
    size = min(count, 128)
    lane = lax.broadcasted_iota(jnp.int32, (size, 128), 1)
    here = lane == lax.broadcasted_iota(jnp.int32, (size, 128), 0)
    powers = [
        jnp.sum(jnp.where(here, scales[piece:piece + 1, :], 0.0), axis=1, keepdims=True)
        for piece in range(count // size)
    ]
    scale = jnp.exp2(jnp.concatenate(powers, axis=0) - 15.0)
    pieces = [
        source[piece * count:(piece + 1) * count, :].astype(jnp.int32).astype(jnp.float32) * scale
        for piece in range(width // 128)
    ]
    return jnp.concatenate(pieces, axis=1)


def order_of(targets, own):
    return [one for one in targets if one in own] + [one for one in targets if one not in own]


def pick(table, row, column):
    found = jnp.int32(table[0][0])
    for at_row, entries in enumerate(table):
        for at_column, entry in enumerate(entries):
            here = jnp.logical_and(row == at_row, column == at_column)
            found = jnp.where(here, jnp.int32(entry), found)
    return found


def image_kernel(
    plan, offsets_ref, taps_hbm, echo_ref, steer_ref, out_ref,
    taps_ref, held, edge_out, edge_in, left, weights, part, got, away, near, away_scale, near_scale, fin, side,
    taps_sem, own_sem, edge_send, edge_recv, echo_send, echo_recv, load_sem, pair_send, pair_recv,
    line_send, line_recv, scale_send, scale_recv, side_send, side_recv,
):
    tiles, chips, chunks, width, lines, groups = plan
    pings = echo_ref.shape[1]
    columns = echo_ref.shape[2]
    count = tiles * 2 * lines
    share = chips // groups
    me = lax.axis_index("rng")
    chip = lax.axis_index("ping") // CORES
    core = lax.axis_index("ping") % CORES
    last = chips - 1
    partner = {"ping": chip * CORES + 1 - core}
    above = {"ping": (chip + 1) * CORES + core}
    below = {"ping": (chip - 1) * CORES + core}
    peers = [{"rng": lax.rem(me + step, tiles)} for step in range(1, tiles)]

    barrier = pltpu.get_barrier_semaphore()
    for peer in peers + [partner]:
        pl.semaphore_signal(barrier, inc=1, device_id=peer, device_id_type=MESH)

    @pl.when(chip < last)
    def _():
        pl.semaphore_signal(barrier, inc=1, device_id=above, device_id_type=MESH)

    @pl.when(chip > 0)
    def _():
        pl.semaphore_signal(barrier, inc=1, device_id=below, device_id_type=MESH)

    tap_copy = pltpu.make_async_copy(taps_hbm, taps_ref, taps_sem)
    tap_copy.start()
    own = pltpu.make_async_copy(echo_ref, held.at[me], own_sem)
    own.start()

    def load(chunk, half):
        return pltpu.make_async_copy(
            steer_ref.at[half, pl.ds(chunk * width, width), :],
            weights.at[chunk, :, pl.ds(half * pings, pings)],
            load_sem.at[chunk, half],
        )

    for chunk in range(chunks):
        for half in range(2):
            load(chunk, half).start()

    def edge():
        return pltpu.make_async_remote_copy(
            src_ref=edge_out,
            dst_ref=edge_in,
            send_sem=edge_send,
            recv_sem=edge_recv,
            device_id={"rng": lax.rem(me + 1, tiles)},
            device_id_type=MESH,
        )

    row = lax.broadcasted_iota(jnp.int32, (128, 128), 0)
    unit = (row == lax.broadcasted_iota(jnp.int32, (128, 128), 1)).astype(jnp.float32).astype(jnp.bfloat16)

    def turn(chosen, value):
        return lax.dot_general(
            chosen, value, (((1,), (1,)), ((), ())), preferred_element_type=jnp.float32
        )

    if groups > 1:
        def pack(index, carry):
            cols = pl.ds(pl.multiple_of(index * 128, 128), 128)
            for half in range(2):
                value = turn(unit[columns - EDGE:], echo_ref[half, cols, :])
                edge_out[half, :, cols] = value.astype(jnp.bfloat16)
            return carry

        lax.fori_loop(0, pings // 128, pack, 0)

    reached = len(peers) + 1 + (chip < last).astype(jnp.int32) + (chip > 0).astype(jnp.int32)
    pl.semaphore_wait(barrier, reached)
    if groups > 1:
        @pl.when(me < tiles - 1)
        def _():
            edge().start()

    copies = []
    for step, peer in enumerate(peers):
        copy = pltpu.make_async_remote_copy(
            src_ref=echo_ref,
            dst_ref=held.at[me],
            send_sem=echo_send.at[step],
            recv_sem=echo_recv.at[step],
            device_id=peer,
            device_id_type=MESH,
        )
        copy.start()
        copies.append(copy)
    own.wait()
    tap_copy.wait()
    column = lax.broadcasted_iota(jnp.int32, (PBLK, 2 * columns), 1)

    def interpolate(tile, before):
        def one(index, carry):
            cols = pl.multiple_of(index * 128, 128)
            turned = []
            for half in range(2):
                ahead = before(half, cols)
                value = held[tile, half, pl.ds(cols, 128), :].astype(jnp.float32)
                value = jnp.concatenate([ahead, value], axis=1)
                blocks = []
                for inner in range(128 // PBLK):
                    block = index * (128 // PBLK) + inner
                    piece = value[inner * PBLK:(inner + 1) * PBLK]
                    offset = offsets_ref[block]
                    result = jnp.zeros((PBLK, columns), jnp.float32)
                    for tap in range(NTAP):
                        moved = pltpu.roll(piece, offset + tap, axis=1)[:, columns:]
                        result = result + taps_ref[tap, block] * moved
                    blocks.append(result)
                turned.append(turn(unit, jnp.concatenate(blocks, axis=0).astype(jnp.bfloat16)).astype(jnp.bfloat16))
            real, imag = turned
            for piece in range(columns // lines):
                row = tile * (columns // lines) + piece
                owner = row // tiles
                target = owner // CORES
                place = (target // share * CORES + owner % CORES) * share + target % share
                place = pl.multiple_of((place * tiles + row % tiles) * 2 * lines, 2 * lines)
                a = real[piece * lines:(piece + 1) * lines]
                b = imag[piece * lines:(piece + 1) * lines]
                left[pl.ds(place, lines), pl.ds(cols, 128)] = a
                left[pl.ds(place + lines, lines), pl.ds(cols, 128)] = b
                left[pl.ds(place, lines), pl.ds(pings + cols, 128)] = -b
                left[pl.ds(place + lines, lines), pl.ds(pings + cols, 128)] = a
            return carry

        lax.fori_loop(0, pings // 128, one, 0, unroll=2)

    def from_edge(half, cols):
        value = edge_in[half, :, pl.ds(cols, 128)].astype(jnp.float32)
        value = jnp.where(me > 0, value, 0.0).astype(jnp.bfloat16)
        value = jnp.concatenate([jnp.zeros((columns - EDGE, 128), jnp.bfloat16), value], axis=0)
        return turn(unit, value)

    def from_tile(tile):
        def before(half, cols):
            value = held[lax.max(tile - 1, 0), half, pl.ds(cols, 128), :].astype(jnp.float32)
            return jnp.where(tile > 0, value, 0.0)

        return before

    def pair(group, chunk):
        rows = pl.ds(pl.multiple_of(group * share * count, share * count), share * count)
        return pltpu.make_async_remote_copy(
            src_ref=part.at[chunk, 1 - core, rows],
            dst_ref=got.at[chunk, rows],
            send_sem=pair_send.at[group, chunk],
            recv_sem=pair_recv.at[group, chunk],
            device_id=partner,
            device_id_type=MESH,
        )

    def line(way, target, chunk):
        return pltpu.make_async_remote_copy(
            src_ref=away.at[way, target, chunk],
            dst_ref=near.at[way, target, chunk],
            send_sem=line_send.at[way, target, chunk],
            recv_sem=line_recv.at[way, target, chunk],
            device_id=(above, below)[way],
            device_id_type=MESH,
        )

    def scale_line(way, target, chunk):
        return pltpu.make_async_remote_copy(
            src_ref=away_scale.at[way, target, chunk],
            dst_ref=near_scale.at[way, target, chunk],
            send_sem=scale_send.at[way, target, chunk],
            recv_sem=scale_recv.at[way, target, chunk],
            device_id=(above, below)[way],
            device_id_type=MESH,
        )

    def rows_of(target):
        return pl.ds(pl.multiple_of(target * count, count), count)

    def collect(way, target, chunk):
        scale_line(way, target, chunk).wait_recv()
        line(way, target, chunk).wait_recv()
        part[chunk, core, rows_of(target), :] += decode(
            near.at[way, target, chunk], near_scale.at[way, target, chunk], count, width
        )

    def pass_on(way, target, chunk, first):
        @pl.when(jnp.logical_not(first))
        def _():
            collect(way, target, chunk)

        encode(
            part[chunk, core, rows_of(target), :], away.at[way, target, chunk], away_scale.at[way, target, chunk]
        )
        scale_line(way, target, chunk).start()
        line(way, target, chunk).start()

    half_rows = share * count
    block = min(512, CORES * half_rows)

    def multiply(group, chunk, first):
        if first:
            for half in range(2):
                load(chunk, half).wait()
        base = group * CORES * half_rows
        if block == CORES * half_rows:
            rows = pl.ds(pl.multiple_of(base, block), block)
            value = lax.dot_general(
                left[rows, :], weights[chunk], (((1,), (1,)), ((), ())),
                preferred_element_type=jnp.float32,
            )
            into = pl.ds(pl.multiple_of(group * half_rows, half_rows), half_rows)
            part[chunk, 0, into, :] = value[:half_rows]
            part[chunk, 1, into, :] = value[half_rows:]
        else:
            def rows_at(index, carry):
                rows = pl.ds(pl.multiple_of(base + index * block, block), block)
                value = lax.dot_general(
                    left[rows, :], weights[chunk], (((1,), (1,)), ((), ())),
                    preferred_element_type=jnp.float32,
                )
                start = group * half_rows + index % (half_rows // block) * block
                into = pl.ds(pl.multiple_of(start, block), block)
                part[chunk, index // (half_rows // block), into, :] = value
                return carry

            lax.fori_loop(0, CORES * half_rows // block, rows_at, 0)
        pair(group, chunk).start()

    def join(group, chunk):
        pair(group, chunk).wait_recv()
        rows = pl.ds(pl.multiple_of(group * half_rows, half_rows), half_rows)
        part[chunk, core, rows, :] += got[chunk, rows, :]

    tables = []
    for way in range(2):
        far_first = (list(range(last, 0, -1)), list(range(last)))[way]
        tables.append(
            [
                order_of(far_first, range(group * share, (group + 1) * share))
                for group in range(groups)
            ]
        )

    def across(step, chunk):
        peer = lax.rem(me + step, tiles)
        return pltpu.make_async_remote_copy(
            src_ref=fin.at[chunk, peer],
            dst_ref=side.at[chunk, step - 1],
            send_sem=side_send.at[step - 1, chunk],
            recv_sem=side_recv.at[step - 1, chunk],
            device_id={"rng": peer},
            device_id_type=MESH,
        )

    def place(source, chunk, value):
        start = pl.multiple_of(source * (chunks * width) + chunk * width, width)
        out_ref[0, :, pl.ds(start, width)] = value[:lines]
        out_ref[1, :, pl.ds(start, width)] = value[lines:]

    def finish(chunk):
        @pl.when(chip > 0)
        def _():
            collect(0, chip, chunk)

        @pl.when(chip < last)
        def _():
            collect(1, chip, chunk)

        for tile in range(tiles):
            rows = pl.ds(pl.multiple_of(chip * count + tile * 2 * lines, 2 * lines), 2 * lines)
            fin[chunk, tile] = part[chunk, core, rows, :]
        for step in range(1, tiles):
            across(step, chunk).start()
        place(me, chunk, fin[chunk, me])

    begins = []
    for way in range(2):
        begins.append(
            [
                [
                    row.index(target) * chunks + (target, last - target)[way] * LAG if target in row else 0
                    for target in range(chips)
                ]
                for row in tables[way]
            ]
        )
    mine = me if groups > 1 else 0
    begin = jnp.maximum(pick(begins[0], mine, chip), pick(begins[1], mine, chip))

    def stream(time):
        for way in range(2):
            hops = (chip, last - chip)[way]
            at = time - hops * LAG
            target = pick(tables[way], mine, at // chunks)
            ahead = (chip < target, chip > target)[way]
            ready = jnp.logical_and(at >= 0, at < last * chunks)

            @pl.when(jnp.logical_and(ready, ahead))
            def _():
                pass_on(way, target, at % chunks, hops == 0)

        done = time - begin

        @pl.when(jnp.logical_and(done >= 0, done < chunks))
        def _():
            finish(done)

    def steps(group, turn):
        def one(chunk, carry):
            multiply(group, chunk, turn == 0)

            @pl.when(chunk > 0)
            def _():
                join(group, chunk - 1)
                stream(turn * chunks + chunk - 1)

            return carry

        lax.fori_loop(0, chunks, one, 0)
        join(group, chunks - 1)
        stream(turn * chunks + chunks - 1)

    if groups > 1:
        @pl.when(me > 0)
        def _():
            edge().wait_recv()

        interpolate(me, from_edge)
        steps(me, 0)
        for step, copy in enumerate(copies):
            source = lax.rem(me + tiles - 1 - step, tiles)
            copy.wait_recv()
        for step, copy in enumerate(copies):
            source = lax.rem(me + tiles - 1 - step, tiles)
            interpolate(source, from_tile(source))
            steps(source, 1 + step)
    else:
        for copy in copies:
            copy.wait_recv()

        def each(tile, carry):
            interpolate(tile, from_tile(tile))
            return carry

        lax.fori_loop(0, tiles, each, 0)
        steps(0, 0)

    def rest(time, carry):
        stream(time)
        return carry

    lax.fori_loop(groups * chunks, last * chunks + last * LAG, rest, 0)

    def arrive(chunk, carry):
        for step in range(1, tiles):
            across(step, chunk).wait()
            place(lax.rem(me + tiles - step, tiles), chunk, side[chunk, step - 1])
        for group in range(groups):
            pair(group, chunk).wait_send()
        for way in range(2):
            for target in range(chips):
                ahead = (chip < target, chip > target)[way]

                @pl.when(ahead)
                def _():
                    line(way, target, chunk).wait_send()
                    scale_line(way, target, chunk).wait_send()

        return carry

    lax.fori_loop(0, chunks, arrive, 0)
    for copy in copies:
        copy.wait_send()
    if groups > 1:
        @pl.when(me < tiles - 1)
        def _():
            edge().wait_send()


def lines_image(echo, steer, offsets, taps):
    tiles = lax.axis_size("rng")
    chips = lax.axis_size("ping") // CORES
    pings, columns = echo.shape[1:]
    cells = steer.shape[1]
    width = 512 if cells % 4096 == 0 else 256
    chunks = cells // width
    lines = columns // (chips * CORES)
    count = tiles * 2 * lines
    rows = chips * count
    groups = tiles if chips % tiles == 0 else 1
    vmem = pl.BlockSpec(memory_space=pltpu.VMEM)
    smem = pl.BlockSpec(memory_space=pltpu.SMEM)
    anywhere = pl.BlockSpec(memory_space=pl.ANY)
    dma = pltpu.SemaphoreType.DMA
    message = (width // 128 * count, 128)
    scales = (max(count // 128, 1), 128)
    others = max(tiles - 1, 1)
    return pl.pallas_call(
        functools.partial(image_kernel, (tiles, chips, chunks, width, lines, groups)),
        out_shape=jax.ShapeDtypeStruct((2, lines, tiles * cells), jnp.float32),
        in_specs=[smem, anywhere, vmem, anywhere],
        out_specs=vmem,
        scratch_shapes=[
            pltpu.SMEM(taps.shape[::-1], jnp.float32),
            pltpu.VMEM((tiles, 2, pings, columns), jnp.bfloat16),
            pltpu.VMEM((2, EDGE, pings), jnp.bfloat16),
            pltpu.VMEM((2, EDGE, pings), jnp.bfloat16),
            pltpu.VMEM((CORES * rows, 2 * pings), jnp.bfloat16),
            pltpu.VMEM((chunks, width, 2 * pings), jnp.bfloat16),
            pltpu.VMEM((chunks, CORES, rows, width), jnp.float32),
            pltpu.VMEM((chunks, rows, width), jnp.float32),
            pltpu.VMEM((2, chips, chunks) + message, jnp.int16),
            pltpu.VMEM((2, chips, chunks) + message, jnp.int16),
            pltpu.VMEM((2, chips, chunks) + scales, jnp.float32),
            pltpu.VMEM((2, chips, chunks) + scales, jnp.float32),
            pltpu.VMEM((chunks, tiles, 2 * lines, width), jnp.float32),
            pltpu.VMEM((chunks, others, 2 * lines, width), jnp.float32),
            dma,
            dma,
            dma,
            dma,
            dma((others,)),
            dma((others,)),
            dma((chunks, 2)),
            dma((groups, chunks)),
            dma((groups, chunks)),
            dma((2, chips, chunks)),
            dma((2, chips, chunks)),
            dma((2, chips, chunks)),
            dma((2, chips, chunks)),
            dma((others, chunks)),
            dma((others, chunks)),
        ],
        compiler_params=pltpu.CompilerParams(
            collective_id=0, has_side_effects=True, vmem_limit_bytes=60 * 2**20
        ),
    )(offsets, taps.T, echo, steer)


LANES = 128
BATCH = 4


def split(value):
    high = value.astype(jnp.bfloat16)
    return high, (value - high.astype(jnp.float32)).astype(jnp.bfloat16)


def exact_dot(left, right):
    total = None
    for _ in range(3):
        piece = right.astype(jnp.bfloat16)
        term = jnp.dot(left, piece, preferred_element_type=jnp.float32)
        total = term if total is None else total + term
        right = right - piece.astype(jnp.float32)
    return total


def dot_exact(left, right):
    total = None
    for _ in range(3):
        piece = left.astype(jnp.bfloat16)
        term = jnp.dot(piece, right, preferred_element_type=jnp.float32)
        total = term if total is None else total + term
        left = left - piece.astype(jnp.float32)
    return total


def stacked(value, axis):
    top, low = split(value)
    return jnp.concatenate([top, low, top], axis=axis)


def spectrum_of(fields, down_ref, over_ref, twist_ref):
    size = len(fields)
    high = fields[0].shape[0] // 2
    first = jnp.dot(
        down_ref[...], stacked(jnp.concatenate(fields, axis=1), 0), preferred_element_type=jnp.float32
    )
    rows = []
    for one in range(size):
        real = first[:high, one * LANES:(one + 1) * LANES]
        imag = first[high:, one * LANES:(one + 1) * LANES]
        rows.append(
            jnp.concatenate(
                [
                    real * twist_ref[0] + imag * twist_ref[1],
                    imag * twist_ref[0] - real * twist_ref[1],
                ],
                axis=1,
            )
        )
    return jnp.dot(
        stacked(jnp.concatenate(rows, axis=0), 1), over_ref[...], preferred_element_type=jnp.float32
    )


def gradient_kernel(
    count, tiles, centers_ref, halves_ref, down_ref, over_ref, twist_ref, image_ref, total_ref, spec_ref,
    grid, value, held, full, turned, send_sem, recv_sem, send_two, recv_two,
):
    me = lax.axis_index("ping") * tiles + lax.axis_index("rng")
    ids = [lax.rem(me + step, count) for step in range(1, count)]
    peers = [{"ping": lax.div(one, tiles), "rng": lax.rem(one, tiles)} for one in ids]
    barrier = pltpu.get_barrier_semaphore()
    for peer in peers:
        pl.semaphore_signal(barrier, inc=1, device_id=peer, device_id_type=MESH)

    lines, length = image_ref.shape[1:]
    high = length // LANES
    for half in range(2):
        for row in range(high):
            grid[pl.ds(half * high + row, lines, stride=2 * high), :] = image_ref[
                half, :, row * LANES:(row + 1) * LANES
            ]

    cells = lax.broadcasted_iota(jnp.int32, (high, LANES), 0) * LANES
    cells = cells + lax.broadcasted_iota(jnp.int32, (high, LANES), 1)
    bottom = lax.broadcasted_iota(jnp.int32, (8, LANES), 0) == 7
    lane = lax.broadcasted_iota(jnp.int32, (8, LANES), 1)
    angle = jnp.zeros((8, LANES), jnp.float32)
    for line in range(lines):
        angle = jnp.where(lane == line, centers_ref[line].astype(jnp.float32), angle)
    angle = angle * (2.0 * math.pi / length)
    turned[0] = jnp.cos(angle)
    turned[1] = jnp.sin(angle)

    def after(part):
        moved = pltpu.roll(part, high - 1, axis=0)
        end = moved[high - 8:]
        end = jnp.where(bottom, pltpu.roll(end, LANES - 1, axis=1), end)
        return jnp.concatenate([moved[:high - 8], end], axis=0)

    def field(line):
        return grid[pl.ds(pl.multiple_of(line * 2 * high, 2 * high), 2 * high), :]

    def windowed(index, carry):
        numer, denom = carry
        chosen = []
        for inner in range(BATCH):
            line = index * BATCH + inner
            distance = cells - centers_ref[line]
            distance = jnp.where(distance < 0, distance + length, distance)
            distance = jnp.minimum(distance, length - distance)
            inside = (distance <= halves_ref[line]).astype(jnp.float32)
            chosen.append(field(line) * jnp.concatenate([inside, inside], axis=0))
        found = spectrum_of(chosen, down_ref, over_ref, twist_ref)
        for inner in range(BATCH):
            real = found[inner * high:(inner + 1) * high, :LANES]
            imag = found[inner * high:(inner + 1) * high, LANES:]
            next_real = after(real)
            next_imag = after(imag)
            here = lane == index * BATCH + inner
            cos = jnp.sum(jnp.where(here, turned[0], 0.0), axis=1, keepdims=True)[:1]
            sin = jnp.sum(jnp.where(here, turned[1], 0.0), axis=1, keepdims=True)[:1]
            numer = numer + (real * next_real + imag * next_imag) * sin
            numer = numer + (real * next_imag - imag * next_real) * cos
            denom = denom + (real * real + imag * imag)
        return numer, denom

    zero = jnp.zeros((high, LANES), jnp.float32)
    numer, denom = lax.fori_loop(0, lines // BATCH, windowed, (zero, zero))
    each = value.shape[1]
    for block in range(count // 2):
        value[block] = numer[block * each:(block + 1) * each]
        value[count // 2 + block] = denom[block * each:(block + 1) * each]

    pl.semaphore_wait(barrier, len(peers))
    copies = []
    for step, peer in enumerate(peers):
        copy = pltpu.make_async_remote_copy(
            src_ref=value.at[ids[step]],
            dst_ref=held.at[step],
            send_sem=send_sem.at[step],
            recv_sem=recv_sem.at[step],
            device_id=peer,
            device_id_type=MESH,
        )
        copy.start()
        copies.append(copy)

    def whole(index, carry):
        found = spectrum_of(
            [field(index * BATCH + inner) for inner in range(BATCH)], down_ref, over_ref, twist_ref
        )
        spec_ref[pl.ds(pl.multiple_of(index * BATCH * high, BATCH * high), BATCH * high), :] = found
        return carry

    lax.fori_loop(0, lines // BATCH, whole, 0)
    total = value[me]
    for step, copy in enumerate(copies):
        copy.wait()
        total = total + held[step]
    full[me] = total
    copies = []
    for step, peer in enumerate(peers):
        copy = pltpu.make_async_remote_copy(
            src_ref=full.at[me],
            dst_ref=full.at[me],
            send_sem=send_two.at[step],
            recv_sem=recv_two.at[step],
            device_id=peer,
            device_id_type=MESH,
        )
        copy.start()
        copies.append(copy)
    for copy in copies:
        copy.wait()
    for block in range(count):
        total_ref[block * each:(block + 1) * each, :] = full[block]


def correct_kernel(
    up_ref, back_ref, twist_ref, total_ref, spec_ref, out_ref, phase_ref, grid, turn, tall,
):
    group = out_ref.shape[1]
    length = out_ref.shape[2]
    high = length // LANES

    @pl.when(pl.program_id(0) == 0)
    def _():
        slope = total_ref[:high] / (total_ref[high:] + epsilon)
        row = lax.broadcasted_iota(jnp.int32, (high, high), 0)
        below = (lax.broadcasted_iota(jnp.int32, (high, high), 1) < row).astype(jnp.float32)
        row = lax.broadcasted_iota(jnp.int32, (LANES, LANES), 0)
        ahead = (row < lax.broadcasted_iota(jnp.int32, (LANES, LANES), 1)).astype(jnp.float32)
        within = exact_dot(below.astype(jnp.bfloat16), slope)
        sums = jnp.broadcast_to(jnp.sum(slope, axis=0, keepdims=True), (8, LANES))
        across = dot_exact(sums, ahead.astype(jnp.bfloat16))
        mean = jnp.sum(sums[:1], axis=1, keepdims=True) / length
        order = lax.broadcasted_iota(jnp.int32, (high, LANES), 0)
        order = order + high * lax.broadcasted_iota(jnp.int32, (high, LANES), 1)
        phase = within + across[:1] - order.astype(jnp.float32) * mean
        ratio = LANES // high
        tall[:, :high] = phase.T
        phase_ref[...] = jnp.concatenate(
            [tall[pl.ds(part, LANES // ratio, stride=ratio), :high] for part in range(ratio)], axis=1
        )
        turn[0] = jnp.cos(phase)
        turn[1] = jnp.sin(phase)

    cos = turn[0]
    sin = turn[1]
    start = pl.program_id(0) * group * high
    rows = []
    for line in range(group):
        at = pl.ds(pl.multiple_of(start + line * high, high), high)
        real = spec_ref[at, :LANES]
        imag = spec_ref[at, LANES:]
        rows.append(jnp.concatenate([real * cos + imag * sin, imag * cos - real * sin], axis=1))
    first = jnp.dot(
        stacked(jnp.concatenate(rows, axis=0), 1), back_ref[...], preferred_element_type=jnp.float32
    )
    fields = []
    for line in range(group):
        real = first[line * high:(line + 1) * high, :LANES]
        imag = first[line * high:(line + 1) * high, LANES:]
        fields.append(
            jnp.concatenate(
                [
                    real * twist_ref[2] - imag * twist_ref[3],
                    real * twist_ref[3] + imag * twist_ref[2],
                ],
                axis=0,
            )
        )
    second = jnp.dot(
        up_ref[...], stacked(jnp.concatenate(fields, axis=1), 0), preferred_element_type=jnp.float32
    )
    for line in range(group):
        grid[line * 2 * high:(line + 1) * 2 * high, :] = second[:, line * LANES:(line + 1) * LANES]
    for half in range(2):
        for row in range(high):
            out_ref[half, :, row * LANES:(row + 1) * LANES] = grid[
                pl.ds(half * high + row, group, stride=2 * high), :
            ]


def waves(size, modulus, columns):
    angle = 2.0 * np.pi / modulus * (np.outer(np.arange(size), np.arange(columns)) % modulus)
    return np.cos(angle), np.sin(angle)


def pieces_of(matrix, axis):
    high = matrix.astype(jnp.bfloat16)
    low = (matrix - high.astype(np.float64)).astype(jnp.bfloat16)
    return np.concatenate([high, high, low], axis=axis)


def focus(image, centers, halves):
    pings, tiles = lax.axis_size("ping"), lax.axis_size("rng")
    count = pings * tiles
    lines, length = image.shape[1:]
    high = length // LANES
    cos, sin = waves(high, high, high)
    down = pieces_of(np.block([[cos, sin], [-sin, cos]]), 1)
    up = pieces_of(np.block([[cos, -sin], [sin, cos]]), 1)
    cos, sin = waves(LANES, LANES, LANES)
    over = pieces_of(np.block([[cos, -sin], [sin, cos]]), 0)
    back = pieces_of(np.block([[cos, sin], [-sin, cos]]), 0)
    cos, sin = waves(high, length, LANES)
    twist = np.stack([cos, sin, cos / length, sin / length]).astype(np.float32)
    each = 2 * high // count
    group = 8
    vmem = pl.BlockSpec(memory_space=pltpu.VMEM)
    smem = pl.BlockSpec(memory_space=pltpu.SMEM)
    semaphores = pltpu.SemaphoreType.DMA((count - 1,))
    total, spec = pl.pallas_call(
        functools.partial(gradient_kernel, count, tiles),
        out_shape=(
            jax.ShapeDtypeStruct((2 * high, LANES), jnp.float32),
            jax.ShapeDtypeStruct((lines * high, 2 * LANES), jnp.float32),
        ),
        in_specs=[smem, smem] + [vmem] * 4,
        out_specs=(vmem, vmem),
        scratch_shapes=[
            pltpu.VMEM((lines * 2 * high, LANES), jnp.float32),
            pltpu.VMEM((count, each, LANES), jnp.float32),
            pltpu.VMEM((count - 1, each, LANES), jnp.float32),
            pltpu.VMEM((count, each, LANES), jnp.float32),
            pltpu.VMEM((2, 8, LANES), jnp.float32),
            semaphores,
            semaphores,
            semaphores,
            semaphores,
        ],
        compiler_params=pltpu.CompilerParams(collective_id=1, has_side_effects=True),
    )(centers, halves, down, over, twist, image)
    focused, phase = pl.pallas_call(
        correct_kernel,
        grid=(lines // group,),
        out_shape=(
            jax.ShapeDtypeStruct((2, lines, length), jnp.float32),
            jax.ShapeDtypeStruct((high, LANES), jnp.float32),
        ),
        in_specs=[vmem] * 5,
        out_specs=(
            pl.BlockSpec((2, group, length), lambda index: (0, index, 0)),
            pl.BlockSpec((high, LANES), lambda index: (0, 0)),
        ),
        scratch_shapes=[
            pltpu.VMEM((group * 2 * high, LANES), jnp.float32),
            pltpu.VMEM((2, high, LANES), jnp.float32),
            pltpu.VMEM((LANES, LANES), jnp.float32),
        ],
    )(up, back, twist, total, spec)
    return focused, phase.reshape(length)


def on_device(echo, steer, offsets, taps, centers, halves):
    image = lines_image(echo, steer, offsets, taps)
    return focus(image, centers, halves)


def solution(mesh):
    in_specs = (
        P(None, ("leg", "ping"), "rng"),
        P(None, ("leg", "rng"), "ping"),
        P(("leg", "ping")),
        P(("leg", "ping"), None),
        P(("leg", "ping", "rng")),
        P(("leg", "ping", "rng")),
    )
    out_specs = (P(None, ("leg", "ping", "rng"), None), P("leg"))
    return jax.shard_map(
        on_device, mesh=mesh, in_specs=in_specs, out_specs=out_specs, check_vma=False
    )
```

```python
import functools
import math

import jax
import jax.numpy as jnp
import numpy as np
from jax import lax
from jax.experimental import pallas as pl
from jax.experimental.pallas import tpu as pltpu
from jax.sharding import PartitionSpec as P

PBLK = 64
NTAP = 4


epsilon = 1e-06


MESH = pl.DeviceIdType.MESH


CORES = 2
LAG = 3
EDGE = 32
SPAN = 512


def encode(value, target, scales):
    count, width = value.shape
    peak = jnp.max(jnp.abs(value), axis=1, keepdims=True)
    power = jnp.floor(jnp.log2(jnp.maximum(peak, 1e-30)) + 1.01)
    whole = jnp.round(value * jnp.exp2(15.0 - power)).astype(jnp.int32).astype(jnp.int16)
    for piece in range(width // 128):
        target[piece * count:(piece + 1) * count, :] = whole[:, piece * 128:(piece + 1) * 128]
    size = min(count, 128)
    lane = lax.broadcasted_iota(jnp.int32, (size, 128), 1)
    here = lane == lax.broadcasted_iota(jnp.int32, (size, 128), 0)
    for piece in range(count // size):
        part = jnp.where(here, power[piece * size:(piece + 1) * size], 0.0)
        scales[piece:piece + 1, :] = jnp.sum(part, axis=0, keepdims=True)


def decode(source, scales, count, width):
    size = min(count, 128)
    lane = lax.broadcasted_iota(jnp.int32, (size, 128), 1)
    here = lane == lax.broadcasted_iota(jnp.int32, (size, 128), 0)
    powers = [
        jnp.sum(jnp.where(here, scales[piece:piece + 1, :], 0.0), axis=1, keepdims=True)
        for piece in range(count // size)
    ]
    scale = jnp.exp2(jnp.concatenate(powers, axis=0) - 15.0)
    pieces = [
        source[piece * count:(piece + 1) * count, :].astype(jnp.int32).astype(jnp.float32) * scale
        for piece in range(width // 128)
    ]
    return jnp.concatenate(pieces, axis=1)


def order_of(targets, own):
    return [one for one in targets if one in own] + [one for one in targets if one not in own]


def pick(table, row, column):
    found = jnp.int32(table[0][0])
    for at_row, entries in enumerate(table):
        for at_column, entry in enumerate(entries):
            here = jnp.logical_and(row == at_row, column == at_column)
            found = jnp.where(here, jnp.int32(entry), found)
    return found


def image_kernel(
    plan, offsets_ref, taps_hbm, echo_ref, steer_ref, out_ref,
    taps_ref, held, edge_out, edge_in, prior, flat, left, weights, part, got, away, near, away_scale, near_scale, fin, side,
    taps_sem, own_sem, edge_send, edge_recv, echo_send, echo_recv, load_sem, pair_send, pair_recv,
    line_send, line_recv, scale_send, scale_recv, side_send, side_recv,
):
    tiles, chips, chunks, width, lines, groups = plan
    pings = echo_ref.shape[1]
    columns = echo_ref.shape[2]
    count = tiles * 2 * lines
    share = chips // groups
    me = lax.axis_index("rng")
    chip = lax.axis_index("ping") // CORES
    core = lax.axis_index("ping") % CORES
    last = chips - 1
    partner = {"ping": chip * CORES + 1 - core}
    above = {"ping": (chip + 1) * CORES + core}
    below = {"ping": (chip - 1) * CORES + core}
    peers = [{"rng": lax.rem(me + step, tiles)} for step in range(1, tiles)]

    barrier = pltpu.get_barrier_semaphore()
    for peer in peers + [partner]:
        pl.semaphore_signal(barrier, inc=1, device_id=peer, device_id_type=MESH)

    @pl.when(chip < last)
    def _():
        pl.semaphore_signal(barrier, inc=1, device_id=above, device_id_type=MESH)

    @pl.when(chip > 0)
    def _():
        pl.semaphore_signal(barrier, inc=1, device_id=below, device_id_type=MESH)

    tap_copy = pltpu.make_async_copy(taps_hbm, taps_ref, taps_sem)
    tap_copy.start()
    own = pltpu.make_async_copy(echo_ref, held.at[me], own_sem)
    own.start()

    def load(chunk, half):
        return pltpu.make_async_copy(
            steer_ref.at[half, pl.ds(chunk * width, width), :],
            weights.at[chunk, :, pl.ds(half * pings, pings)],
            load_sem.at[chunk, half],
        )


    def edge():
        return pltpu.make_async_remote_copy(
            src_ref=edge_out,
            dst_ref=edge_in,
            send_sem=edge_send,
            recv_sem=edge_recv,
            device_id={"rng": lax.rem(me + 1, tiles)},
            device_id_type=MESH,
        )

    row = lax.broadcasted_iota(jnp.int32, (128, 128), 0)
    unit = (row == lax.broadcasted_iota(jnp.int32, (128, 128), 1)).astype(jnp.float32).astype(jnp.bfloat16)

    def turn(chosen, value):
        return lax.dot_general(
            chosen, value, (((1,), (1,)), ((), ())), preferred_element_type=jnp.float32
        )

    if groups > 1:
        for half in range(2):
            for start in range(0, pings, SPAN):
                value = turn(unit[columns - EDGE:], echo_ref[half, start:start + SPAN, :])
                edge_out[half, :, start:start + SPAN] = value.astype(jnp.bfloat16)

    reached = len(peers) + 1 + (chip < last).astype(jnp.int32) + (chip > 0).astype(jnp.int32)
    pl.semaphore_wait(barrier, reached)
    if groups > 1:
        @pl.when(me < tiles - 1)
        def _():
            edge().start()

    copies = []
    for step, peer in enumerate(peers):
        copy = pltpu.make_async_remote_copy(
            src_ref=echo_ref,
            dst_ref=held.at[me],
            send_sem=echo_send.at[step],
            recv_sem=echo_recv.at[step],
            device_id=peer,
            device_id_type=MESH,
        )
        copy.start()
        copies.append(copy)
    for chunk in range(chunks):
        for half in range(2):
            load(chunk, half).start()
    own.wait()
    tap_copy.wait()
    column = lax.broadcasted_iota(jnp.int32, (PBLK, 2 * columns), 1)

    def interpolate(tile, before):
        def one(index, carry):
            cols = pl.multiple_of(index * 128, 128)
            for half in range(2):
                value = held[tile, half, pl.ds(cols, 128), :].astype(jnp.float32)
                value = jnp.concatenate([before(half, cols).astype(jnp.float32), value], axis=1)
                blocks = []
                for inner in range(128 // PBLK):
                    block = index * (128 // PBLK) + inner
                    piece = value[inner * PBLK:(inner + 1) * PBLK]
                    offset = offsets_ref[block]
                    result = jnp.zeros((PBLK, columns), jnp.float32)
                    for tap in range(NTAP):
                        moved = pltpu.roll(piece, offset + tap, axis=1)[:, columns:]
                        result = result + taps_ref[tap, block] * moved
                    blocks.append(result)
                flat[half, pl.ds(cols, 128), :] = jnp.concatenate(blocks, axis=0).astype(jnp.bfloat16)
            return carry

        lax.fori_loop(0, pings // 128, one, 0, unroll=2)
        for start in range(0, pings, SPAN):
            real, imag = [
                turn(unit, flat[half, start:start + SPAN, :]).astype(jnp.bfloat16) for half in range(2)
            ]
            for piece in range(columns // lines):
                row = tile * (columns // lines) + piece
                owner = row // tiles
                target = owner // CORES
                place = (target // share * CORES + owner % CORES) * share + target % share
                place = pl.multiple_of((place * tiles + row % tiles) * 2 * lines, 2 * lines)
                a = real[piece * lines:(piece + 1) * lines]
                b = imag[piece * lines:(piece + 1) * lines]
                left[pl.ds(place, lines), start:start + SPAN] = a
                left[pl.ds(place + lines, lines), start:start + SPAN] = b
                left[pl.ds(place, lines), pings + start:pings + start + SPAN] = -b
                left[pl.ds(place + lines, lines), pings + start:pings + start + SPAN] = a

    def unpack():
        for half in range(2):
            for start in range(0, pings, 128):
                value = edge_in[half, :, start:start + 128]
                value = jnp.concatenate([jnp.zeros((columns - EDGE, 128), jnp.bfloat16), value], axis=0)
                prior[half, start:start + 128, :] = turn(unit, value).astype(jnp.bfloat16)

    def from_edge(half, cols):
        return prior[half, pl.ds(cols, 128), :]

    def from_tile(tile):
        def before(half, cols):
            value = held[lax.max(tile - 1, 0), half, pl.ds(cols, 128), :].astype(jnp.float32)
            return jnp.where(tile > 0, value, 0.0)

        return before

    def pair(group, chunk):
        rows = pl.ds(pl.multiple_of(group * share * count, share * count), share * count)
        return pltpu.make_async_remote_copy(
            src_ref=part.at[chunk, 1 - core, rows],
            dst_ref=got.at[chunk, rows],
            send_sem=pair_send.at[group, chunk],
            recv_sem=pair_recv.at[group, chunk],
            device_id=partner,
            device_id_type=MESH,
        )

    def line(way, target, chunk):
        return pltpu.make_async_remote_copy(
            src_ref=away.at[way, target, chunk],
            dst_ref=near.at[way, target, chunk],
            send_sem=line_send.at[way, target, chunk],
            recv_sem=line_recv.at[way, target, chunk],
            device_id=(above, below)[way],
            device_id_type=MESH,
        )

    def scale_line(way, target, chunk):
        return pltpu.make_async_remote_copy(
            src_ref=away_scale.at[way, target, chunk],
            dst_ref=near_scale.at[way, target, chunk],
            send_sem=scale_send.at[way, target, chunk],
            recv_sem=scale_recv.at[way, target, chunk],
            device_id=(above, below)[way],
            device_id_type=MESH,
        )

    def rows_of(target):
        return pl.ds(pl.multiple_of(target * count, count), count)

    def collect(way, target, chunk):
        scale_line(way, target, chunk).wait_recv()
        line(way, target, chunk).wait_recv()
        part[chunk, core, rows_of(target), :] += decode(
            near.at[way, target, chunk], near_scale.at[way, target, chunk], count, width
        )

    def pass_on(way, target, chunk, first):
        @pl.when(jnp.logical_not(first))
        def _():
            collect(way, target, chunk)

        encode(
            part[chunk, core, rows_of(target), :], away.at[way, target, chunk], away_scale.at[way, target, chunk]
        )
        scale_line(way, target, chunk).start()
        line(way, target, chunk).start()

    half_rows = share * count
    block = min(512, CORES * half_rows)

    def multiply(group, chunk, first):
        if first:
            for half in range(2):
                load(chunk, half).wait()
        base = group * CORES * half_rows
        if block == CORES * half_rows:
            rows = pl.ds(pl.multiple_of(base, block), block)
            value = lax.dot_general(
                left[rows, :], weights[chunk], (((1,), (1,)), ((), ())),
                preferred_element_type=jnp.float32,
            )
            into = pl.ds(pl.multiple_of(group * half_rows, half_rows), half_rows)
            part[chunk, 0, into, :] = value[:half_rows]
            part[chunk, 1, into, :] = value[half_rows:]
        else:
            def rows_at(index, carry):
                rows = pl.ds(pl.multiple_of(base + index * block, block), block)
                value = lax.dot_general(
                    left[rows, :], weights[chunk], (((1,), (1,)), ((), ())),
                    preferred_element_type=jnp.float32,
                )
                start = group * half_rows + index % (half_rows // block) * block
                into = pl.ds(pl.multiple_of(start, block), block)
                part[chunk, index // (half_rows // block), into, :] = value
                return carry

            lax.fori_loop(0, CORES * half_rows // block, rows_at, 0)
        pair(group, chunk).start()

    def join(group, chunk):
        pair(group, chunk).wait_recv()
        rows = pl.ds(pl.multiple_of(group * half_rows, half_rows), half_rows)
        part[chunk, core, rows, :] += got[chunk, rows, :]

    tables = []
    for way in range(2):
        far_first = (list(range(last, 0, -1)), list(range(last)))[way]
        tables.append(
            [
                order_of(far_first, range(group * share, (group + 1) * share))
                for group in range(groups)
            ]
        )

    def across(step, chunk):
        peer = lax.rem(me + step, tiles)
        return pltpu.make_async_remote_copy(
            src_ref=fin.at[chunk, peer],
            dst_ref=side.at[chunk, step - 1],
            send_sem=side_send.at[step - 1, chunk],
            recv_sem=side_recv.at[step - 1, chunk],
            device_id={"rng": peer},
            device_id_type=MESH,
        )

    def place(source, chunk, value):
        start = pl.multiple_of(source * (chunks * width) + chunk * width, width)
        out_ref[0, :, pl.ds(start, width)] = value[:lines]
        out_ref[1, :, pl.ds(start, width)] = value[lines:]

    def finish(chunk):
        @pl.when(chip > 0)
        def _():
            collect(0, chip, chunk)

        @pl.when(chip < last)
        def _():
            collect(1, chip, chunk)

        for tile in range(tiles):
            rows = pl.ds(pl.multiple_of(chip * count + tile * 2 * lines, 2 * lines), 2 * lines)
            fin[chunk, tile] = part[chunk, core, rows, :]
        for step in range(1, tiles):
            across(step, chunk).start()
        place(me, chunk, fin[chunk, me])

    begins = []
    for way in range(2):
        begins.append(
            [
                [
                    row.index(target) * chunks + (target, last - target)[way] * LAG if target in row else 0
                    for target in range(chips)
                ]
                for row in tables[way]
            ]
        )
    mine = me if groups > 1 else 0
    begin = jnp.maximum(pick(begins[0], mine, chip), pick(begins[1], mine, chip))

    def stream(time):
        for way in range(2):
            hops = (chip, last - chip)[way]
            at = time - hops * LAG
            target = pick(tables[way], mine, at // chunks)
            ahead = (chip < target, chip > target)[way]
            ready = jnp.logical_and(at >= 0, at < last * chunks)

            @pl.when(jnp.logical_and(ready, ahead))
            def _():
                pass_on(way, target, at % chunks, hops == 0)

        done = time - begin

        @pl.when(jnp.logical_and(done >= 0, done < chunks))
        def _():
            finish(done)

    def steps(group, turn):
        def one(chunk, carry):
            multiply(group, chunk, turn == 0)

            @pl.when(chunk > 0)
            def _():
                join(group, chunk - 1)
                stream(turn * chunks + chunk - 1)

            return carry

        lax.fori_loop(0, chunks, one, 0)
        join(group, chunks - 1)
        stream(turn * chunks + chunks - 1)

    if groups > 1:
        @pl.when(me > 0)
        def _():
            edge().wait_recv()
            unpack()

        @pl.when(me == 0)
        def _():
            prior[...] = jnp.zeros_like(prior)

        interpolate(me, from_edge)
        steps(me, 0)
        for step, copy in enumerate(copies):
            source = lax.rem(me + tiles - 1 - step, tiles)
            copy.wait_recv()
        for step, copy in enumerate(copies):
            source = lax.rem(me + tiles - 1 - step, tiles)
            interpolate(source, from_tile(source))
            steps(source, 1 + step)
    else:
        for copy in copies:
            copy.wait_recv()

        def each(tile, carry):
            interpolate(tile, from_tile(tile))
            return carry

        lax.fori_loop(0, tiles, each, 0)
        steps(0, 0)

    def rest(time, carry):
        stream(time)
        return carry

    lax.fori_loop(groups * chunks, last * chunks + last * LAG, rest, 0)

    def arrive(chunk, carry):
        for step in range(1, tiles):
            across(step, chunk).wait()
            place(lax.rem(me + tiles - step, tiles), chunk, side[chunk, step - 1])
        for group in range(groups):
            pair(group, chunk).wait_send()
        for way in range(2):
            for target in range(chips):
                ahead = (chip < target, chip > target)[way]

                @pl.when(ahead)
                def _():
                    line(way, target, chunk).wait_send()
                    scale_line(way, target, chunk).wait_send()

        return carry

    lax.fori_loop(0, chunks, arrive, 0)
    for copy in copies:
        copy.wait_send()
    if groups > 1:
        @pl.when(me < tiles - 1)
        def _():
            edge().wait_send()


def lines_image(echo, steer, offsets, taps):
    tiles = lax.axis_size("rng")
    chips = lax.axis_size("ping") // CORES
    pings, columns = echo.shape[1:]
    cells = steer.shape[1]
    width = 512 if cells % 4096 == 0 else 256
    chunks = cells // width
    lines = columns // (chips * CORES)
    count = tiles * 2 * lines
    rows = chips * count
    groups = tiles if chips % tiles == 0 else 1
    vmem = pl.BlockSpec(memory_space=pltpu.VMEM)
    smem = pl.BlockSpec(memory_space=pltpu.SMEM)
    anywhere = pl.BlockSpec(memory_space=pl.ANY)
    dma = pltpu.SemaphoreType.DMA
    message = (width // 128 * count, 128)
    scales = (max(count // 128, 1), 128)
    others = max(tiles - 1, 1)
    return pl.pallas_call(
        functools.partial(image_kernel, (tiles, chips, chunks, width, lines, groups)),
        out_shape=jax.ShapeDtypeStruct((2, lines, tiles * cells), jnp.float32),
        in_specs=[smem, anywhere, vmem, anywhere],
        out_specs=vmem,
        scratch_shapes=[
            pltpu.SMEM(taps.shape[::-1], jnp.float32),
            pltpu.VMEM((tiles, 2, pings, columns), jnp.bfloat16),
            pltpu.VMEM((2, EDGE, pings), jnp.bfloat16),
            pltpu.VMEM((2, EDGE, pings), jnp.bfloat16),
            pltpu.VMEM((2, pings, columns), jnp.bfloat16),
            pltpu.VMEM((2, pings, columns), jnp.bfloat16),
            pltpu.VMEM((CORES * rows, 2 * pings), jnp.bfloat16),
            pltpu.VMEM((chunks, width, 2 * pings), jnp.bfloat16),
            pltpu.VMEM((chunks, CORES, rows, width), jnp.float32),
            pltpu.VMEM((chunks, rows, width), jnp.float32),
            pltpu.VMEM((2, chips, chunks) + message, jnp.int16),
            pltpu.VMEM((2, chips, chunks) + message, jnp.int16),
            pltpu.VMEM((2, chips, chunks) + scales, jnp.float32),
            pltpu.VMEM((2, chips, chunks) + scales, jnp.float32),
            pltpu.VMEM((chunks, tiles, 2 * lines, width), jnp.float32),
            pltpu.VMEM((chunks, others, 2 * lines, width), jnp.float32),
            dma,
            dma,
            dma,
            dma,
            dma((others,)),
            dma((others,)),
            dma((chunks, 2)),
            dma((groups, chunks)),
            dma((groups, chunks)),
            dma((2, chips, chunks)),
            dma((2, chips, chunks)),
            dma((2, chips, chunks)),
            dma((2, chips, chunks)),
            dma((others, chunks)),
            dma((others, chunks)),
        ],
        compiler_params=pltpu.CompilerParams(
            collective_id=0, has_side_effects=True, vmem_limit_bytes=60 * 2**20
        ),
    )(offsets, taps.T, echo, steer)


LANES = 128
BATCH = 4


def split(value):
    high = value.astype(jnp.bfloat16)
    return high, (value - high.astype(jnp.float32)).astype(jnp.bfloat16)


def exact_dot(left, right):
    total = None
    for _ in range(3):
        piece = right.astype(jnp.bfloat16)
        term = jnp.dot(left, piece, preferred_element_type=jnp.float32)
        total = term if total is None else total + term
        right = right - piece.astype(jnp.float32)
    return total


def dot_exact(left, right):
    total = None
    for _ in range(3):
        piece = left.astype(jnp.bfloat16)
        term = jnp.dot(piece, right, preferred_element_type=jnp.float32)
        total = term if total is None else total + term
        left = left - piece.astype(jnp.float32)
    return total


def stacked(value, axis):
    top, low = split(value)
    return jnp.concatenate([top, low, top], axis=axis)


def spectrum_of(fields, down_ref, over_ref, twist_ref):
    size = len(fields)
    high = fields[0].shape[0] // 2
    first = jnp.dot(
        down_ref[...], stacked(jnp.concatenate(fields, axis=1), 0), preferred_element_type=jnp.float32
    )
    rows = []
    for one in range(size):
        real = first[:high, one * LANES:(one + 1) * LANES]
        imag = first[high:, one * LANES:(one + 1) * LANES]
        rows.append(
            jnp.concatenate(
                [
                    real * twist_ref[0] + imag * twist_ref[1],
                    imag * twist_ref[0] - real * twist_ref[1],
                ],
                axis=1,
            )
        )
    return jnp.dot(
        stacked(jnp.concatenate(rows, axis=0), 1), over_ref[...], preferred_element_type=jnp.float32
    )


def gradient_kernel(
    count, tiles, centers_ref, halves_ref, down_ref, over_ref, twist_ref, image_ref, total_ref, spec_ref,
    grid, value, held, full, turned, send_sem, recv_sem, send_two, recv_two,
):
    me = lax.axis_index("ping") * tiles + lax.axis_index("rng")
    ids = [lax.rem(me + step, count) for step in range(1, count)]
    peers = [{"ping": lax.div(one, tiles), "rng": lax.rem(one, tiles)} for one in ids]
    barrier = pltpu.get_barrier_semaphore()
    for peer in peers:
        pl.semaphore_signal(barrier, inc=1, device_id=peer, device_id_type=MESH)

    lines, length = image_ref.shape[1:]
    high = length // LANES
    for half in range(2):
        for row in range(high):
            grid[pl.ds(half * high + row, lines, stride=2 * high), :] = image_ref[
                half, :, row * LANES:(row + 1) * LANES
            ]

    cells = lax.broadcasted_iota(jnp.int32, (high, LANES), 0) * LANES
    cells = cells + lax.broadcasted_iota(jnp.int32, (high, LANES), 1)
    bottom = lax.broadcasted_iota(jnp.int32, (8, LANES), 0) == 7
    lane = lax.broadcasted_iota(jnp.int32, (8, LANES), 1)
    angle = jnp.zeros((8, LANES), jnp.float32)
    for line in range(lines):
        angle = jnp.where(lane == line, centers_ref[line].astype(jnp.float32), angle)
    angle = angle * (2.0 * math.pi / length)
    turned[0] = jnp.cos(angle)
    turned[1] = jnp.sin(angle)

    def after(part):
        moved = pltpu.roll(part, high - 1, axis=0)
        end = moved[high - 8:]
        end = jnp.where(bottom, pltpu.roll(end, LANES - 1, axis=1), end)
        return jnp.concatenate([moved[:high - 8], end], axis=0)

    def field(line):
        return grid[pl.ds(pl.multiple_of(line * 2 * high, 2 * high), 2 * high), :]

    def windowed(index, carry):
        numer, denom = carry
        chosen = []
        for inner in range(BATCH):
            line = index * BATCH + inner
            distance = cells - centers_ref[line]
            distance = jnp.where(distance < 0, distance + length, distance)
            distance = jnp.minimum(distance, length - distance)
            inside = (distance <= halves_ref[line]).astype(jnp.float32)
            chosen.append(field(line) * jnp.concatenate([inside, inside], axis=0))
        found = spectrum_of(chosen, down_ref, over_ref, twist_ref)
        for inner in range(BATCH):
            real = found[inner * high:(inner + 1) * high, :LANES]
            imag = found[inner * high:(inner + 1) * high, LANES:]
            next_real = after(real)
            next_imag = after(imag)
            here = lane == index * BATCH + inner
            cos = jnp.sum(jnp.where(here, turned[0], 0.0), axis=1, keepdims=True)[:1]
            sin = jnp.sum(jnp.where(here, turned[1], 0.0), axis=1, keepdims=True)[:1]
            numer = numer + (real * next_real + imag * next_imag) * sin
            numer = numer + (real * next_imag - imag * next_real) * cos
            denom = denom + (real * real + imag * imag)
        return numer, denom

    zero = jnp.zeros((high, LANES), jnp.float32)
    numer, denom = lax.fori_loop(0, lines // BATCH, windowed, (zero, zero))
    each = value.shape[1]
    for block in range(count // 2):
        value[block] = numer[block * each:(block + 1) * each]
        value[count // 2 + block] = denom[block * each:(block + 1) * each]

    pl.semaphore_wait(barrier, len(peers))
    copies = []
    for step, peer in enumerate(peers):
        copy = pltpu.make_async_remote_copy(
            src_ref=value.at[ids[step]],
            dst_ref=held.at[step],
            send_sem=send_sem.at[step],
            recv_sem=recv_sem.at[step],
            device_id=peer,
            device_id_type=MESH,
        )
        copy.start()
        copies.append(copy)

    def whole(index, carry):
        found = spectrum_of(
            [field(index * BATCH + inner) for inner in range(BATCH)], down_ref, over_ref, twist_ref
        )
        spec_ref[pl.ds(pl.multiple_of(index * BATCH * high, BATCH * high), BATCH * high), :] = found
        return carry

    lax.fori_loop(0, lines // BATCH, whole, 0)
    total = value[me]
    for step, copy in enumerate(copies):
        copy.wait()
        total = total + held[step]
    full[me] = total
    copies = []
    for step, peer in enumerate(peers):
        copy = pltpu.make_async_remote_copy(
            src_ref=full.at[me],
            dst_ref=full.at[me],
            send_sem=send_two.at[step],
            recv_sem=recv_two.at[step],
            device_id=peer,
            device_id_type=MESH,
        )
        copy.start()
        copies.append(copy)
    for copy in copies:
        copy.wait()
    for block in range(count):
        total_ref[block * each:(block + 1) * each, :] = full[block]


def correct_kernel(
    up_ref, back_ref, twist_ref, total_ref, spec_ref, out_ref, phase_ref, grid, turn, tall,
):
    group = out_ref.shape[1]
    length = out_ref.shape[2]
    high = length // LANES

    @pl.when(pl.program_id(0) == 0)
    def _():
        slope = total_ref[:high] / (total_ref[high:] + epsilon)
        row = lax.broadcasted_iota(jnp.int32, (high, high), 0)
        below = (lax.broadcasted_iota(jnp.int32, (high, high), 1) < row).astype(jnp.float32)
        row = lax.broadcasted_iota(jnp.int32, (LANES, LANES), 0)
        ahead = (row < lax.broadcasted_iota(jnp.int32, (LANES, LANES), 1)).astype(jnp.float32)
        within = exact_dot(below.astype(jnp.bfloat16), slope)
        sums = jnp.broadcast_to(jnp.sum(slope, axis=0, keepdims=True), (8, LANES))
        across = dot_exact(sums, ahead.astype(jnp.bfloat16))
        mean = jnp.sum(sums[:1], axis=1, keepdims=True) / length
        order = lax.broadcasted_iota(jnp.int32, (high, LANES), 0)
        order = order + high * lax.broadcasted_iota(jnp.int32, (high, LANES), 1)
        phase = within + across[:1] - order.astype(jnp.float32) * mean
        ratio = LANES // high
        tall[:, :high] = phase.T
        phase_ref[...] = jnp.concatenate(
            [tall[pl.ds(part, LANES // ratio, stride=ratio), :high] for part in range(ratio)], axis=1
        )
        turn[0] = jnp.cos(phase)
        turn[1] = jnp.sin(phase)

    cos = turn[0]
    sin = turn[1]
    start = pl.program_id(0) * group * high
    rows = []
    for line in range(group):
        at = pl.ds(pl.multiple_of(start + line * high, high), high)
        real = spec_ref[at, :LANES]
        imag = spec_ref[at, LANES:]
        rows.append(jnp.concatenate([real * cos + imag * sin, imag * cos - real * sin], axis=1))
    first = jnp.dot(
        stacked(jnp.concatenate(rows, axis=0), 1), back_ref[...], preferred_element_type=jnp.float32
    )
    fields = []
    for line in range(group):
        real = first[line * high:(line + 1) * high, :LANES]
        imag = first[line * high:(line + 1) * high, LANES:]
        fields.append(
            jnp.concatenate(
                [
                    real * twist_ref[2] - imag * twist_ref[3],
                    real * twist_ref[3] + imag * twist_ref[2],
                ],
                axis=0,
            )
        )
    second = jnp.dot(
        up_ref[...], stacked(jnp.concatenate(fields, axis=1), 0), preferred_element_type=jnp.float32
    )
    for line in range(group):
        grid[line * 2 * high:(line + 1) * 2 * high, :] = second[:, line * LANES:(line + 1) * LANES]
    for half in range(2):
        for row in range(high):
            out_ref[half, :, row * LANES:(row + 1) * LANES] = grid[
                pl.ds(half * high + row, group, stride=2 * high), :
            ]


def waves(size, modulus, columns):
    angle = 2.0 * np.pi / modulus * (np.outer(np.arange(size), np.arange(columns)) % modulus)
    return np.cos(angle), np.sin(angle)


def pieces_of(matrix, axis):
    high = matrix.astype(jnp.bfloat16)
    low = (matrix - high.astype(np.float64)).astype(jnp.bfloat16)
    return np.concatenate([high, high, low], axis=axis)


def focus(image, centers, halves):
    pings, tiles = lax.axis_size("ping"), lax.axis_size("rng")
    count = pings * tiles
    lines, length = image.shape[1:]
    high = length // LANES
    cos, sin = waves(high, high, high)
    down = pieces_of(np.block([[cos, sin], [-sin, cos]]), 1)
    up = pieces_of(np.block([[cos, -sin], [sin, cos]]), 1)
    cos, sin = waves(LANES, LANES, LANES)
    over = pieces_of(np.block([[cos, -sin], [sin, cos]]), 0)
    back = pieces_of(np.block([[cos, sin], [-sin, cos]]), 0)
    cos, sin = waves(high, length, LANES)
    twist = np.stack([cos, sin, cos / length, sin / length]).astype(np.float32)
    each = 2 * high // count
    group = 8
    vmem = pl.BlockSpec(memory_space=pltpu.VMEM)
    smem = pl.BlockSpec(memory_space=pltpu.SMEM)
    semaphores = pltpu.SemaphoreType.DMA((count - 1,))
    total, spec = pl.pallas_call(
        functools.partial(gradient_kernel, count, tiles),
        out_shape=(
            jax.ShapeDtypeStruct((2 * high, LANES), jnp.float32),
            jax.ShapeDtypeStruct((lines * high, 2 * LANES), jnp.float32),
        ),
        in_specs=[smem, smem] + [vmem] * 4,
        out_specs=(vmem, vmem),
        scratch_shapes=[
            pltpu.VMEM((lines * 2 * high, LANES), jnp.float32),
            pltpu.VMEM((count, each, LANES), jnp.float32),
            pltpu.VMEM((count - 1, each, LANES), jnp.float32),
            pltpu.VMEM((count, each, LANES), jnp.float32),
            pltpu.VMEM((2, 8, LANES), jnp.float32),
            semaphores,
            semaphores,
            semaphores,
            semaphores,
        ],
        compiler_params=pltpu.CompilerParams(collective_id=1, has_side_effects=True),
    )(centers, halves, down, over, twist, image)
    focused, phase = pl.pallas_call(
        correct_kernel,
        grid=(lines // group,),
        out_shape=(
            jax.ShapeDtypeStruct((2, lines, length), jnp.float32),
            jax.ShapeDtypeStruct((high, LANES), jnp.float32),
        ),
        in_specs=[vmem] * 5,
        out_specs=(
            pl.BlockSpec((2, group, length), lambda index: (0, index, 0)),
            pl.BlockSpec((high, LANES), lambda index: (0, 0)),
        ),
        scratch_shapes=[
            pltpu.VMEM((group * 2 * high, LANES), jnp.float32),
            pltpu.VMEM((2, high, LANES), jnp.float32),
            pltpu.VMEM((LANES, LANES), jnp.float32),
        ],
    )(up, back, twist, total, spec)
    return focused, phase.reshape(length)


def on_device(echo, steer, offsets, taps, centers, halves):
    image = lines_image(echo, steer, offsets, taps)
    return focus(image, centers, halves)


def solution(mesh):
    in_specs = (
        P(None, ("leg", "ping"), "rng"),
        P(None, ("leg", "rng"), "ping"),
        P(("leg", "ping")),
        P(("leg", "ping"), None),
        P(("leg", "ping", "rng")),
        P(("leg", "ping", "rng")),
    )
    out_specs = (P(None, ("leg", "ping", "rng"), None), P("leg"))
    return jax.shard_map(
        on_device, mesh=mesh, in_specs=in_specs, out_specs=out_specs, check_vma=False
    )
```

```python
import functools
import math

import jax
import jax.numpy as jnp
import numpy as np
from jax import lax
from jax.experimental import pallas as pl
from jax.experimental.pallas import tpu as pltpu
from jax.sharding import PartitionSpec as P

PBLK = 64
NTAP = 4


epsilon = 1e-06


MESH = pl.DeviceIdType.MESH


CORES = 2
LAG = 3
EDGE = 24
SPAN = 512


def encode(value, target, scales):
    count, width = value.shape
    peak = jnp.max(jnp.abs(value), axis=1, keepdims=True)
    power = jnp.floor(jnp.log2(jnp.maximum(peak, 1e-30)) + 1.01)
    whole = jnp.round(value * jnp.exp2(15.0 - power)).astype(jnp.int32).astype(jnp.int16)
    for piece in range(width // 128):
        target[piece * count:(piece + 1) * count, :] = whole[:, piece * 128:(piece + 1) * 128]
    size = min(count, 128)
    lane = lax.broadcasted_iota(jnp.int32, (size, 128), 1)
    here = lane == lax.broadcasted_iota(jnp.int32, (size, 128), 0)
    for piece in range(count // size):
        part = jnp.where(here, power[piece * size:(piece + 1) * size], 0.0)
        scales[piece:piece + 1, :] = jnp.sum(part, axis=0, keepdims=True)


def decode(source, scales, count, width):
    size = min(count, 128)
    lane = lax.broadcasted_iota(jnp.int32, (size, 128), 1)
    here = lane == lax.broadcasted_iota(jnp.int32, (size, 128), 0)
    powers = [
        jnp.sum(jnp.where(here, scales[piece:piece + 1, :], 0.0), axis=1, keepdims=True)
        for piece in range(count // size)
    ]
    scale = jnp.exp2(jnp.concatenate(powers, axis=0) - 15.0)
    pieces = [
        source[piece * count:(piece + 1) * count, :].astype(jnp.int32).astype(jnp.float32) * scale
        for piece in range(width // 128)
    ]
    return jnp.concatenate(pieces, axis=1)


def order_of(targets, own):
    return [one for one in targets if one in own] + [one for one in targets if one not in own]


def pick(table, row, column):
    found = jnp.int32(table[0][0])
    for at_row, entries in enumerate(table):
        for at_column, entry in enumerate(entries):
            here = jnp.logical_and(row == at_row, column == at_column)
            found = jnp.where(here, jnp.int32(entry), found)
    return found


def image_kernel(
    plan, offsets_ref, taps_hbm, echo_ref, steer_ref, out_ref,
    taps_ref, held, edge_out, edge_in, prior, flat, left, weights, part, got, away, near, away_scale, near_scale, fin, side,
    taps_sem, own_sem, edge_send, edge_recv, echo_send, echo_recv, load_sem, pair_send, pair_recv,
    line_send, line_recv, scale_send, scale_recv, side_send, side_recv,
):
    tiles, chips, chunks, width, lines, groups = plan
    pings = echo_ref.shape[1]
    columns = echo_ref.shape[2]
    count = tiles * 2 * lines
    share = chips // groups
    me = lax.axis_index("rng")
    chip = lax.axis_index("ping") // CORES
    core = lax.axis_index("ping") % CORES
    last = chips - 1
    partner = {"ping": chip * CORES + 1 - core}
    above = {"ping": (chip + 1) * CORES + core}
    below = {"ping": (chip - 1) * CORES + core}
    peers = [{"rng": lax.rem(me + step, tiles)} for step in range(1, tiles)]

    barrier = pltpu.get_barrier_semaphore()
    for peer in peers + [partner]:
        pl.semaphore_signal(barrier, inc=1, device_id=peer, device_id_type=MESH)

    @pl.when(chip < last)
    def _():
        pl.semaphore_signal(barrier, inc=1, device_id=above, device_id_type=MESH)

    @pl.when(chip > 0)
    def _():
        pl.semaphore_signal(barrier, inc=1, device_id=below, device_id_type=MESH)

    tap_copy = pltpu.make_async_copy(taps_hbm, taps_ref, taps_sem)
    tap_copy.start()
    own = pltpu.make_async_copy(echo_ref, held.at[me], own_sem)
    own.start()

    def load(chunk, half):
        return pltpu.make_async_copy(
            steer_ref.at[half, pl.ds(chunk * width, width), :],
            weights.at[chunk, :, pl.ds(half * pings, pings)],
            load_sem.at[chunk, half],
        )


    def edge():
        return pltpu.make_async_remote_copy(
            src_ref=edge_out,
            dst_ref=edge_in,
            send_sem=edge_send,
            recv_sem=edge_recv,
            device_id={"rng": lax.rem(me + 1, tiles)},
            device_id_type=MESH,
        )

    row = lax.broadcasted_iota(jnp.int32, (128, 128), 0)
    unit = (row == lax.broadcasted_iota(jnp.int32, (128, 128), 1)).astype(jnp.float32).astype(jnp.bfloat16)

    def turn(chosen, value):
        return lax.dot_general(
            chosen, value, (((1,), (1,)), ((), ())), preferred_element_type=jnp.float32
        )

    if groups > 1:
        for half in range(2):
            for start in range(0, pings, SPAN):
                value = turn(unit[columns - EDGE:], echo_ref[half, start:start + SPAN, :])
                edge_out[half, :, start:start + SPAN] = value.astype(jnp.bfloat16)

    reached = len(peers) + 1 + (chip < last).astype(jnp.int32) + (chip > 0).astype(jnp.int32)
    pl.semaphore_wait(barrier, reached)
    if groups > 1:
        @pl.when(me < tiles - 1)
        def _():
            edge().start()

    copies = []
    for step, peer in enumerate(peers):
        copy = pltpu.make_async_remote_copy(
            src_ref=echo_ref,
            dst_ref=held.at[me],
            send_sem=echo_send.at[step],
            recv_sem=echo_recv.at[step],
            device_id=peer,
            device_id_type=MESH,
        )
        copy.start()
        copies.append(copy)
    for chunk in range(chunks):
        for half in range(2):
            load(chunk, half).start()
    own.wait()
    tap_copy.wait()
    column = lax.broadcasted_iota(jnp.int32, (PBLK, 2 * columns), 1)

    def interpolate(tile, before):
        def one(index, carry):
            cols = pl.multiple_of(index * 128, 128)
            for half in range(2):
                value = held[tile, half, pl.ds(cols, 128), :].astype(jnp.float32)
                value = jnp.concatenate([before(half, cols).astype(jnp.float32), value], axis=1)
                blocks = []
                for inner in range(128 // PBLK):
                    block = index * (128 // PBLK) + inner
                    piece = value[inner * PBLK:(inner + 1) * PBLK]
                    offset = offsets_ref[block]
                    result = jnp.zeros((PBLK, columns), jnp.float32)
                    for tap in range(NTAP):
                        moved = pltpu.roll(piece, offset + tap, axis=1)[:, columns:]
                        result = result + taps_ref[tap, block] * moved
                    blocks.append(result)
                flat[half, pl.ds(cols, 128), :] = jnp.concatenate(blocks, axis=0).astype(jnp.bfloat16)
            return carry

        lax.fori_loop(0, pings // 128, one, 0, unroll=2)
        for start in range(0, pings, SPAN):
            real, imag = [
                turn(unit, flat[half, start:start + SPAN, :]).astype(jnp.bfloat16) for half in range(2)
            ]
            for piece in range(columns // lines):
                row = tile * (columns // lines) + piece
                owner = row // tiles
                target = owner // CORES
                place = (target // share * CORES + owner % CORES) * share + target % share
                place = pl.multiple_of((place * tiles + row % tiles) * 2 * lines, 2 * lines)
                a = real[piece * lines:(piece + 1) * lines]
                b = imag[piece * lines:(piece + 1) * lines]
                left[pl.ds(place, lines), start:start + SPAN] = a
                left[pl.ds(place + lines, lines), start:start + SPAN] = b
                left[pl.ds(place, lines), pings + start:pings + start + SPAN] = -b
                left[pl.ds(place + lines, lines), pings + start:pings + start + SPAN] = a

    def unpack():
        for half in range(2):
            for start in range(0, pings, 128):
                value = edge_in[half, :, start:start + 128]
                value = jnp.concatenate([jnp.zeros((columns - EDGE, 128), jnp.bfloat16), value], axis=0)
                prior[half, start:start + 128, :] = turn(unit, value).astype(jnp.bfloat16)

    def from_edge(half, cols):
        return prior[half, pl.ds(cols, 128), :]

    def from_tile(tile):
        def before(half, cols):
            value = held[lax.max(tile - 1, 0), half, pl.ds(cols, 128), :].astype(jnp.float32)
            return jnp.where(tile > 0, value, 0.0)

        return before

    def pair(group, chunk):
        rows = pl.ds(pl.multiple_of(group * share * count, share * count), share * count)
        return pltpu.make_async_remote_copy(
            src_ref=part.at[chunk, 1 - core, rows],
            dst_ref=got.at[chunk, rows],
            send_sem=pair_send.at[group, chunk],
            recv_sem=pair_recv.at[group, chunk],
            device_id=partner,
            device_id_type=MESH,
        )

    def line(way, target, chunk):
        return pltpu.make_async_remote_copy(
            src_ref=away.at[way, target, chunk],
            dst_ref=near.at[way, target, chunk],
            send_sem=line_send.at[way, target, chunk],
            recv_sem=line_recv.at[way, target, chunk],
            device_id=(above, below)[way],
            device_id_type=MESH,
        )

    def scale_line(way, target, chunk):
        return pltpu.make_async_remote_copy(
            src_ref=away_scale.at[way, target, chunk],
            dst_ref=near_scale.at[way, target, chunk],
            send_sem=scale_send.at[way, target, chunk],
            recv_sem=scale_recv.at[way, target, chunk],
            device_id=(above, below)[way],
            device_id_type=MESH,
        )

    def rows_of(target):
        return pl.ds(pl.multiple_of(target * count, count), count)

    def collect(way, target, chunk):
        scale_line(way, target, chunk).wait_recv()
        line(way, target, chunk).wait_recv()
        part[chunk, core, rows_of(target), :] += decode(
            near.at[way, target, chunk], near_scale.at[way, target, chunk], count, width
        )

    def pass_on(way, target, chunk, first):
        @pl.when(jnp.logical_not(first))
        def _():
            collect(way, target, chunk)

        encode(
            part[chunk, core, rows_of(target), :], away.at[way, target, chunk], away_scale.at[way, target, chunk]
        )
        scale_line(way, target, chunk).start()
        line(way, target, chunk).start()

    half_rows = share * count
    block = min(512, CORES * half_rows)

    def multiply(group, chunk, first):
        if first:
            for half in range(2):
                load(chunk, half).wait()
        base = group * CORES * half_rows
        if block == CORES * half_rows:
            rows = pl.ds(pl.multiple_of(base, block), block)
            value = lax.dot_general(
                left[rows, :], weights[chunk], (((1,), (1,)), ((), ())),
                preferred_element_type=jnp.float32,
            )
            into = pl.ds(pl.multiple_of(group * half_rows, half_rows), half_rows)
            part[chunk, 0, into, :] = value[:half_rows]
            part[chunk, 1, into, :] = value[half_rows:]
        else:
            def rows_at(index, carry):
                rows = pl.ds(pl.multiple_of(base + index * block, block), block)
                value = lax.dot_general(
                    left[rows, :], weights[chunk], (((1,), (1,)), ((), ())),
                    preferred_element_type=jnp.float32,
                )
                start = group * half_rows + index % (half_rows // block) * block
                into = pl.ds(pl.multiple_of(start, block), block)
                part[chunk, index // (half_rows // block), into, :] = value
                return carry

            lax.fori_loop(0, CORES * half_rows // block, rows_at, 0)
        pair(group, chunk).start()

    def join(group, chunk):
        pair(group, chunk).wait_recv()
        rows = pl.ds(pl.multiple_of(group * half_rows, half_rows), half_rows)
        part[chunk, core, rows, :] += got[chunk, rows, :]

    tables = []
    for way in range(2):
        far_first = (list(range(last, 0, -1)), list(range(last)))[way]
        tables.append(
            [
                order_of(far_first, range(group * share, (group + 1) * share))
                for group in range(groups)
            ]
        )

    def across(step, chunk):
        peer = lax.rem(me + step, tiles)
        return pltpu.make_async_remote_copy(
            src_ref=fin.at[chunk, peer],
            dst_ref=side.at[chunk, step - 1],
            send_sem=side_send.at[step - 1, chunk],
            recv_sem=side_recv.at[step - 1, chunk],
            device_id={"rng": peer},
            device_id_type=MESH,
        )

    def place(source, chunk, value):
        start = pl.multiple_of(source * (chunks * width) + chunk * width, width)
        out_ref[0, :, pl.ds(start, width)] = value[:lines]
        out_ref[1, :, pl.ds(start, width)] = value[lines:]

    def finish(chunk):
        @pl.when(chip > 0)
        def _():
            collect(0, chip, chunk)

        @pl.when(chip < last)
        def _():
            collect(1, chip, chunk)

        for tile in range(tiles):
            rows = pl.ds(pl.multiple_of(chip * count + tile * 2 * lines, 2 * lines), 2 * lines)
            fin[chunk, tile] = part[chunk, core, rows, :]
        for step in range(1, tiles):
            across(step, chunk).start()
        place(me, chunk, fin[chunk, me])

    begins = []
    for way in range(2):
        begins.append(
            [
                [
                    row.index(target) * chunks + (target, last - target)[way] * LAG if target in row else 0
                    for target in range(chips)
                ]
                for row in tables[way]
            ]
        )
    mine = me if groups > 1 else 0
    begin = jnp.maximum(pick(begins[0], mine, chip), pick(begins[1], mine, chip))

    def stream(time):
        for way in range(2):
            hops = (chip, last - chip)[way]
            at = time - hops * LAG
            target = pick(tables[way], mine, at // chunks)
            ahead = (chip < target, chip > target)[way]
            ready = jnp.logical_and(at >= 0, at < last * chunks)

            @pl.when(jnp.logical_and(ready, ahead))
            def _():
                pass_on(way, target, at % chunks, hops == 0)

        done = time - begin

        @pl.when(jnp.logical_and(done >= 0, done < chunks))
        def _():
            finish(done)

    def steps(group, turn):
        def one(chunk, carry):
            multiply(group, chunk, turn == 0)

            @pl.when(chunk > 0)
            def _():
                join(group, chunk - 1)
                stream(turn * chunks + chunk - 1)

            return carry

        lax.fori_loop(0, chunks, one, 0)
        join(group, chunks - 1)
        stream(turn * chunks + chunks - 1)

    if groups > 1:
        @pl.when(me > 0)
        def _():
            edge().wait_recv()
            unpack()

        @pl.when(me == 0)
        def _():
            prior[...] = jnp.zeros_like(prior)

        interpolate(me, from_edge)
        steps(me, 0)
        for step, copy in enumerate(copies):
            source = lax.rem(me + tiles - 1 - step, tiles)
            copy.wait_recv()
        for step, copy in enumerate(copies):
            source = lax.rem(me + tiles - 1 - step, tiles)
            interpolate(source, from_tile(source))
            steps(source, 1 + step)
    else:
        for copy in copies:
            copy.wait_recv()

        def each(tile, carry):
            interpolate(tile, from_tile(tile))
            return carry

        lax.fori_loop(0, tiles, each, 0)
        steps(0, 0)

    def rest(time, carry):
        stream(time)
        return carry

    lax.fori_loop(groups * chunks, last * chunks + last * LAG, rest, 0)

    def arrive(chunk, carry):
        for step in range(1, tiles):
            across(step, chunk).wait()
            place(lax.rem(me + tiles - step, tiles), chunk, side[chunk, step - 1])
        for group in range(groups):
            pair(group, chunk).wait_send()
        for way in range(2):
            for target in range(chips):
                ahead = (chip < target, chip > target)[way]

                @pl.when(ahead)
                def _():
                    line(way, target, chunk).wait_send()
                    scale_line(way, target, chunk).wait_send()

        return carry

    lax.fori_loop(0, chunks, arrive, 0)
    for copy in copies:
        copy.wait_send()
    if groups > 1:
        @pl.when(me < tiles - 1)
        def _():
            edge().wait_send()


def lines_image(echo, steer, offsets, taps):
    tiles = lax.axis_size("rng")
    chips = lax.axis_size("ping") // CORES
    pings, columns = echo.shape[1:]
    cells = steer.shape[1]
    width = 512 if cells % 4096 == 0 else 256
    chunks = cells // width
    lines = columns // (chips * CORES)
    count = tiles * 2 * lines
    rows = chips * count
    groups = tiles if chips % tiles == 0 else 1
    vmem = pl.BlockSpec(memory_space=pltpu.VMEM)
    smem = pl.BlockSpec(memory_space=pltpu.SMEM)
    anywhere = pl.BlockSpec(memory_space=pl.ANY)
    dma = pltpu.SemaphoreType.DMA
    message = (width // 128 * count, 128)
    scales = (max(count // 128, 1), 128)
    others = max(tiles - 1, 1)
    return pl.pallas_call(
        functools.partial(image_kernel, (tiles, chips, chunks, width, lines, groups)),
        out_shape=jax.ShapeDtypeStruct((2, lines, tiles * cells), jnp.float32),
        in_specs=[smem, anywhere, vmem, anywhere],
        out_specs=vmem,
        scratch_shapes=[
            pltpu.SMEM(taps.shape[::-1], jnp.float32),
            pltpu.VMEM((tiles, 2, pings, columns), jnp.bfloat16),
            pltpu.VMEM((2, EDGE, pings), jnp.bfloat16),
            pltpu.VMEM((2, EDGE, pings), jnp.bfloat16),
            pltpu.VMEM((2, pings, columns), jnp.bfloat16),
            pltpu.VMEM((2, pings, columns), jnp.bfloat16),
            pltpu.VMEM((CORES * rows, 2 * pings), jnp.bfloat16),
            pltpu.VMEM((chunks, width, 2 * pings), jnp.bfloat16),
            pltpu.VMEM((chunks, CORES, rows, width), jnp.float32),
            pltpu.VMEM((chunks, rows, width), jnp.float32),
            pltpu.VMEM((2, chips, chunks) + message, jnp.int16),
            pltpu.VMEM((2, chips, chunks) + message, jnp.int16),
            pltpu.VMEM((2, chips, chunks) + scales, jnp.float32),
            pltpu.VMEM((2, chips, chunks) + scales, jnp.float32),
            pltpu.VMEM((chunks, tiles, 2 * lines, width), jnp.float32),
            pltpu.VMEM((chunks, others, 2 * lines, width), jnp.float32),
            dma,
            dma,
            dma,
            dma,
            dma((others,)),
            dma((others,)),
            dma((chunks, 2)),
            dma((groups, chunks)),
            dma((groups, chunks)),
            dma((2, chips, chunks)),
            dma((2, chips, chunks)),
            dma((2, chips, chunks)),
            dma((2, chips, chunks)),
            dma((others, chunks)),
            dma((others, chunks)),
        ],
        compiler_params=pltpu.CompilerParams(
            collective_id=0, has_side_effects=True, vmem_limit_bytes=60 * 2**20
        ),
    )(offsets, taps.T, echo, steer)


LANES = 128


def split(value):
    high = value.astype(jnp.bfloat16)
    return high, (value - high.astype(jnp.float32)).astype(jnp.bfloat16)


def exact_dot(left, right):
    total = None
    for _ in range(3):
        piece = right.astype(jnp.bfloat16)
        term = jnp.dot(left, piece, preferred_element_type=jnp.float32)
        total = term if total is None else total + term
        right = right - piece.astype(jnp.float32)
    return total


def dot_exact(left, right):
    total = None
    for _ in range(3):
        piece = left.astype(jnp.bfloat16)
        term = jnp.dot(piece, right, preferred_element_type=jnp.float32)
        total = term if total is None else total + term
        left = left - piece.astype(jnp.float32)
    return total


def stacked(value, axis):
    top, low = split(value)
    return jnp.concatenate([top, low, top], axis=axis)


def spectrum_of(fields, down_ref, over_ref, twist_ref):
    size = len(fields)
    high = fields[0].shape[0] // 2
    first = jnp.dot(
        down_ref[...], stacked(jnp.concatenate(fields, axis=1), 0), preferred_element_type=jnp.float32
    )
    rows = []
    for one in range(size):
        real = first[:high, one * LANES:(one + 1) * LANES]
        imag = first[high:, one * LANES:(one + 1) * LANES]
        rows.append(
            jnp.concatenate(
                [
                    real * twist_ref[0] + imag * twist_ref[1],
                    imag * twist_ref[0] - real * twist_ref[1],
                ],
                axis=1,
            )
        )
    return jnp.dot(
        stacked(jnp.concatenate(rows, axis=0), 1), over_ref[...], preferred_element_type=jnp.float32
    )


def gradient_kernel(
    count, tiles, centers_ref, halves_ref, down_ref, over_ref, twist_ref, image_ref, total_ref, spec_ref,
    grid, value, held, full, turned, send_sem, recv_sem, send_two, recv_two,
):
    me = lax.axis_index("ping") * tiles + lax.axis_index("rng")
    ids = [lax.rem(me + step, count) for step in range(1, count)]
    peers = [{"ping": lax.div(one, tiles), "rng": lax.rem(one, tiles)} for one in ids]
    barrier = pltpu.get_barrier_semaphore()
    for peer in peers:
        pl.semaphore_signal(barrier, inc=1, device_id=peer, device_id_type=MESH)

    lines, length = image_ref.shape[1:]
    high = length // LANES
    batch = min(lines, 16)
    for half in range(2):
        for row in range(high):
            grid[pl.ds(half * high + row, lines, stride=2 * high), :] = image_ref[
                half, :, row * LANES:(row + 1) * LANES
            ]

    cells = lax.broadcasted_iota(jnp.int32, (high, LANES), 0) * LANES
    cells = cells + lax.broadcasted_iota(jnp.int32, (high, LANES), 1)
    bottom = lax.broadcasted_iota(jnp.int32, (8, LANES), 0) == 7
    lane = lax.broadcasted_iota(jnp.int32, (8, LANES), 1)
    angle = jnp.zeros((8, LANES), jnp.float32)
    for line in range(lines):
        angle = jnp.where(lane == line, centers_ref[line].astype(jnp.float32), angle)
    angle = angle * (2.0 * math.pi / length)
    turned[0] = jnp.cos(angle)
    turned[1] = jnp.sin(angle)

    def after(part):
        moved = pltpu.roll(part, high - 1, axis=0)
        end = moved[high - 8:]
        end = jnp.where(bottom, pltpu.roll(end, LANES - 1, axis=1), end)
        return jnp.concatenate([moved[:high - 8], end], axis=0)

    def field(line):
        return grid[pl.ds(pl.multiple_of(line * 2 * high, 2 * high), 2 * high), :]

    def windowed(index, carry):
        numer, denom = carry
        chosen = []
        for inner in range(batch):
            line = index * batch + inner
            distance = cells - centers_ref[line]
            distance = jnp.where(distance < 0, distance + length, distance)
            distance = jnp.minimum(distance, length - distance)
            inside = (distance <= halves_ref[line]).astype(jnp.float32)
            chosen.append(field(line) * jnp.concatenate([inside, inside], axis=0))
        found = spectrum_of(chosen, down_ref, over_ref, twist_ref)
        for inner in range(batch):
            real = found[inner * high:(inner + 1) * high, :LANES]
            imag = found[inner * high:(inner + 1) * high, LANES:]
            next_real = after(real)
            next_imag = after(imag)
            here = lane == index * batch + inner
            cos = jnp.sum(jnp.where(here, turned[0], 0.0), axis=1, keepdims=True)[:1]
            sin = jnp.sum(jnp.where(here, turned[1], 0.0), axis=1, keepdims=True)[:1]
            numer = numer + (real * next_real + imag * next_imag) * sin
            numer = numer + (real * next_imag - imag * next_real) * cos
            denom = denom + (real * real + imag * imag)
        return numer, denom

    zero = jnp.zeros((high, LANES), jnp.float32)
    numer, denom = lax.fori_loop(0, lines // batch, windowed, (zero, zero))
    each = value.shape[1]
    for block in range(count // 2):
        value[block] = numer[block * each:(block + 1) * each]
        value[count // 2 + block] = denom[block * each:(block + 1) * each]

    pl.semaphore_wait(barrier, len(peers))
    copies = []
    for step, peer in enumerate(peers):
        copy = pltpu.make_async_remote_copy(
            src_ref=value.at[ids[step]],
            dst_ref=held.at[step],
            send_sem=send_sem.at[step],
            recv_sem=recv_sem.at[step],
            device_id=peer,
            device_id_type=MESH,
        )
        copy.start()
        copies.append(copy)

    def whole(index, carry):
        found = spectrum_of(
            [field(index * batch + inner) for inner in range(batch)], down_ref, over_ref, twist_ref
        )
        spec_ref[pl.ds(pl.multiple_of(index * batch * high, batch * high), batch * high), :] = found
        return carry

    lax.fori_loop(0, lines // batch, whole, 0)
    total = value[me]
    for step, copy in enumerate(copies):
        copy.wait()
        total = total + held[step]
    full[me] = total
    copies = []
    for step, peer in enumerate(peers):
        copy = pltpu.make_async_remote_copy(
            src_ref=full.at[me],
            dst_ref=full.at[me],
            send_sem=send_two.at[step],
            recv_sem=recv_two.at[step],
            device_id=peer,
            device_id_type=MESH,
        )
        copy.start()
        copies.append(copy)
    for copy in copies:
        copy.wait()
    for block in range(count):
        total_ref[block * each:(block + 1) * each, :] = full[block]


def correct_kernel(
    up_ref, back_ref, twist_ref, total_ref, spec_ref, out_ref, phase_ref, grid, turn, tall,
):
    group = out_ref.shape[1]
    length = out_ref.shape[2]
    high = length // LANES

    @pl.when(pl.program_id(0) == 0)
    def _():
        slope = total_ref[:high] / (total_ref[high:] + epsilon)
        row = lax.broadcasted_iota(jnp.int32, (high, high), 0)
        below = (lax.broadcasted_iota(jnp.int32, (high, high), 1) < row).astype(jnp.float32)
        row = lax.broadcasted_iota(jnp.int32, (LANES, LANES), 0)
        ahead = (row < lax.broadcasted_iota(jnp.int32, (LANES, LANES), 1)).astype(jnp.float32)
        within = exact_dot(below.astype(jnp.bfloat16), slope)
        sums = jnp.broadcast_to(jnp.sum(slope, axis=0, keepdims=True), (8, LANES))
        across = dot_exact(sums, ahead.astype(jnp.bfloat16))
        mean = jnp.sum(sums[:1], axis=1, keepdims=True) / length
        order = lax.broadcasted_iota(jnp.int32, (high, LANES), 0)
        order = order + high * lax.broadcasted_iota(jnp.int32, (high, LANES), 1)
        phase = within + across[:1] - order.astype(jnp.float32) * mean
        ratio = LANES // high
        tall[:, :high] = phase.T
        phase_ref[...] = jnp.concatenate(
            [tall[pl.ds(part, LANES // ratio, stride=ratio), :high] for part in range(ratio)], axis=1
        )
        turn[0] = jnp.cos(phase)
        turn[1] = jnp.sin(phase)

    cos = turn[0]
    sin = turn[1]
    start = pl.program_id(0) * group * high
    rows = []
    for line in range(group):
        at = pl.ds(pl.multiple_of(start + line * high, high), high)
        real = spec_ref[at, :LANES]
        imag = spec_ref[at, LANES:]
        rows.append(jnp.concatenate([real * cos + imag * sin, imag * cos - real * sin], axis=1))
    first = jnp.dot(
        stacked(jnp.concatenate(rows, axis=0), 1), back_ref[...], preferred_element_type=jnp.float32
    )
    fields = []
    for line in range(group):
        real = first[line * high:(line + 1) * high, :LANES]
        imag = first[line * high:(line + 1) * high, LANES:]
        fields.append(
            jnp.concatenate(
                [
                    real * twist_ref[2] - imag * twist_ref[3],
                    real * twist_ref[3] + imag * twist_ref[2],
                ],
                axis=0,
            )
        )
    second = jnp.dot(
        up_ref[...], stacked(jnp.concatenate(fields, axis=1), 0), preferred_element_type=jnp.float32
    )
    for line in range(group):
        grid[line * 2 * high:(line + 1) * 2 * high, :] = second[:, line * LANES:(line + 1) * LANES]
    for half in range(2):
        for row in range(high):
            out_ref[half, :, row * LANES:(row + 1) * LANES] = grid[
                pl.ds(half * high + row, group, stride=2 * high), :
            ]


def waves(size, modulus, columns):
    angle = 2.0 * np.pi / modulus * (np.outer(np.arange(size), np.arange(columns)) % modulus)
    return np.cos(angle), np.sin(angle)


def pieces_of(matrix, axis):
    high = matrix.astype(jnp.bfloat16)
    low = (matrix - high.astype(np.float64)).astype(jnp.bfloat16)
    return np.concatenate([high, high, low], axis=axis)


def focus(image, centers, halves):
    pings, tiles = lax.axis_size("ping"), lax.axis_size("rng")
    count = pings * tiles
    lines, length = image.shape[1:]
    high = length // LANES
    cos, sin = waves(high, high, high)
    down = pieces_of(np.block([[cos, sin], [-sin, cos]]), 1)
    up = pieces_of(np.block([[cos, -sin], [sin, cos]]), 1)
    cos, sin = waves(LANES, LANES, LANES)
    over = pieces_of(np.block([[cos, -sin], [sin, cos]]), 0)
    back = pieces_of(np.block([[cos, sin], [-sin, cos]]), 0)
    cos, sin = waves(high, length, LANES)
    twist = np.stack([cos, sin, cos / length, sin / length]).astype(np.float32)
    each = 2 * high // count
    group = lines
    vmem = pl.BlockSpec(memory_space=pltpu.VMEM)
    smem = pl.BlockSpec(memory_space=pltpu.SMEM)
    semaphores = pltpu.SemaphoreType.DMA((count - 1,))
    total, spec = pl.pallas_call(
        functools.partial(gradient_kernel, count, tiles),
        out_shape=(
            jax.ShapeDtypeStruct((2 * high, LANES), jnp.float32),
            jax.ShapeDtypeStruct((lines * high, 2 * LANES), jnp.float32),
        ),
        in_specs=[smem, smem] + [vmem] * 4,
        out_specs=(vmem, vmem),
        scratch_shapes=[
            pltpu.VMEM((lines * 2 * high, LANES), jnp.float32),
            pltpu.VMEM((count, each, LANES), jnp.float32),
            pltpu.VMEM((count - 1, each, LANES), jnp.float32),
            pltpu.VMEM((count, each, LANES), jnp.float32),
            pltpu.VMEM((2, 8, LANES), jnp.float32),
            semaphores,
            semaphores,
            semaphores,
            semaphores,
        ],
        compiler_params=pltpu.CompilerParams(collective_id=1, has_side_effects=True),
    )(centers, halves, down, over, twist, image)
    focused, phase = pl.pallas_call(
        correct_kernel,
        grid=(lines // group,),
        out_shape=(
            jax.ShapeDtypeStruct((2, lines, length), jnp.float32),
            jax.ShapeDtypeStruct((high, LANES), jnp.float32),
        ),
        in_specs=[vmem] * 5,
        out_specs=(
            pl.BlockSpec((2, group, length), lambda index: (0, index, 0)),
            pl.BlockSpec((high, LANES), lambda index: (0, 0)),
        ),
        scratch_shapes=[
            pltpu.VMEM((group * 2 * high, LANES), jnp.float32),
            pltpu.VMEM((2, high, LANES), jnp.float32),
            pltpu.VMEM((LANES, LANES), jnp.float32),
        ],
    )(up, back, twist, total, spec)
    return focused, phase.reshape(length)


def on_device(echo, steer, offsets, taps, centers, halves):
    image = lines_image(echo, steer, offsets, taps)
    return focus(image, centers, halves)


def solution(mesh):
    in_specs = (
        P(None, ("leg", "ping"), "rng"),
        P(None, ("leg", "rng"), "ping"),
        P(("leg", "ping")),
        P(("leg", "ping"), None),
        P(("leg", "ping", "rng")),
        P(("leg", "ping", "rng")),
    )
    out_specs = (P(None, ("leg", "ping", "rng"), None), P("leg"))
    return jax.shard_map(
        on_device, mesh=mesh, in_specs=in_specs, out_specs=out_specs, check_vma=False
    )
```

```python
import functools
import math

import jax
import jax.numpy as jnp
import numpy as np
from jax import lax
from jax.experimental import pallas as pl
from jax.experimental.pallas import tpu as pltpu
from jax.sharding import PartitionSpec as P

PBLK = 64
NTAP = 4


epsilon = 1e-06


MESH = pl.DeviceIdType.MESH


CORES = 2
LAG = 3
EDGE = 24
SPAN = 512


def encode(value, target, scales):
    count, width = value.shape
    peak = jnp.max(jnp.abs(value), axis=1, keepdims=True)
    power = jnp.floor(jnp.log2(jnp.maximum(peak, 1e-30)) + 1.01)
    whole = jnp.round(value * jnp.exp2(15.0 - power)).astype(jnp.int32).astype(jnp.int16)
    for piece in range(width // 128):
        target[piece * count:(piece + 1) * count, :] = whole[:, piece * 128:(piece + 1) * 128]
    size = min(count, 128)
    lane = lax.broadcasted_iota(jnp.int32, (size, 128), 1)
    here = lane == lax.broadcasted_iota(jnp.int32, (size, 128), 0)
    for piece in range(count // size):
        part = jnp.where(here, power[piece * size:(piece + 1) * size], 0.0)
        scales[piece:piece + 1, :] = jnp.sum(part, axis=0, keepdims=True)


def decode(source, scales, count, width):
    size = min(count, 128)
    lane = lax.broadcasted_iota(jnp.int32, (size, 128), 1)
    here = lane == lax.broadcasted_iota(jnp.int32, (size, 128), 0)
    powers = [
        jnp.sum(jnp.where(here, scales[piece:piece + 1, :], 0.0), axis=1, keepdims=True)
        for piece in range(count // size)
    ]
    scale = jnp.exp2(jnp.concatenate(powers, axis=0) - 15.0)
    pieces = [
        source[piece * count:(piece + 1) * count, :].astype(jnp.int32).astype(jnp.float32) * scale
        for piece in range(width // 128)
    ]
    return jnp.concatenate(pieces, axis=1)


def order_of(targets, own):
    return [one for one in targets if one in own] + [one for one in targets if one not in own]


def pick(table, row, column):
    found = jnp.int32(table[0][0])
    for at_row, entries in enumerate(table):
        for at_column, entry in enumerate(entries):
            here = jnp.logical_and(row == at_row, column == at_column)
            found = jnp.where(here, jnp.int32(entry), found)
    return found


def image_kernel(
    plan, offsets_ref, taps_hbm, echo_ref, steer_ref, out_ref,
    taps_ref, held, edge_out, edge_in, prior, flat, left, weights, part, got, away, near, away_scale, near_scale, fin, side,
    taps_sem, own_sem, edge_send, edge_recv, echo_send, echo_recv, load_sem, pair_send, pair_recv,
    line_send, line_recv, scale_send, scale_recv, side_send, side_recv,
):
    tiles, chips, chunks, width, lines, groups = plan
    pings = echo_ref.shape[1]
    columns = echo_ref.shape[2]
    count = tiles * 2 * lines
    share = chips // groups
    me = lax.axis_index("rng")
    chip = lax.axis_index("ping") // CORES
    core = lax.axis_index("ping") % CORES
    last = chips - 1
    partner = {"ping": chip * CORES + 1 - core}
    above = {"ping": lax.min(chip + 1, last) * CORES + core}
    below = {"ping": lax.max(chip - 1, 0) * CORES + core}
    peers = [{"rng": lax.rem(me + step, tiles)} for step in range(1, tiles)]

    barrier = pltpu.get_barrier_semaphore()
    for peer in peers + [partner]:
        pl.semaphore_signal(barrier, inc=1, device_id=peer, device_id_type=MESH)

    @pl.when(chip < last)
    def _():
        pl.semaphore_signal(barrier, inc=1, device_id=above, device_id_type=MESH)

    @pl.when(chip > 0)
    def _():
        pl.semaphore_signal(barrier, inc=1, device_id=below, device_id_type=MESH)

    tap_copy = pltpu.make_async_copy(taps_hbm, taps_ref, taps_sem)
    tap_copy.start()
    own = pltpu.make_async_copy(echo_ref, held.at[me], own_sem)
    own.start()

    def load(chunk, half):
        return pltpu.make_async_copy(
            steer_ref.at[half, pl.ds(chunk * width, width), :],
            weights.at[chunk, :, pl.ds(half * pings, pings)],
            load_sem.at[chunk, half],
        )


    def edge():
        return pltpu.make_async_remote_copy(
            src_ref=edge_out,
            dst_ref=edge_in,
            send_sem=edge_send,
            recv_sem=edge_recv,
            device_id={"rng": lax.rem(me + 1, tiles)},
            device_id_type=MESH,
        )

    row = lax.broadcasted_iota(jnp.int32, (128, 128), 0)
    unit = (row == lax.broadcasted_iota(jnp.int32, (128, 128), 1)).astype(jnp.float32).astype(jnp.bfloat16)

    def turn(chosen, value):
        return lax.dot_general(
            chosen, value, (((1,), (1,)), ((), ())), preferred_element_type=jnp.float32
        )

    if groups > 1:
        for half in range(2):
            for start in range(0, pings, SPAN):
                value = turn(unit[columns - EDGE:], echo_ref[half, start:start + SPAN, :])
                edge_out[half, :, start:start + SPAN] = value.astype(jnp.bfloat16)

    reached = len(peers) + 1 + (chip < last).astype(jnp.int32) + (chip > 0).astype(jnp.int32)
    pl.semaphore_wait(barrier, reached)
    if groups > 1:
        @pl.when(me < tiles - 1)
        def _():
            edge().start()

    copies = []
    for step, peer in enumerate(peers):
        copy = pltpu.make_async_remote_copy(
            src_ref=echo_ref,
            dst_ref=held.at[me],
            send_sem=echo_send.at[step],
            recv_sem=echo_recv.at[step],
            device_id=peer,
            device_id_type=MESH,
        )
        copy.start()
        copies.append(copy)
    for chunk in range(chunks):
        for half in range(2):
            load(chunk, half).start()
    own.wait()
    tap_copy.wait()
    column = lax.broadcasted_iota(jnp.int32, (PBLK, 2 * columns), 1)

    def interpolate(tile, before):
        def one(index, carry):
            cols = pl.multiple_of(index * 128, 128)
            for half in range(2):
                value = held[tile, half, pl.ds(cols, 128), :].astype(jnp.float32)
                value = jnp.concatenate([before(half, cols).astype(jnp.float32), value], axis=1)
                blocks = []
                for inner in range(128 // PBLK):
                    block = index * (128 // PBLK) + inner
                    piece = value[inner * PBLK:(inner + 1) * PBLK]
                    offset = offsets_ref[block]
                    result = jnp.zeros((PBLK, columns), jnp.float32)
                    for tap in range(NTAP):
                        moved = pltpu.roll(piece, offset + tap, axis=1)[:, columns:]
                        result = result + taps_ref[tap, block] * moved
                    blocks.append(result)
                flat[half, pl.ds(cols, 128), :] = jnp.concatenate(blocks, axis=0).astype(jnp.bfloat16)
            return carry

        lax.fori_loop(0, pings // 128, one, 0, unroll=2)
        for start in range(0, pings, SPAN):
            real, imag = [
                turn(unit, flat[half, start:start + SPAN, :]).astype(jnp.bfloat16) for half in range(2)
            ]
            for piece in range(columns // lines):
                row = tile * (columns // lines) + piece
                owner = row // tiles
                target = owner // CORES
                place = (target // share * CORES + owner % CORES) * share + target % share
                place = pl.multiple_of((place * tiles + row % tiles) * 2 * lines, 2 * lines)
                a = real[piece * lines:(piece + 1) * lines]
                b = imag[piece * lines:(piece + 1) * lines]
                left[pl.ds(place, lines), start:start + SPAN] = a
                left[pl.ds(place + lines, lines), start:start + SPAN] = b
                left[pl.ds(place, lines), pings + start:pings + start + SPAN] = -b
                left[pl.ds(place + lines, lines), pings + start:pings + start + SPAN] = a

    def unpack():
        for half in range(2):
            for start in range(0, pings, 128):
                value = edge_in[half, :, start:start + 128]
                value = jnp.concatenate([jnp.zeros((columns - EDGE, 128), jnp.bfloat16), value], axis=0)
                prior[half, start:start + 128, :] = turn(unit, value).astype(jnp.bfloat16)

    def from_edge(half, cols):
        return prior[half, pl.ds(cols, 128), :]

    def from_tile(tile):
        def before(half, cols):
            value = held[lax.max(tile - 1, 0), half, pl.ds(cols, 128), :].astype(jnp.float32)
            return jnp.where(tile > 0, value, 0.0)

        return before

    def pair(group, chunk):
        rows = pl.ds(pl.multiple_of(group * share * count, share * count), share * count)
        return pltpu.make_async_remote_copy(
            src_ref=part.at[chunk, 1 - core, rows],
            dst_ref=got.at[chunk, rows],
            send_sem=pair_send.at[group, chunk],
            recv_sem=pair_recv.at[group, chunk],
            device_id=partner,
            device_id_type=MESH,
        )

    def line(way, target, chunk):
        return pltpu.make_async_remote_copy(
            src_ref=away.at[way, target, chunk],
            dst_ref=near.at[way, target, chunk],
            send_sem=line_send.at[way, target, chunk],
            recv_sem=line_recv.at[way, target, chunk],
            device_id=(above, below)[way],
            device_id_type=MESH,
        )

    def scale_line(way, target, chunk):
        return pltpu.make_async_remote_copy(
            src_ref=away_scale.at[way, target, chunk],
            dst_ref=near_scale.at[way, target, chunk],
            send_sem=scale_send.at[way, target, chunk],
            recv_sem=scale_recv.at[way, target, chunk],
            device_id=(above, below)[way],
            device_id_type=MESH,
        )

    def rows_of(target):
        return pl.ds(pl.multiple_of(target * count, count), count)

    def collect(way, target, chunk):
        scale_line(way, target, chunk).wait_recv()
        line(way, target, chunk).wait_recv()
        part[chunk, core, rows_of(target), :] += decode(
            near.at[way, target, chunk], near_scale.at[way, target, chunk], count, width
        )

    def pass_on(way, target, chunk, first):
        @pl.when(jnp.logical_not(first))
        def _():
            collect(way, target, chunk)

        encode(
            part[chunk, core, rows_of(target), :], away.at[way, target, chunk], away_scale.at[way, target, chunk]
        )
        scale_line(way, target, chunk).start()
        line(way, target, chunk).start()

    half_rows = share * count
    block = min(512, CORES * half_rows)

    def multiply(group, chunk, first):
        if first:
            for half in range(2):
                load(chunk, half).wait()
        base = group * CORES * half_rows
        if block == CORES * half_rows:
            rows = pl.ds(pl.multiple_of(base, block), block)
            value = lax.dot_general(
                left[rows, :], weights[chunk], (((1,), (1,)), ((), ())),
                preferred_element_type=jnp.float32,
            )
            into = pl.ds(pl.multiple_of(group * half_rows, half_rows), half_rows)
            part[chunk, 0, into, :] = value[:half_rows]
            part[chunk, 1, into, :] = value[half_rows:]
        else:
            def rows_at(index, carry):
                rows = pl.ds(pl.multiple_of(base + index * block, block), block)
                value = lax.dot_general(
                    left[rows, :], weights[chunk], (((1,), (1,)), ((), ())),
                    preferred_element_type=jnp.float32,
                )
                start = group * half_rows + index % (half_rows // block) * block
                into = pl.ds(pl.multiple_of(start, block), block)
                part[chunk, index // (half_rows // block), into, :] = value
                return carry

            lax.fori_loop(0, CORES * half_rows // block, rows_at, 0)
        pair(group, chunk).start()

    def join(group, chunk):
        pair(group, chunk).wait_recv()
        rows = pl.ds(pl.multiple_of(group * half_rows, half_rows), half_rows)
        part[chunk, core, rows, :] += got[chunk, rows, :]

    tables = []
    for way in range(2):
        far_first = (list(range(last, 0, -1)), list(range(last)))[way]
        tables.append(
            [
                order_of(far_first, range(group * share, (group + 1) * share))
                for group in range(groups)
            ]
        )

    def across(step, chunk):
        peer = lax.rem(me + step, tiles)
        return pltpu.make_async_remote_copy(
            src_ref=fin.at[chunk, peer],
            dst_ref=side.at[chunk, step - 1],
            send_sem=side_send.at[step - 1, chunk],
            recv_sem=side_recv.at[step - 1, chunk],
            device_id={"rng": peer},
            device_id_type=MESH,
        )

    def place(source, chunk, value):
        start = pl.multiple_of(source * (chunks * width) + chunk * width, width)
        out_ref[0, :, pl.ds(start, width)] = value[:lines]
        out_ref[1, :, pl.ds(start, width)] = value[lines:]

    def finish(chunk):
        @pl.when(chip > 0)
        def _():
            collect(0, chip, chunk)

        @pl.when(chip < last)
        def _():
            collect(1, chip, chunk)

        for tile in range(tiles):
            rows = pl.ds(pl.multiple_of(chip * count + tile * 2 * lines, 2 * lines), 2 * lines)
            fin[chunk, tile] = part[chunk, core, rows, :]
        for step in range(1, tiles):
            across(step, chunk).start()
        place(me, chunk, fin[chunk, me])

    begins = []
    for way in range(2):
        begins.append(
            [
                [
                    row.index(target) * chunks + (target, last - target)[way] * LAG if target in row else 0
                    for target in range(chips)
                ]
                for row in tables[way]
            ]
        )
    mine = me if groups > 1 else 0
    begin = jnp.maximum(pick(begins[0], mine, chip), pick(begins[1], mine, chip))

    def stream(time):
        for way in range(2):
            hops = (chip, last - chip)[way]
            at = time - hops * LAG
            target = pick(tables[way], mine, at // chunks)
            ahead = (chip < target, chip > target)[way]
            ready = jnp.logical_and(at >= 0, at < last * chunks)

            @pl.when(jnp.logical_and(ready, ahead))
            def _():
                pass_on(way, target, at % chunks, hops == 0)

        done = time - begin

        @pl.when(jnp.logical_and(done >= 0, done < chunks))
        def _():
            finish(done)

    def steps(group, turn):
        def one(chunk, carry):
            multiply(group, chunk, turn == 0)

            @pl.when(chunk > 0)
            def _():
                join(group, chunk - 1)
                stream(turn * chunks + chunk - 1)

            return carry

        lax.fori_loop(0, chunks, one, 0)
        join(group, chunks - 1)
        stream(turn * chunks + chunks - 1)

    if groups > 1:
        @pl.when(me > 0)
        def _():
            edge().wait_recv()
            unpack()

        @pl.when(me == 0)
        def _():
            prior[...] = jnp.zeros_like(prior)

        interpolate(me, from_edge)
        steps(me, 0)
        for step, copy in enumerate(copies):
            source = lax.rem(me + tiles - 1 - step, tiles)
            copy.wait_recv()
        for step, copy in enumerate(copies):
            source = lax.rem(me + tiles - 1 - step, tiles)
            interpolate(source, from_tile(source))
            steps(source, 1 + step)
    else:
        for copy in copies:
            copy.wait_recv()

        def each(tile, carry):
            interpolate(tile, from_tile(tile))
            return carry

        lax.fori_loop(0, tiles, each, 0)
        steps(0, 0)

    def rest(time, carry):
        stream(time)
        return carry

    lax.fori_loop(groups * chunks, last * chunks + last * LAG, rest, 0)

    def arrive(chunk, carry):
        for step in range(1, tiles):
            across(step, chunk).wait()
            place(lax.rem(me + tiles - step, tiles), chunk, side[chunk, step - 1])
        for group in range(groups):
            pair(group, chunk).wait_send()
        for way in range(2):
            for target in range(chips):
                ahead = (chip < target, chip > target)[way]

                @pl.when(ahead)
                def _():
                    line(way, target, chunk).wait_send()
                    scale_line(way, target, chunk).wait_send()

        return carry

    lax.fori_loop(0, chunks, arrive, 0)
    for copy in copies:
        copy.wait_send()
    if groups > 1:
        @pl.when(me < tiles - 1)
        def _():
            edge().wait_send()


def lines_image(echo, steer, offsets, taps):
    tiles = lax.axis_size("rng")
    chips = lax.axis_size("ping") // CORES
    pings, columns = echo.shape[1:]
    cells = steer.shape[1]
    width = 512 if cells % 4096 == 0 else 256
    chunks = cells // width
    lines = columns // (chips * CORES)
    count = tiles * 2 * lines
    rows = chips * count
    groups = tiles if chips % tiles == 0 else 1
    vmem = pl.BlockSpec(memory_space=pltpu.VMEM)
    smem = pl.BlockSpec(memory_space=pltpu.SMEM)
    anywhere = pl.BlockSpec(memory_space=pl.ANY)
    dma = pltpu.SemaphoreType.DMA
    message = (width // 128 * count, 128)
    scales = (max(count // 128, 1), 128)
    others = max(tiles - 1, 1)
    return pl.pallas_call(
        functools.partial(image_kernel, (tiles, chips, chunks, width, lines, groups)),
        out_shape=jax.ShapeDtypeStruct((2, lines, tiles * cells), jnp.float32),
        in_specs=[smem, anywhere, vmem, anywhere],
        out_specs=vmem,
        scratch_shapes=[
            pltpu.SMEM(taps.shape[::-1], jnp.float32),
            pltpu.VMEM((tiles, 2, pings, columns), jnp.bfloat16),
            pltpu.VMEM((2, EDGE, pings), jnp.bfloat16),
            pltpu.VMEM((2, EDGE, pings), jnp.bfloat16),
            pltpu.VMEM((2, pings, columns), jnp.bfloat16),
            pltpu.VMEM((2, pings, columns), jnp.bfloat16),
            pltpu.VMEM((CORES * rows, 2 * pings), jnp.bfloat16),
            pltpu.VMEM((chunks, width, 2 * pings), jnp.bfloat16),
            pltpu.VMEM((chunks, CORES, rows, width), jnp.float32),
            pltpu.VMEM((chunks, rows, width), jnp.float32),
            pltpu.VMEM((2, chips, chunks) + message, jnp.int16),
            pltpu.VMEM((2, chips, chunks) + message, jnp.int16),
            pltpu.VMEM((2, chips, chunks) + scales, jnp.float32),
            pltpu.VMEM((2, chips, chunks) + scales, jnp.float32),
            pltpu.VMEM((chunks, tiles, 2 * lines, width), jnp.float32),
            pltpu.VMEM((chunks, others, 2 * lines, width), jnp.float32),
            dma,
            dma,
            dma,
            dma,
            dma((others,)),
            dma((others,)),
            dma((chunks, 2)),
            dma((groups, chunks)),
            dma((groups, chunks)),
            dma((2, chips, chunks)),
            dma((2, chips, chunks)),
            dma((2, chips, chunks)),
            dma((2, chips, chunks)),
            dma((others, chunks)),
            dma((others, chunks)),
        ],
        compiler_params=pltpu.CompilerParams(
            collective_id=0, has_side_effects=True, vmem_limit_bytes=60 * 2**20
        ),
    )(offsets, taps.T, echo, steer)


LANES = 128


def split(value):
    high = value.astype(jnp.bfloat16)
    return high, (value - high.astype(jnp.float32)).astype(jnp.bfloat16)


def exact_dot(left, right):
    total = None
    for _ in range(3):
        piece = right.astype(jnp.bfloat16)
        term = jnp.dot(left, piece, preferred_element_type=jnp.float32)
        total = term if total is None else total + term
        right = right - piece.astype(jnp.float32)
    return total


def dot_exact(left, right):
    total = None
    for _ in range(3):
        piece = left.astype(jnp.bfloat16)
        term = jnp.dot(piece, right, preferred_element_type=jnp.float32)
        total = term if total is None else total + term
        left = left - piece.astype(jnp.float32)
    return total


def stacked(value, axis):
    top, low = split(value)
    return jnp.concatenate([top, low, top], axis=axis)


def spectrum_of(fields, down_ref, over_ref, twist_ref):
    size = len(fields)
    high = fields[0].shape[0] // 2
    first = jnp.dot(
        down_ref[...], stacked(jnp.concatenate(fields, axis=1), 0), preferred_element_type=jnp.float32
    )
    rows = []
    for one in range(size):
        real = first[:high, one * LANES:(one + 1) * LANES]
        imag = first[high:, one * LANES:(one + 1) * LANES]
        rows.append(
            jnp.concatenate(
                [
                    real * twist_ref[0] + imag * twist_ref[1],
                    imag * twist_ref[0] - real * twist_ref[1],
                ],
                axis=1,
            )
        )
    return jnp.dot(
        stacked(jnp.concatenate(rows, axis=0), 1), over_ref[...], preferred_element_type=jnp.float32
    )


def gradient_kernel(
    count, tiles, centers_ref, halves_ref, down_ref, over_ref, twist_ref, image_ref, total_ref, spec_ref,
    grid, value, held, full, turned, send_sem, recv_sem, send_two, recv_two,
):
    me = lax.axis_index("ping") * tiles + lax.axis_index("rng")
    ids = [lax.rem(me + step, count) for step in range(1, count)]
    peers = [{"ping": lax.div(one, tiles), "rng": lax.rem(one, tiles)} for one in ids]
    barrier = pltpu.get_barrier_semaphore()
    for peer in peers:
        pl.semaphore_signal(barrier, inc=1, device_id=peer, device_id_type=MESH)

    lines, length = image_ref.shape[1:]
    high = length // LANES
    batch = min(lines, 16)
    for half in range(2):
        for row in range(high):
            grid[pl.ds(half * high + row, lines, stride=2 * high), :] = image_ref[
                half, :, row * LANES:(row + 1) * LANES
            ]

    cells = lax.broadcasted_iota(jnp.int32, (high, LANES), 0) * LANES
    cells = cells + lax.broadcasted_iota(jnp.int32, (high, LANES), 1)
    bottom = lax.broadcasted_iota(jnp.int32, (8, LANES), 0) == 7
    lane = lax.broadcasted_iota(jnp.int32, (8, LANES), 1)
    angle = jnp.zeros((8, LANES), jnp.float32)
    for line in range(lines):
        angle = jnp.where(lane == line, centers_ref[line].astype(jnp.float32), angle)
    angle = angle * (2.0 * math.pi / length)
    turned[0] = jnp.cos(angle)
    turned[1] = jnp.sin(angle)

    def after(part):
        moved = pltpu.roll(part, high - 1, axis=0)
        end = moved[high - 8:]
        end = jnp.where(bottom, pltpu.roll(end, LANES - 1, axis=1), end)
        return jnp.concatenate([moved[:high - 8], end], axis=0)

    def field(line):
        return grid[pl.ds(pl.multiple_of(line * 2 * high, 2 * high), 2 * high), :]

    def windowed(index, carry):
        numer, denom = carry
        chosen = []
        for inner in range(batch):
            line = index * batch + inner
            distance = cells - centers_ref[line]
            distance = jnp.where(distance < 0, distance + length, distance)
            distance = jnp.minimum(distance, length - distance)
            inside = (distance <= halves_ref[line]).astype(jnp.float32)
            chosen.append(field(line) * jnp.concatenate([inside, inside], axis=0))
        found = spectrum_of(chosen, down_ref, over_ref, twist_ref)
        for inner in range(batch):
            real = found[inner * high:(inner + 1) * high, :LANES]
            imag = found[inner * high:(inner + 1) * high, LANES:]
            next_real = after(real)
            next_imag = after(imag)
            here = lane == index * batch + inner
            cos = jnp.sum(jnp.where(here, turned[0], 0.0), axis=1, keepdims=True)[:1]
            sin = jnp.sum(jnp.where(here, turned[1], 0.0), axis=1, keepdims=True)[:1]
            numer = numer + (real * next_real + imag * next_imag) * sin
            numer = numer + (real * next_imag - imag * next_real) * cos
            denom = denom + (real * real + imag * imag)
        return numer, denom

    zero = jnp.zeros((high, LANES), jnp.float32)
    numer, denom = lax.fori_loop(0, lines // batch, windowed, (zero, zero))
    each = value.shape[1]
    for block in range(count // 2):
        value[block] = numer[block * each:(block + 1) * each]
        value[count // 2 + block] = denom[block * each:(block + 1) * each]

    pl.semaphore_wait(barrier, len(peers))
    copies = []
    for step, peer in enumerate(peers):
        copy = pltpu.make_async_remote_copy(
            src_ref=value.at[ids[step]],
            dst_ref=held.at[step],
            send_sem=send_sem.at[step],
            recv_sem=recv_sem.at[step],
            device_id=peer,
            device_id_type=MESH,
        )
        copy.start()
        copies.append(copy)

    def whole(index, carry):
        found = spectrum_of(
            [field(index * batch + inner) for inner in range(batch)], down_ref, over_ref, twist_ref
        )
        spec_ref[pl.ds(pl.multiple_of(index * batch * high, batch * high), batch * high), :] = found
        return carry

    lax.fori_loop(0, lines // batch, whole, 0)
    total = value[me]
    for step, copy in enumerate(copies):
        copy.wait()
        total = total + held[step]
    full[me] = total
    copies = []
    for step, peer in enumerate(peers):
        copy = pltpu.make_async_remote_copy(
            src_ref=full.at[me],
            dst_ref=full.at[me],
            send_sem=send_two.at[step],
            recv_sem=recv_two.at[step],
            device_id=peer,
            device_id_type=MESH,
        )
        copy.start()
        copies.append(copy)
    for copy in copies:
        copy.wait()
    for block in range(count):
        total_ref[block * each:(block + 1) * each, :] = full[block]


def correct_kernel(
    up_ref, back_ref, twist_ref, total_ref, spec_ref, out_ref, phase_ref, grid, turn, tall,
):
    group = out_ref.shape[1]
    length = out_ref.shape[2]
    high = length // LANES

    @pl.when(pl.program_id(0) == 0)
    def _():
        slope = total_ref[:high] / (total_ref[high:] + epsilon)
        row = lax.broadcasted_iota(jnp.int32, (high, high), 0)
        below = (lax.broadcasted_iota(jnp.int32, (high, high), 1) < row).astype(jnp.float32)
        row = lax.broadcasted_iota(jnp.int32, (LANES, LANES), 0)
        ahead = (row < lax.broadcasted_iota(jnp.int32, (LANES, LANES), 1)).astype(jnp.float32)
        within = exact_dot(below.astype(jnp.bfloat16), slope)
        sums = jnp.broadcast_to(jnp.sum(slope, axis=0, keepdims=True), (8, LANES))
        across = dot_exact(sums, ahead.astype(jnp.bfloat16))
        mean = jnp.sum(sums[:1], axis=1, keepdims=True) / length
        order = lax.broadcasted_iota(jnp.int32, (high, LANES), 0)
        order = order + high * lax.broadcasted_iota(jnp.int32, (high, LANES), 1)
        phase = within + across[:1] - order.astype(jnp.float32) * mean
        ratio = LANES // high
        tall[:, :high] = phase.T
        phase_ref[...] = jnp.concatenate(
            [tall[pl.ds(part, LANES // ratio, stride=ratio), :high] for part in range(ratio)], axis=1
        )
        turn[0] = jnp.cos(phase)
        turn[1] = jnp.sin(phase)

    cos = turn[0]
    sin = turn[1]
    start = pl.program_id(0) * group * high
    rows = []
    for line in range(group):
        at = pl.ds(pl.multiple_of(start + line * high, high), high)
        real = spec_ref[at, :LANES]
        imag = spec_ref[at, LANES:]
        rows.append(jnp.concatenate([real * cos + imag * sin, imag * cos - real * sin], axis=1))
    first = jnp.dot(
        stacked(jnp.concatenate(rows, axis=0), 1), back_ref[...], preferred_element_type=jnp.float32
    )
    fields = []
    for line in range(group):
        real = first[line * high:(line + 1) * high, :LANES]
        imag = first[line * high:(line + 1) * high, LANES:]
        fields.append(
            jnp.concatenate(
                [
                    real * twist_ref[2] - imag * twist_ref[3],
                    real * twist_ref[3] + imag * twist_ref[2],
                ],
                axis=0,
            )
        )
    second = jnp.dot(
        up_ref[...], stacked(jnp.concatenate(fields, axis=1), 0), preferred_element_type=jnp.float32
    )
    for line in range(group):
        grid[line * 2 * high:(line + 1) * 2 * high, :] = second[:, line * LANES:(line + 1) * LANES]
    for half in range(2):
        for row in range(high):
            out_ref[half, :, row * LANES:(row + 1) * LANES] = grid[
                pl.ds(half * high + row, group, stride=2 * high), :
            ]


def waves(size, modulus, columns):
    angle = 2.0 * np.pi / modulus * (np.outer(np.arange(size), np.arange(columns)) % modulus)
    return np.cos(angle), np.sin(angle)


def pieces_of(matrix, axis):
    high = matrix.astype(jnp.bfloat16)
    low = (matrix - high.astype(np.float64)).astype(jnp.bfloat16)
    return np.concatenate([high, high, low], axis=axis)


def focus(image, centers, halves):
    pings, tiles = lax.axis_size("ping"), lax.axis_size("rng")
    count = pings * tiles
    lines, length = image.shape[1:]
    high = length // LANES
    cos, sin = waves(high, high, high)
    down = pieces_of(np.block([[cos, sin], [-sin, cos]]), 1)
    up = pieces_of(np.block([[cos, -sin], [sin, cos]]), 1)
    cos, sin = waves(LANES, LANES, LANES)
    over = pieces_of(np.block([[cos, -sin], [sin, cos]]), 0)
    back = pieces_of(np.block([[cos, sin], [-sin, cos]]), 0)
    cos, sin = waves(high, length, LANES)
    twist = np.stack([cos, sin, cos / length, sin / length]).astype(np.float32)
    each = 2 * high // count
    group = lines
    vmem = pl.BlockSpec(memory_space=pltpu.VMEM)
    smem = pl.BlockSpec(memory_space=pltpu.SMEM)
    semaphores = pltpu.SemaphoreType.DMA((count - 1,))
    total, spec = pl.pallas_call(
        functools.partial(gradient_kernel, count, tiles),
        out_shape=(
            jax.ShapeDtypeStruct((2 * high, LANES), jnp.float32),
            jax.ShapeDtypeStruct((lines * high, 2 * LANES), jnp.float32),
        ),
        in_specs=[smem, smem] + [vmem] * 4,
        out_specs=(vmem, vmem),
        scratch_shapes=[
            pltpu.VMEM((lines * 2 * high, LANES), jnp.float32),
            pltpu.VMEM((count, each, LANES), jnp.float32),
            pltpu.VMEM((count - 1, each, LANES), jnp.float32),
            pltpu.VMEM((count, each, LANES), jnp.float32),
            pltpu.VMEM((2, 8, LANES), jnp.float32),
            semaphores,
            semaphores,
            semaphores,
            semaphores,
        ],
        compiler_params=pltpu.CompilerParams(collective_id=1, has_side_effects=True),
    )(centers, halves, down, over, twist, image)
    focused, phase = pl.pallas_call(
        correct_kernel,
        grid=(lines // group,),
        out_shape=(
            jax.ShapeDtypeStruct((2, lines, length), jnp.float32),
            jax.ShapeDtypeStruct((high, LANES), jnp.float32),
        ),
        in_specs=[vmem] * 5,
        out_specs=(
            pl.BlockSpec((2, group, length), lambda index: (0, index, 0)),
            pl.BlockSpec((high, LANES), lambda index: (0, 0)),
        ),
        scratch_shapes=[
            pltpu.VMEM((group * 2 * high, LANES), jnp.float32),
            pltpu.VMEM((2, high, LANES), jnp.float32),
            pltpu.VMEM((LANES, LANES), jnp.float32),
        ],
    )(up, back, twist, total, spec)
    return focused, phase.reshape(length)


def on_device(echo, steer, offsets, taps, centers, halves):
    image = lines_image(echo, steer, offsets, taps)
    return focus(image, centers, halves)


def solution(mesh):
    in_specs = (
        P(None, ("leg", "ping"), "rng"),
        P(None, ("leg", "rng"), "ping"),
        P(("leg", "ping")),
        P(("leg", "ping"), None),
        P(("leg", "ping", "rng")),
        P(("leg", "ping", "rng")),
    )
    out_specs = (P(None, ("leg", "ping", "rng"), None), P("leg"))
    return jax.shard_map(
        on_device, mesh=mesh, in_specs=in_specs, out_specs=out_specs, check_vma=False
    )
```
